256 devices in a mesh: rows: 16 (over z_lo, x), cols: 16 (over y, z_hi, core).
Axes of the slice: x: 4, y: 4, z: 8 (z_hi: 2, z_lo: 4; z = z_hi * 4 + z_lo), core: 2. Of those that a mesh axis runs over, the one named last changes fastest.
Arguments:
- kernel_hat: bfloat16 [2, 256, 512, 4096], P(None, 'rows', 'cols'), may hold values from -0.5 to 0.5
- coefficients: float32 [128, 512], P(None, 'cols'), may hold values from -6 to 6
- wave_speed_sq: float32 [4096, 4096], P('rows', 'cols'), may hold values from 1 to 4
- wet_mask: int32 [4096, 4096], P('rows', 'cols'), may hold values 0 or 1
- boundary_cell: int32 [4096], replicated, may hold values from 0 to 4095, each once
- height: float32 [4096, 4096], P('rows', 'cols'), may hold values from -3 to 3
- flux_x: float32 [4096, 4096], P('rows', 'cols'), may hold values from -3 to 3
- flux_y: float32 [4096, 4096], P('rows', 'cols'), may hold values from -3 to 3
Outputs:
- boundary_series: float32 [128, 4096], P('rows', 'cols')
- height_out: float32 [4096, 4096], P('rows', 'cols')
- flux_x_out: float32 [4096, 4096], P('rows', 'cols')
- flux_y_out: float32 [4096, 4096], P('rows', 'cols')
The draws below stay inside these ranges and needn't reach their ends.
Inputs may be any that keep to these rules, and one draw needn't show every extreme that they name: `boundary_cell`: each of the 4096 boundary points names a different grid column, so each column is named by exactly one point.
All inputs are finite; a program needn't handle non-finite values. No bound on the sum of `wet_mask` on one device may be relied on, other than what follows from the above.
Results may differ from the reference program's by a relative error of at most 0.0029.
Values sent between devices are 32-bit elements; how exact they have to be, the bound alone decides.
A program may use at most 64 MiB of HBM per device.

```python
import math
import jax
import jax.numpy as jnp
from jax import lax

NT = 128
SRC = 512
NF = 256
OBS = 4096
NR = 4096
NC = 4096


def touch_ends(array, own_key, least, top_value):
    longest = array.shape.index(max(array.shape))
    spots = []
    for shift in (0, 1):
        where = [jax.random.randint(jax.random.fold_in(own_key, axis), (), 0, length) for axis, length in enumerate(array.shape)]
        where[longest] = (where[longest] + shift) % array.shape[longest]
        spots.append(tuple(where))
    return array.at[spots[0]].set(least).at[spots[1]].set(top_value)


def block_scale(rng, extent, shards, least, largest):
    factor_of, own = 1.0, jax.random.fold_in(rng, 6)
    for axis_at, shards_of in shards:
        steps = jnp.exp(jax.random.uniform(jax.random.fold_in(own, axis_at), (shards_of,), jnp.float32, least / len(shards), largest / len(shards)))
        factor_of = factor_of * jnp.repeat(steps, extent[axis_at] // shards_of).reshape([-1 if axis == axis_at else 1 for axis in range(len(extent))])
    return factor_of


def scatter_about(key, shape, width, reach, cuts=(), kind=jnp.bfloat16):
    values = width * jax.random.normal(key, shape, jnp.float32)
    if cuts:
        values = values * block_scale(key, shape, cuts, -0.22, 0.18)
    return jnp.clip(values, -reach, reach).astype(kind)


def setup_inputs(seed: int = 0) -> dict:
    keys = jax.random.split(jax.random.key(seed), 9)
    return {
        "kernel_hat": scatter_about(keys[0], (2, NF, SRC, OBS), (SRC // 4) ** -0.5, 0.5, ((1, 16), (2, 16))),
        "coefficients": scatter_about(keys[1], (NT, SRC), 1.0, 6.0, ((1, 16),), jnp.float32),
        "wave_speed_sq": jnp.clip(jnp.exp(math.log(4.0) - 1.3862944 * jax.random.uniform(keys[2], (NR, NC), jnp.float32) ** block_scale(keys[2], (NR, NC), ((0, 16), (1, 16)), -0.2, 0.2)), 1.0, 4.0),
        "wet_mask": touch_ends((jax.random.randint(keys[3], (NR, NC), 0, 4) < 3).astype(jnp.int32), jax.random.fold_in(keys[3], 1), 0, 1),
        "boundary_cell": jax.random.permutation(keys[4], OBS).astype(jnp.int32),
        "height": scatter_about(keys[5], (NR, NC), 0.5, 3.0, ((0, 16), (1, 16)), jnp.float32),
        "flux_x": scatter_about(keys[6], (NR, NC), 0.5, 3.0, ((0, 16), (1, 16)), jnp.float32),
        "flux_y": scatter_about(keys[7], (NR, NC), 0.5, 3.0, ((0, 16), (1, 16)), jnp.float32),
    }


STEP_RATIO = 0.25

def neighbours(values, along_dim):
    if along_dim == 1:
        return (values[1:-1, :-1], values[1:-1, 1:])
    return (values[:-1, 1:-1], values[1:, 1:-1])

def face_fluxes(surface, along, across, speed_sq, celerity, wet, along_dim):
    left_surf, right_surf = neighbours(surface, along_dim)
    left_along, right_along = neighbours(along, along_dim)
    left_across, right_across = neighbours(across, along_dim)
    left_sq, right_sq = neighbours(speed_sq, along_dim)
    left_speed, right_speed = neighbours(celerity, along_dim)
    left_wet, right_wet = neighbours(wet, along_dim)
    opened = left_wet * right_wet
    damping = 0.25 * (left_speed + right_speed)
    mass_flux = opened * (0.5 * (left_along + right_along) - damping * (right_surf - left_surf))
    momentum = opened * (0.5 * (left_sq * left_surf + right_sq * right_surf) - damping * (right_along - left_along))
    shear_flux = opened * (-damping * (right_across - left_across))
    return (mass_flux, momentum, shear_flux)

def advance(surface, along_x, along_y, speed_sq, wet):
    celerity = jnp.sqrt(speed_sq)
    mass_x, momentum_x, shear_x = face_fluxes(surface, along_x, along_y, speed_sq, celerity, wet, 1)
    mass_y, momentum_y, shear_y = face_fluxes(surface, along_y, along_x, speed_sq, celerity, wet, 0)
    interior_wet = wet[1:-1, 1:-1]

    def update(values, flux_cols, flux_rows):
        change = flux_cols[:, 1:] - flux_cols[:, :-1] + (flux_rows[1:] - flux_rows[:-1])
        return interior_wet * (values[1:-1, 1:-1] - STEP_RATIO * change)
    return (update(surface, mass_x, mass_y), update(along_x, momentum_x, shear_y), update(along_y, shear_x, momentum_y))

def reference(kernel_hat, coefficients, wave_speed_sq, wet_mask, boundary_cell, height, flux_x, flux_y):
    spectrum = jnp.fft.fft(coefficients, n=NF, axis=0)
    coef_re = lax.optimization_barrier(jnp.real(spectrum).astype(jnp.bfloat16)).astype(jnp.float32)
    coef_im = lax.optimization_barrier(jnp.imag(spectrum).astype(jnp.bfloat16)).astype(jnp.float32)
    high = lax.Precision.HIGHEST

    def one_frequency(index):
        kern_re = lax.dynamic_index_in_dim(kernel_hat[0], index, 0, keepdims=False).astype(jnp.float32)
        kern_im = lax.dynamic_index_in_dim(kernel_hat[1], index, 0, keepdims=False).astype(jnp.float32)
        row_re = lax.dynamic_index_in_dim(coef_re, index, 0, keepdims=False)
        row_im = lax.dynamic_index_in_dim(coef_im, index, 0, keepdims=False)
        spec_re = jnp.dot(row_re, kern_re, precision=high) - jnp.dot(row_im, kern_im, precision=high)
        spec_im = jnp.dot(row_im, kern_re, precision=high) + jnp.dot(row_re, kern_im, precision=high)
        return (spec_re, spec_im)
    spec_re, spec_im = lax.map(one_frequency, jnp.arange(NF, dtype=jnp.int32))
    times = jnp.arange(NT, dtype=jnp.int32)
    freqs = jnp.arange(NF, dtype=jnp.int32)
    phase = (times[:, None] * freqs[None, :] % NF).astype(jnp.float32) * (2.0 * math.pi / NF)
    series = (jnp.dot(jnp.cos(phase), spec_re, precision=high) - jnp.dot(jnp.sin(phase), spec_im, precision=high)) / NF
    latest = series[NT - 2:]
    ghost = jnp.zeros((2, NC), jnp.float32).at[:, boundary_cell].set(latest)
    wet = wet_mask.astype(jnp.float32)
    speed_pad = jnp.pad(wave_speed_sq, 1).at[-1].set(1.0)
    wet_pad = jnp.pad(wet, 1).at[-1].set(1.0)
    surface, along_x, along_y = (height, flux_x, flux_y)
    for step in range(2):
        surf_pad = jnp.pad(surface, 1).at[-1, 1:-1].set(ghost[step])
        surface, along_x, along_y = advance(surf_pad, jnp.pad(along_x, 1), jnp.pad(along_y, 1), speed_pad, wet_pad)
    return (series, surface, along_x, along_y)
```

```python
import functools

import jax
import jax.numpy as jnp
import numpy as np
from jax import lax
from jax.experimental import pallas as pl
from jax.experimental.pallas import tpu as pltpu
from jax.sharding import PartitionSpec as P

F32 = jnp.float32
BF16 = jnp.bfloat16
HIGH = lax.Precision.HIGHEST
MESH = pl.DeviceIdType.MESH
ORDER = (2, 1, 3, 0)


def transform_tables():
    table = np.zeros((16, 128, 128), np.float32)
    times = np.arange(128)
    inner = times.reshape(4, 4, 8).transpose(1, 0, 2).reshape(-1)
    for row in range(16):
        freqs = row * 16 + np.arange(16)
        angle = 2.0 * np.pi * ((freqs[:, None] * inner[None, :]) % 256) / 256.0
        table[row, 0:16] = np.cos(angle) / 256.0
        table[row, 16:32] = -np.sin(angle) / 256.0
        angle = 2.0 * np.pi * ((freqs[:, None] * times[None, :]) % 256) / 256.0
        table[row, 32:48] = np.cos(angle)
        table[row, 48:64] = -np.sin(angle)
        table[row, 64:80] = np.sin(angle)
        table[row, 80:96] = np.cos(angle)
    return table


def after(values, axis):
    return pltpu.roll(values, values.shape[axis] - 1, axis)


def before(values, axis):
    return pltpu.roll(values, 1, axis)


def face_terms(speed, wet):
    celerity = jnp.sqrt(speed)
    terms = []
    for axis in (1, 0):
        opened = wet * after(wet, axis)
        terms.append((0.5 * opened, opened * (0.25 * (celerity + after(celerity, axis)))))
    return terms


def advance(surface, along_x, along_y, speed, wet, terms):
    pressure = speed * surface
    changes = []
    for axis, along, across in ((1, along_x, along_y), (0, along_y, along_x)):
        half, damp = terms[1 - axis]
        next_along = after(along, axis)
        mass = half * (along + next_along) - damp * (after(surface, axis) - surface)
        push = half * (pressure + after(pressure, axis)) - damp * (next_along - along)
        shear = damp * (across - after(across, axis))
        changes.append(tuple(flux - before(flux, axis) for flux in (mass, push, shear)))
    (mass_x, push_x, shear_x), (mass_y, push_y, shear_y) = changes
    return (
        wet * (surface - 0.25 * (mass_x + mass_y)),
        wet * (along_x - 0.25 * (push_x + shear_y)),
        wet * (along_y - 0.25 * (shear_x + push_y)),
    )


def kernel(
    kern, coef, speed, mask, cells, surf, flow_x, flow_y, table,
    series_o, surf_o, flow_x_o, flow_y_o,
    kbuf, tab, cbuf, mbuf, cellbuf, left, own, dsend, drecv, ysend, yrecv,
    xsend, xrecv, zsend, zrecv, gsend, grecv, fields, ewsend, ewrecv, onehot, latest,
    ksem, lsem, dsem, ysem, xsem, zsem, gssem, grsem, nssem, ewsem,
):
    row, col = lax.axis_index("rows"), lax.axis_index("cols")
    x, z_lo = row % 4, row // 4
    y, z_hi, core = col // 4, (col // 2) % 2, col % 2
    z = z_hi * 4 + z_lo
    is_edge = row == 15

    def place(at_x, at_y, at_z, at_core):
        return ((at_z % 4) * 4 + at_x, at_y * 4 + (at_z // 4) * 2 + at_core)

    partner = place(x, y, z, 1 - core)
    y_peer = [place(x, (y + d) % 4, z, core) for d in range(4)]
    x_peer = [place((x + d) % 4, y, z, core) for d in range(4)]
    z_peer = [place(x, y, (z + d) % 8, core) for d in range(8)]
    north, south = ((row + 15) % 16, col), ((row + 1) % 16, col)
    west, east = (row, (col + 15) % 16), (row, (col + 1) % 16)

    barrier = pltpu.get_barrier_semaphore()
    for peer in [partner, *y_peer[1:], *x_peer[1:], *z_peer[1:], north, south, west, east]:
        pl.semaphore_signal(barrier, inc=1, device_id=peer, device_id_type=MESH)

    @pl.when(is_edge)
    def _():
        def greet(index, carry):
            at_z, at_col = index // 8, index % 8
            peer = place(3, at_col // 2, at_z, at_col % 2)

            @pl.when((peer[0] != row) | (peer[1] != col))
            def _():
                pl.semaphore_signal(barrier, inc=1, device_id=peer, device_id_type=MESH)

            return carry

        lax.fori_loop(0, 64, greet, 0)

    local = [
        pltpu.make_async_copy(table.at[row], tab, lsem.at[0]),
        pltpu.make_async_copy(coef, cbuf, lsem.at[1]),
    ]
    for copy in local:
        copy.start()
    loads = []
    for i, d in enumerate(ORDER):
        for side, par in enumerate((1 - core, core)):
            for part in range(2):
                slot = i * 4 + side * 2 + part
                start = pl.multiple_of(((((y + d) % 4) * 2 + part) * 2 + par) * 256, 256)
                copy = pltpu.make_async_copy(
                    kern.at[:, pl.ds(start, 256)], kbuf.at[slot], ksem.at[slot]
                )
                copy.start()
                loads.append(copy)
    inner = (pl.ds(8, 256), pl.ds(0, 256))
    grids = [
        pltpu.make_async_copy(ref, fields.at[(j, *inner)], lsem.at[2 + j])
        for j, ref in enumerate((surf, flow_x, flow_y, speed))
    ]
    grids += [
        pltpu.make_async_copy(mask, mbuf, lsem.at[6]),
        pltpu.make_async_copy(cells, cellbuf, lsem.at[7]),
    ]
    for copy in grids:
        copy.start()

    for copy in local:
        copy.wait()
    tables = tab[...]
    coefs = jnp.dot(tables[32:96], cbuf[...], precision=HIGH, preferred_element_type=F32)
    lanes = lax.broadcasted_iota(jnp.int32, (32, 512), 1)
    subs = lax.broadcasted_iota(jnp.int32, (32, 512), 0)
    spread = (lanes % 32 == subs).astype(F32).astype(BF16)
    tiled = jnp.dot(coefs.astype(BF16), spread, preferred_element_type=F32)
    diagonal = lanes // 32 == subs % 16
    left[:, 0:512] = jnp.where(diagonal, tiled[0:32], 0.0).astype(BF16)
    left[:, 512:1024] = jnp.where(diagonal, tiled[32:64], 0.0).astype(BF16)

    dcopy, ycopy = [], {}

    def merge(i):
        d = ORDER[i]
        dcopy[i].wait_recv()
        total = own[i] + drecv[i]
        if d == 0:
            own[i] = total
            return
        ysend[d - 1] = total
        ycopy[d] = pltpu.make_async_remote_copy(
            src_ref=ysend.at[d - 1], dst_ref=yrecv.at[d - 1],
            send_sem=ysem.at[0, d - 1], recv_sem=ysem.at[1, d - 1],
            device_id=y_peer[d], device_id_type=MESH,
        )
        ycopy[d].start()

    for i in range(4):
        for side in range(2):
            for part in range(2):
                slot = i * 4 + side * 2 + part
                loads[slot].wait()
                spec = jnp.dot(left[...], kbuf[slot], preferred_element_type=F32)
                target = own if side else dsend
                target[i, :, part * 256 : part * 256 + 256] = spec
            if side == 0:
                if i == 0:
                    pl.semaphore_wait(
                        barrier, 18 + jnp.where(x == 3, 16 - is_edge.astype(jnp.int32), 0)
                    )
                copy = pltpu.make_async_remote_copy(
                    src_ref=dsend.at[i], dst_ref=drecv.at[i],
                    send_sem=dsem.at[0, i], recv_sem=dsem.at[1, i],
                    device_id=partner, device_id_type=MESH,
                )
                copy.start()
                dcopy.append(copy)
        if i >= 1:
            merge(i - 1)

    for copy in grids:
        copy.wait()
    fields[(4, *inner)] = mbuf[...].astype(F32)
    ns_copies = []
    for at, (first, last, peer) in enumerate(((8, 264, north), (256, 0, south))):
        copy = pltpu.make_async_remote_copy(
            src_ref=fields.at[:, pl.ds(first, 8), pl.ds(0, 256)],
            dst_ref=fields.at[:, pl.ds(last, 8), pl.ds(0, 256)],
            send_sem=nssem.at[0, at], recv_sem=nssem.at[1, at],
            device_id=peer, device_id_type=MESH,
        )
        copy.start()
        ns_copies.append(copy)
    merge(3)

    def select(block, carry):
        at = lax.broadcasted_iota(jnp.int32, (384, 128), 0)
        column = col * 256 + jnp.where(at >= 320, at - 384, at)
        found = cellbuf[pl.ds(block, 1), :] == column
        onehot[:, pl.ds(pl.multiple_of(block * 128, 128), 128)] = jnp.where(
            found, 1.0, 0.0
        ).astype(BF16)
        return carry

    @pl.when(is_edge)
    def _():
        lax.fori_loop(0, 32, select, 0)

    for copy in ns_copies:
        copy.wait_recv()

    @pl.when(row == 0)
    def _():
        fields[:, 0:8, 0:256] = jnp.zeros((5, 8, 256), F32)

    @pl.when(is_edge)
    def _():
        fields[:, 264:272, 0:256] = jnp.zeros((5, 8, 256), F32)

    lane = lax.broadcasted_iota(jnp.int32, (272, 128), 1)
    ew_copies = []
    for at, (first, shift, peer) in enumerate(((0, 0, west), (128, 2, east))):
        packed = jnp.zeros((272, 128), F32)
        for j in range(5):
            block = fields[j, :, first : first + 128]
            if 2 * j + shift:
                block = pltpu.roll(block, 2 * j + shift, 1)
            packed = jnp.where(lane // 2 == j, block, packed)
        packed = jnp.concatenate([packed, jnp.zeros((112, 128), F32)], axis=0)
        ewsend[at] = packed.T[0:16]
        copy = pltpu.make_async_remote_copy(
            src_ref=ewsend.at[at], dst_ref=ewrecv.at[at],
            send_sem=ewsem.at[0, at], recv_sem=ewsem.at[1, at],
            device_id=peer, device_id_type=MESH,
        )
        copy.start()
        ew_copies.append(copy)

    total = own[3]
    for d in (1, 3, 2):
        ycopy[d].wait_recv()
        total = total + yrecv[d - 1]
    inverse = tables.T[:, 0:32]
    partial = jnp.dot(inverse, total, precision=HIGH, preferred_element_type=F32)
    for at in range(4):
        xsend[at] = partial[at * 32 : at * 32 + 32]
    xcopy = {}
    for d in (2, 1, 3):
        xcopy[d] = pltpu.make_async_remote_copy(
            src_ref=xsend.at[(x + d) % 4], dst_ref=xrecv.at[d - 1],
            send_sem=xsem.at[0, d - 1], recv_sem=xsem.at[1, d - 1],
            device_id=x_peer[d], device_id_type=MESH,
        )
        xcopy[d].start()

    for copy in ew_copies:
        copy.wait_recv()
    sides = []
    for at, end in ((0, 15), (1, 0)):
        message = jnp.where(col == end, 0.0, ewrecv[at])
        padded = jnp.concatenate([message, jnp.zeros((112, 384), F32)], axis=0)
        sides.append(padded.T[0:272])
    for j in range(5):
        right = pltpu.roll(sides[0], 128 - 2 * j, 1) if j else sides[0]
        wrapped = pltpu.roll(sides[1], 126 - 2 * j, 1)
        fields[j, :, 256:384] = jnp.where(
            lane < 2, right, jnp.where(lane >= 126, wrapped, 0.0)
        )

    total = xsend[x]
    for d in (1, 3, 2):
        xcopy[d].wait_recv()
        total = total + xrecv[d - 1]
    zsend[0] = total[:, 0:256]
    zsend[1] = total[:, 256:512]
    gsend[...] = total[30:32]
    me = z * 8 + y * 2 + core

    def ghost_copy(index):
        return pltpu.make_async_remote_copy(
            src_ref=gsend, dst_ref=grecv.at[me],
            send_sem=gssem.at[index], recv_sem=grsem,
            device_id=(15, index), device_id_type=MESH,
        )

    @pl.when(x == 3)
    def _():
        def send(index, carry):
            @pl.when((row != 15) | (index != col))
            def _():
                ghost_copy(index).start()

            return carry

        lax.fori_loop(0, 16, send, 0)

    zcopy = {}
    for d in (4, 3, 5, 2, 6, 1, 7):
        to = (z + d) % 8
        zcopy[d] = pltpu.make_async_remote_copy(
            src_ref=zsend.at[to // 4, pl.ds(pl.multiple_of((to % 4) * 8, 8), 8)],
            dst_ref=zrecv.at[d - 1],
            send_sem=zsem.at[0, d - 1], recv_sem=zsem.at[1, d - 1],
            device_id=z_peer[d], device_id_type=MESH,
        )
        zcopy[d].start()

    def strip(at, carry):
        base = pl.multiple_of(at * 32, 8)
        state = [fields[j, pl.ds(base, 48), :] for j in range(5)]
        values, rest = state[0:3], state[3:5]
        terms = face_terms(*rest)
        for _ in range(2):
            values = advance(*values, *rest, terms)
        for ref, value in zip((surf_o, flow_x_o, flow_y_o), values):
            ref[pl.ds(base, 32), :] = value[8:40, 0:256]
        return carry

    lax.fori_loop(0, 8, strip, 0)

    total = zsend[z_hi, pl.ds(pl.multiple_of(z_lo * 8, 8), 8)]
    for d in range(1, 8):
        zcopy[d].wait_recv()
        total = total + zrecv[d - 1]
    series_o[...] = total

    @pl.when(is_edge)
    def _():
        grecv[me] = gsend[...]
        pltpu.make_async_copy(grecv.at[pl.ds(0, 63)], grecv.at[pl.ds(0, 63)], grsem).wait()
        latest[...] = jnp.zeros((8, 4096), F32)
        for at in range(8):
            summed = grecv[at]
            for other in range(1, 8):
                summed = summed + grecv[other * 8 + at]
            for part in range(2):
                first = ((at // 2 * 2 + part) * 2 + at % 2) * 256
                latest[0:2, first : first + 256] = summed[:, part * 256 : part * 256 + 256]
        value = latest[...]
        high = value.astype(BF16)
        value = value - high.astype(F32)
        middle = value.astype(BF16)
        low = (value - middle.astype(F32)).astype(BF16)
        ghost = jnp.zeros((8, 384), F32)
        for piece in (low, middle, high):
            ghost = ghost + lax.dot_general(
                piece, onehot[...], (((1,), (1,)), ((), ())), preferred_element_type=F32
            )
        beyond = lax.broadcasted_iota(jnp.int32, (24, 384), 0) == 16
        state = [fields[j, 248:272, :] for j in range(5)]
        rest = [jnp.where(beyond, 1.0, value) for value in state[3:5]]
        values = state[0:3]
        terms = face_terms(*rest)
        for step in range(2):
            values = [
                jnp.where(beyond, ghost[step : step + 1], values[0]),
                jnp.where(beyond, 0.0, values[1]),
                jnp.where(beyond, 0.0, values[2]),
            ]
            values = advance(*values, *rest, terms)
        for ref, value in zip((surf_o, flow_x_o, flow_y_o), values):
            ref[248:256, :] = value[8:16, 0:256]

    for copy in [*dcopy, *ycopy.values(), *xcopy.values(), *zcopy.values(), *ns_copies, *ew_copies]:
        copy.wait_send()

    @pl.when(x == 3)
    def _():
        def finish(index, carry):
            @pl.when((row != 15) | (index != col))
            def _():
                ghost_copy(index).wait_send()

            return carry

        lax.fori_loop(0, 16, finish, 0)


def on_device(
    kernel_hat, coefficients, wave_speed_sq, wet_mask, boundary_cell, height, flux_x, flux_y
):
    field = jax.ShapeDtypeStruct((256, 256), F32)
    dma = pltpu.SemaphoreType.DMA
    return pl.pallas_call(
        kernel,
        out_shape=(jax.ShapeDtypeStruct((8, 256), F32), field, field, field),
        in_specs=[pl.BlockSpec(memory_space=pltpu.MemorySpace.HBM)] * 9,
        out_specs=[pl.BlockSpec(memory_space=pltpu.VMEM)] * 4,
        scratch_shapes=[
            pltpu.VMEM((16, 1024, 256), BF16),
            pltpu.VMEM((128, 128), F32),
            pltpu.VMEM((128, 32), F32),
            pltpu.VMEM((256, 256), jnp.int32),
            pltpu.VMEM((32, 128), jnp.int32),
            pltpu.VMEM((32, 1024), BF16),
            pltpu.VMEM((4, 32, 512), F32),
            pltpu.VMEM((4, 32, 512), F32),
            pltpu.VMEM((4, 32, 512), F32),
            pltpu.VMEM((3, 32, 512), F32),
            pltpu.VMEM((3, 32, 512), F32),
            pltpu.VMEM((4, 32, 512), F32),
            pltpu.VMEM((3, 32, 512), F32),
            pltpu.VMEM((2, 32, 256), F32),
            pltpu.VMEM((7, 8, 256), F32),
            pltpu.VMEM((2, 512), F32),
            pltpu.VMEM((64, 2, 512), F32),
            pltpu.VMEM((5, 272, 384), F32),
            pltpu.VMEM((2, 16, 384), F32),
            pltpu.VMEM((2, 16, 384), F32),
            pltpu.VMEM((384, 4096), BF16),
            pltpu.VMEM((8, 4096), F32),
            dma((16,)),
            dma((8,)),
            dma((2, 4)),
            dma((2, 3)),
            dma((2, 3)),
            dma((2, 7)),
            dma((16,)),
            dma(()),
            dma((2, 2)),
            dma((2, 2)),
        ],
        compiler_params=pltpu.CompilerParams(
            collective_id=0, has_side_effects=True, vmem_limit_bytes=48 * 1024 * 1024
        ),
    )(
        kernel_hat.reshape(1024, 4096),
        coefficients,
        wave_speed_sq,
        wet_mask,
        boundary_cell.reshape(32, 128),
        height,
        flux_x,
        flux_y,
        jnp.asarray(transform_tables()),
    )


def solution(mesh):
    return jax.shard_map(
        on_device,
        mesh=mesh,
        in_specs=(
            P(None, "rows", "cols", None),
            P(None, "cols"),
            P("rows", "cols"),
            P("rows", "cols"),
            P(),
            P("rows", "cols"),
            P("rows", "cols"),
            P("rows", "cols"),
        ),
        out_specs=(P("rows", "cols"), P("rows", "cols"), P("rows", "cols"), P("rows", "cols")),
        check_vma=False,
    )
```

```python
import functools

import jax
import jax.numpy as jnp
import numpy as np
from jax import lax
from jax.experimental import pallas as pl
from jax.experimental.pallas import tpu as pltpu
from jax.sharding import PartitionSpec as P

F32 = jnp.float32
BF16 = jnp.bfloat16
HIGH = lax.Precision.HIGHEST
MESH = pl.DeviceIdType.MESH
ORDER = (2, 1, 3, 0)


def transform_tables():
    table = np.zeros((16, 128, 128), np.float32)
    times = np.arange(128)
    inner = times.reshape(4, 4, 8).transpose(1, 0, 2).reshape(-1)
    for row in range(16):
        freqs = row * 16 + np.arange(16)
        angle = 2.0 * np.pi * ((freqs[:, None] * inner[None, :]) % 256) / 256.0
        table[row, 0:16] = np.cos(angle) / 256.0
        table[row, 16:32] = -np.sin(angle) / 256.0
        angle = 2.0 * np.pi * ((freqs[:, None] * times[None, :]) % 256) / 256.0
        table[row, 32:48] = np.cos(angle)
        table[row, 48:64] = -np.sin(angle)
        table[row, 64:80] = np.sin(angle)
        table[row, 80:96] = np.cos(angle)
    return table


def after(values, axis):
    return pltpu.roll(values, values.shape[axis] - 1, axis)


def before(values, axis):
    return pltpu.roll(values, 1, axis)


def face_terms(speed, wet):
    celerity = jnp.sqrt(speed)
    terms = []
    for axis in (1, 0):
        opened = wet * after(wet, axis)
        terms.append((0.5 * opened, opened * (0.25 * (celerity + after(celerity, axis)))))
    return terms


def advance(surface, along_x, along_y, speed, wet, terms):
    pressure = speed * surface
    changes = []
    for axis, along, across in ((1, along_x, along_y), (0, along_y, along_x)):
        half, damp = terms[1 - axis]
        next_along = after(along, axis)
        mass = half * (along + next_along) - damp * (after(surface, axis) - surface)
        push = half * (pressure + after(pressure, axis)) - damp * (next_along - along)
        shear = damp * (across - after(across, axis))
        changes.append(tuple(flux - before(flux, axis) for flux in (mass, push, shear)))
    (mass_x, push_x, shear_x), (mass_y, push_y, shear_y) = changes
    return (
        wet * (surface - 0.25 * (mass_x + mass_y)),
        wet * (along_x - 0.25 * (push_x + shear_y)),
        wet * (along_y - 0.25 * (shear_x + push_y)),
    )


def kernel(
    kern, coef, speed, mask, cells, surf, flow_x, flow_y, table,
    series_o, surf_o, flow_x_o, flow_y_o,
    kbuf, tab, cbuf, mbuf, cellbuf, left, own, dsend, drecv, ysend, yrecv,
    xsend, xrecv, zsend, zrecv, gsend, grecv, fields, ewsend, ewrecv, onehot, latest,
    ksem, lsem, dsem, ysem, xsem, zsem, gssem, grsem, nssem, ewsem,
):
    row, col = lax.axis_index("rows"), lax.axis_index("cols")
    x, z_lo = row % 4, row // 4
    y, z_hi, core = col // 4, (col // 2) % 2, col % 2
    z = z_hi * 4 + z_lo
    is_edge = row == 15

    def place(at_x, at_y, at_z, at_core):
        return ((at_z % 4) * 4 + at_x, at_y * 4 + (at_z // 4) * 2 + at_core)

    partner = place(x, y, z, 1 - core)
    y_peer = [place(x, (y + d) % 4, z, core) for d in range(4)]
    x_peer = [place((x + d) % 4, y, z, core) for d in range(4)]
    z_peer = [place(x, y, (z + d) % 8, core) for d in range(8)]
    north, south = ((row + 15) % 16, col), ((row + 1) % 16, col)
    west, east = (row, (col + 15) % 16), (row, (col + 1) % 16)

    with jax.named_scope("greet_peers"):
        barrier = pltpu.get_barrier_semaphore()
        for peer in [partner, *y_peer[1:], *x_peer[1:], *z_peer[1:], north, south, west, east]:
            pl.semaphore_signal(barrier, inc=1, device_id=peer, device_id_type=MESH)

        @pl.when(is_edge)
        def _():
            def greet(index, carry):
                at_z, at_col = index // 8, index % 8
                peer = place(3, at_col // 2, at_z, at_col % 2)

                @pl.when((peer[0] != row) | (peer[1] != col))
                def _():
                    pl.semaphore_signal(barrier, inc=1, device_id=peer, device_id_type=MESH)

                return carry

            lax.fori_loop(0, 64, greet, 0)

    with jax.named_scope("start_loads"):
        local = [
            pltpu.make_async_copy(table.at[row], tab, lsem.at[0]),
            pltpu.make_async_copy(coef, cbuf, lsem.at[1]),
        ]
        for copy in local:
            copy.start()
        loads = []
        for i, d in enumerate(ORDER):
            for side, par in enumerate((1 - core, core)):
                for part in range(2):
                    slot = i * 4 + side * 2 + part
                    start = pl.multiple_of(((((y + d) % 4) * 2 + part) * 2 + par) * 256, 256)
                    copy = pltpu.make_async_copy(
                        kern.at[:, pl.ds(start, 256)], kbuf.at[slot], ksem.at[slot]
                    )
                    copy.start()
                    loads.append(copy)
        inner = (pl.ds(8, 256), pl.ds(0, 256))
        grids = [
            pltpu.make_async_copy(ref, fields.at[(j, *inner)], lsem.at[2 + j])
            for j, ref in enumerate((surf, flow_x, flow_y, speed))
        ]
        grids += [
            pltpu.make_async_copy(mask, mbuf, lsem.at[6]),
            pltpu.make_async_copy(cells, cellbuf, lsem.at[7]),
        ]
        for copy in grids:
            copy.start()

    with jax.named_scope("build_left"):
        for copy in local:
            copy.wait()
        tables = tab[...]
        coefs = lax.dot_general(
            tables[32:96], cbuf[...], (((1,), (1,)), ((), ())),
            precision=HIGH, preferred_element_type=F32,
        )
        lanes = lax.broadcasted_iota(jnp.int32, (32, 512), 1)
        subs = lax.broadcasted_iota(jnp.int32, (32, 512), 0)
        spread = (lanes % 32 == subs).astype(F32).astype(BF16)
        tiled = jnp.dot(coefs.astype(BF16), spread, preferred_element_type=F32)
        diagonal = lanes // 32 == subs % 16
        left[:, 0:512] = jnp.where(diagonal, tiled[0:32], 0.0).astype(BF16)
        left[:, 512:1024] = jnp.where(diagonal, tiled[32:64], 0.0).astype(BF16)

        dcopy, ycopy = [], {}

        def merge(i):
            d = ORDER[i]
            dcopy[i].wait_recv()
            total = own[i] + drecv[i]
            if d == 0:
                own[i] = total
                return
            ysend[d - 1] = total
            ycopy[d] = pltpu.make_async_remote_copy(
                src_ref=ysend.at[d - 1], dst_ref=yrecv.at[d - 1],
                send_sem=ysem.at[0, d - 1], recv_sem=ysem.at[1, d - 1],
                device_id=y_peer[d], device_id_type=MESH,
            )
            ycopy[d].start()

    with jax.named_scope("spectrum"):
        for i in range(4):
            for side in range(2):
                for part in range(2):
                    slot = i * 4 + side * 2 + part
                    loads[slot].wait()
                    spec = jnp.dot(left[...], kbuf[slot], preferred_element_type=F32)
                    target = own if side else dsend
                    target[i, :, part * 256 : part * 256 + 256] = spec
                if side == 0:
                    if i == 0:
                        pl.semaphore_wait(
                            barrier, 18 + jnp.where(x == 3, 16 - is_edge.astype(jnp.int32), 0)
                        )
                    copy = pltpu.make_async_remote_copy(
                        src_ref=dsend.at[i], dst_ref=drecv.at[i],
                        send_sem=dsem.at[0, i], recv_sem=dsem.at[1, i],
                        device_id=partner, device_id_type=MESH,
                    )
                    copy.start()
                    dcopy.append(copy)
            if i >= 1:
                merge(i - 1)

    with jax.named_scope("row_halos"):
        for copy in grids:
            copy.wait()
        fields[(4, *inner)] = mbuf[...].astype(F32)
        ns_copies = []
        for at, (first, last, peer) in enumerate(((8, 264, north), (256, 0, south))):
            copy = pltpu.make_async_remote_copy(
                src_ref=fields.at[:, pl.ds(first, 8), pl.ds(0, 256)],
                dst_ref=fields.at[:, pl.ds(last, 8), pl.ds(0, 256)],
                send_sem=nssem.at[0, at], recv_sem=nssem.at[1, at],
                device_id=peer, device_id_type=MESH,
            )
            copy.start()
            ns_copies.append(copy)
        merge(3)

    with jax.named_scope("selection"):
        def select(block, carry):
            at = lax.broadcasted_iota(jnp.int32, (384, 128), 0)
            column = col * 256 + jnp.where(at >= 320, at - 384, at)
            found = cellbuf[pl.ds(block, 1), :] == column
            onehot[:, pl.ds(pl.multiple_of(block * 128, 128), 128)] = jnp.where(
                found, 1.0, 0.0
            ).astype(BF16)
            return carry

        @pl.when(is_edge)
        def _():
            lax.fori_loop(0, 32, select, 0)

    with jax.named_scope("column_halos"):
        for copy in ns_copies:
            copy.wait_recv()

        @pl.when(row == 0)
        def _():
            fields[:, 0:8, 0:256] = jnp.zeros((5, 8, 256), F32)

        @pl.when(is_edge)
        def _():
            fields[:, 264:272, 0:256] = jnp.zeros((5, 8, 256), F32)

        lane = lax.broadcasted_iota(jnp.int32, (272, 128), 1)
        ew_copies = []
        for at, (first, shift, peer) in enumerate(((0, 0, west), (128, 2, east))):
            packed = jnp.zeros((272, 128), F32)
            for j in range(5):
                block = fields[j, :, first : first + 128]
                if 2 * j + shift:
                    block = pltpu.roll(block, 2 * j + shift, 1)
                packed = jnp.where(lane // 2 == j, block, packed)
            packed = jnp.concatenate([packed, jnp.zeros((112, 128), F32)], axis=0)
            ewsend[at] = packed.T[0:16]
            copy = pltpu.make_async_remote_copy(
                src_ref=ewsend.at[at], dst_ref=ewrecv.at[at],
                send_sem=ewsem.at[0, at], recv_sem=ewsem.at[1, at],
                device_id=peer, device_id_type=MESH,
            )
            copy.start()
            ew_copies.append(copy)

    with jax.named_scope("sum_y"):
        total = own[3]
        for d in (1, 3, 2):
            ycopy[d].wait_recv()
            total = total + yrecv[d - 1]
        inverse = tables.T[:, 0:32]
        partial = jnp.dot(inverse, total, precision=HIGH, preferred_element_type=F32)
        for at in range(4):
            xsend[at] = partial[at * 32 : at * 32 + 32]
        xcopy = {}
        for d in (2, 1, 3):
            xcopy[d] = pltpu.make_async_remote_copy(
                src_ref=xsend.at[(x + d) % 4], dst_ref=xrecv.at[d - 1],
                send_sem=xsem.at[0, d - 1], recv_sem=xsem.at[1, d - 1],
                device_id=x_peer[d], device_id_type=MESH,
            )
            xcopy[d].start()

    with jax.named_scope("place_halos"):
        for copy in ew_copies:
            copy.wait_recv()
        sides = []
        for at, end in ((0, 15), (1, 0)):
            message = jnp.where(col == end, 0.0, ewrecv[at])
            padded = jnp.concatenate([message, jnp.zeros((112, 384), F32)], axis=0)
            sides.append(padded.T[0:272])
        for j in range(5):
            right = pltpu.roll(sides[0], 128 - 2 * j, 1) if j else sides[0]
            wrapped = pltpu.roll(sides[1], 126 - 2 * j, 1)
            fields[j, :, 256:384] = jnp.where(
                lane < 2, right, jnp.where(lane >= 126, wrapped, 0.0)
            )

    with jax.named_scope("sum_x"):
        total = xsend[x]
        for d in (1, 3, 2):
            xcopy[d].wait_recv()
            total = total + xrecv[d - 1]
        zsend[0] = total[:, 0:256]
        zsend[1] = total[:, 256:512]
        gsend[...] = total[30:32]
        me = z * 8 + y * 2 + core

        def ghost_copy(index):
            return pltpu.make_async_remote_copy(
                src_ref=gsend, dst_ref=grecv.at[me],
                send_sem=gssem.at[index], recv_sem=grsem,
                device_id=(15, index), device_id_type=MESH,
            )

        @pl.when(x == 3)
        def _():
            def send(index, carry):
                @pl.when((row != 15) | (index != col))
                def _():
                    ghost_copy(index).start()

                return carry

            lax.fori_loop(0, 16, send, 0)

        zcopy = {}
        for d in (4, 3, 5, 2, 6, 1, 7):
            to = (z + d) % 8
            zcopy[d] = pltpu.make_async_remote_copy(
                src_ref=zsend.at[to // 4, pl.ds(pl.multiple_of((to % 4) * 8, 8), 8)],
                dst_ref=zrecv.at[d - 1],
                send_sem=zsem.at[0, d - 1], recv_sem=zsem.at[1, d - 1],
                device_id=z_peer[d], device_id_type=MESH,
            )
            zcopy[d].start()

    with jax.named_scope("water"):
        def strip(at, carry):
            base = pl.multiple_of(at * 32, 8)
            state = [fields[j, pl.ds(base, 48), :] for j in range(5)]
            values, rest = state[0:3], state[3:5]
            terms = face_terms(*rest)
            for _ in range(2):
                values = advance(*values, *rest, terms)
            for ref, value in zip((surf_o, flow_x_o, flow_y_o), values):
                ref[pl.ds(base, 32), :] = value[8:40, 0:256]
            return carry

        lax.fori_loop(0, 8, strip, 0)

    with jax.named_scope("sum_z"):
        total = zsend[z_hi, pl.ds(pl.multiple_of(z_lo * 8, 8), 8)]
        for d in range(1, 8):
            zcopy[d].wait_recv()
            total = total + zrecv[d - 1]
        series_o[...] = total

    with jax.named_scope("ghost"):
        @pl.when(is_edge)
        def _():
            grecv[me] = gsend[...]
            pltpu.make_async_copy(grecv.at[pl.ds(0, 63)], grecv.at[pl.ds(0, 63)], grsem).wait()
            latest[...] = jnp.zeros((8, 4096), F32)
            for at in range(8):
                summed = grecv[at]
                for other in range(1, 8):
                    summed = summed + grecv[other * 8 + at]
                for part in range(2):
                    first = ((at // 2 * 2 + part) * 2 + at % 2) * 256
                    latest[0:2, first : first + 256] = summed[:, part * 256 : part * 256 + 256]
            value = latest[...]
            high = value.astype(BF16)
            value = value - high.astype(F32)
            middle = value.astype(BF16)
            low = (value - middle.astype(F32)).astype(BF16)
            ghost = jnp.zeros((8, 384), F32)
            for piece in (low, middle, high):
                ghost = ghost + lax.dot_general(
                    piece, onehot[...], (((1,), (1,)), ((), ())), preferred_element_type=F32
                )
            beyond = lax.broadcasted_iota(jnp.int32, (24, 384), 0) == 16
            state = [fields[j, 248:272, :] for j in range(5)]
            rest = [jnp.where(beyond, 1.0, value) for value in state[3:5]]
            values = state[0:3]
            terms = face_terms(*rest)
            for step in range(2):
                values = [
                    jnp.where(beyond, ghost[step : step + 1], values[0]),
                    jnp.where(beyond, 0.0, values[1]),
                    jnp.where(beyond, 0.0, values[2]),
                ]
                values = advance(*values, *rest, terms)
            for ref, value in zip((surf_o, flow_x_o, flow_y_o), values):
                ref[248:256, :] = value[8:16, 0:256]

    with jax.named_scope("drain"):
        for copy in [*dcopy, *ycopy.values(), *xcopy.values(), *zcopy.values(), *ns_copies, *ew_copies]:
            copy.wait_send()

        @pl.when(x == 3)
        def _():
            def finish(index, carry):
                @pl.when((row != 15) | (index != col))
                def _():
                    ghost_copy(index).wait_send()

                return carry

            lax.fori_loop(0, 16, finish, 0)


def write_out(*refs):
    sources, targets, sems = refs[0:4], refs[4:8], refs[8]
    copies = [
        pltpu.make_async_copy(source, target, sems.at[j])
        for j, (source, target) in enumerate(zip(sources, targets))
    ]
    for copy in copies:
        copy.start()
    for copy in copies:
        copy.wait()


def on_device(
    kernel_hat, coefficients, wave_speed_sq, wet_mask, boundary_cell, height, flux_x, flux_y
):
    field = jax.ShapeDtypeStruct((256, 256), F32)
    dma = pltpu.SemaphoreType.DMA
    shapes = (jax.ShapeDtypeStruct((8, 256), F32), field, field, field)
    operands = [
        pltpu.with_memory_space_constraint(value, pltpu.MemorySpace.HBM)
        for value in (
            kernel_hat.reshape(1024, 4096),
            coefficients.T,
            wave_speed_sq,
            wet_mask,
            boundary_cell.reshape(32, 128),
            height,
            flux_x,
            flux_y,
            jnp.asarray(transform_tables()),
        )
    ]
    results = pl.pallas_call(
        kernel,
        out_shape=shapes,
        in_specs=[pl.BlockSpec(memory_space=pltpu.MemorySpace.HBM)] * 9,
        out_specs=[pl.BlockSpec(memory_space=pltpu.VMEM)] * 4,
        scratch_shapes=[
            pltpu.VMEM((16, 1024, 256), BF16),
            pltpu.VMEM((128, 128), F32),
            pltpu.VMEM((32, 128), F32),
            pltpu.VMEM((256, 256), jnp.int32),
            pltpu.VMEM((32, 128), jnp.int32),
            pltpu.VMEM((32, 1024), BF16),
            pltpu.VMEM((4, 32, 512), F32),
            pltpu.VMEM((4, 32, 512), F32),
            pltpu.VMEM((4, 32, 512), F32),
            pltpu.VMEM((3, 32, 512), F32),
            pltpu.VMEM((3, 32, 512), F32),
            pltpu.VMEM((4, 32, 512), F32),
            pltpu.VMEM((3, 32, 512), F32),
            pltpu.VMEM((2, 32, 256), F32),
            pltpu.VMEM((7, 8, 256), F32),
            pltpu.VMEM((2, 512), F32),
            pltpu.VMEM((64, 2, 512), F32),
            pltpu.VMEM((5, 272, 384), F32),
            pltpu.VMEM((2, 16, 384), F32),
            pltpu.VMEM((2, 16, 384), F32),
            pltpu.VMEM((384, 4096), BF16),
            pltpu.VMEM((8, 4096), F32),
            dma((16,)),
            dma((8,)),
            dma((2, 4)),
            dma((2, 3)),
            dma((2, 3)),
            dma((2, 7)),
            dma((16,)),
            dma(()),
            dma((2, 2)),
            dma((2, 2)),
        ],
        compiler_params=pltpu.CompilerParams(
            collective_id=0, has_side_effects=True, vmem_limit_bytes=48 * 1024 * 1024
        ),
    )(*operands)
    return pl.pallas_call(
        write_out,
        out_shape=shapes,
        in_specs=[pl.BlockSpec(memory_space=pltpu.VMEM)] * 4,
        out_specs=[pl.BlockSpec(memory_space=pltpu.MemorySpace.HBM)] * 4,
        scratch_shapes=[dma((4,))],
        compiler_params=pltpu.CompilerParams(vmem_limit_bytes=16 * 1024 * 1024),
    )(*results)


def solution(mesh):
    return jax.shard_map(
        on_device,
        mesh=mesh,
        in_specs=(
            P(None, "rows", "cols", None),
            P(None, "cols"),
            P("rows", "cols"),
            P("rows", "cols"),
            P(),
            P("rows", "cols"),
            P("rows", "cols"),
            P("rows", "cols"),
        ),
        out_specs=(P("rows", "cols"), P("rows", "cols"), P("rows", "cols"), P("rows", "cols")),
        check_vma=False,
    )
```

```python
import functools

import jax
import jax.numpy as jnp
import numpy as np
from jax import lax
from jax.experimental import pallas as pl
from jax.experimental.pallas import tpu as pltpu
from jax.sharding import PartitionSpec as P

F32 = jnp.float32
BF16 = jnp.bfloat16
HIGH = lax.Precision.HIGHEST
MESH = pl.DeviceIdType.MESH
ORDER = (2, 1, 3, 0)
LOADS = (0, 1, 4, 5, 2, 3, 8, 9, 6, 7, 12, 13, 10, 11, 14, 15)


def transform_tables():
    table = np.zeros((16, 128, 128), np.float32)
    times = np.arange(128)
    inner = times.reshape(4, 4, 8).transpose(1, 0, 2).reshape(-1)
    for row in range(16):
        freqs = row * 16 + np.arange(16)
        angle = 2.0 * np.pi * ((freqs[:, None] * inner[None, :]) % 256) / 256.0
        table[row, 0:16] = np.cos(angle) / 256.0
        table[row, 16:32] = -np.sin(angle) / 256.0
        angle = 2.0 * np.pi * ((freqs[:, None] * times[None, :]) % 256) / 256.0
        table[row, 32:48] = np.cos(angle)
        table[row, 48:64] = -np.sin(angle)
        table[row, 64:80] = np.sin(angle)
        table[row, 80:96] = np.cos(angle)
    return table


def after(values, axis):
    return pltpu.roll(values, values.shape[axis] - 1, axis)


def before(values, axis):
    return pltpu.roll(values, 1, axis)


def split_rows(value):
    high = value.astype(BF16)
    value = value - high.astype(F32)
    middle = value.astype(BF16)
    return [high, middle, (value - middle.astype(F32)).astype(BF16)]


def face_terms(speed, wet):
    celerity = jnp.sqrt(speed)
    terms = []
    for axis in (1, 0):
        opened = wet * after(wet, axis)
        terms.append((0.5 * opened, opened * (0.25 * (celerity + after(celerity, axis)))))
    return terms


def advance(surface, along_x, along_y, speed, wet, terms):
    pressure = speed * surface
    changes = []
    for axis, along, across in ((1, along_x, along_y), (0, along_y, along_x)):
        half, damp = terms[1 - axis]
        next_along = after(along, axis)
        mass = half * (along + next_along) - damp * (after(surface, axis) - surface)
        push = half * (pressure + after(pressure, axis)) - damp * (next_along - along)
        shear = damp * (across - after(across, axis))
        changes.append(tuple(flux - before(flux, axis) for flux in (mass, push, shear)))
    (mass_x, push_x, shear_x), (mass_y, push_y, shear_y) = changes
    return (
        wet * (surface - 0.25 * (mass_x + mass_y)),
        wet * (along_x - 0.25 * (push_x + shear_y)),
        wet * (along_y - 0.25 * (shear_x + push_y)),
    )


def kernel(
    kern, coef, speed, mask, cells, surf, flow_x, flow_y, table,
    series_o, surf_o, flow_x_o, flow_y_o,
    kbuf, tab, cbuf, mbuf, cellbuf, left, own, dsend, drecv, ysend, yrecv,
    xsend, xrecv, zsend, zrecv, gsend, grecv, fields, ewsend, ewrecv, onehot, blocks, wide,
    ksem, lsem, dsem, ysem, xsem, zsem, gssem, grsem, nssem, ewsem,
):
    row, col = lax.axis_index("rows"), lax.axis_index("cols")
    x, z_lo = row % 4, row // 4
    y, z_hi, core = col // 4, (col // 2) % 2, col % 2
    z = z_hi * 4 + z_lo
    is_edge = row == 15

    def place(at_x, at_y, at_z, at_core):
        return ((at_z % 4) * 4 + at_x, at_y * 4 + (at_z // 4) * 2 + at_core)

    partner = place(x, y, z, 1 - core)
    y_peer = [place(x, (y + d) % 4, z, core) for d in range(4)]
    x_peer = [place((x + d) % 4, y, z, core) for d in range(4)]
    z_peer = [place(x, y, (z + d) % 8, core) for d in range(8)]
    north, south = ((row + 15) % 16, col), ((row + 1) % 16, col)
    west, east = (row, (col + 15) % 16), (row, (col + 1) % 16)

    with jax.named_scope("start_loads"):
        local = [pltpu.make_async_copy(table.at[row], tab, lsem.at[0])]
        local[0].start()
        for i in range(16):
            pltpu.make_async_copy(coef, cbuf.at[pl.ds(i * 32, 32)], lsem.at[1]).start()
        local.append(pltpu.make_async_copy(cbuf, cbuf, lsem.at[1]))
        loads = []
        for i, d in enumerate(ORDER):
            for side, par in enumerate((1 - core, core)):
                for part in range(2):
                    slot = i * 4 + side * 2 + part
                    start = pl.multiple_of(((((y + d) % 4) * 2 + part) * 2 + par) * 256, 256)
                    loads.append(
                        pltpu.make_async_copy(
                            kern.at[:, pl.ds(start, 256)], kbuf.at[slot], ksem.at[slot]
                        )
                    )
        for slot in LOADS:
            loads[slot].start()
        inner = (pl.ds(8, 256), pl.ds(0, 256))
        grids = [
            pltpu.make_async_copy(ref, fields.at[(j, *inner)], lsem.at[2 + j])
            for j, ref in enumerate((surf, flow_x, flow_y, speed))
        ]
        grids += [
            pltpu.make_async_copy(mask, mbuf, lsem.at[6]),
            pltpu.make_async_copy(cells, cellbuf, lsem.at[7]),
        ]
        for copy in grids:
            copy.start()

    with jax.named_scope("greet_peers"):
        barrier = pltpu.get_barrier_semaphore()
        for peer in [partner, *y_peer[1:], *x_peer[1:], *z_peer[1:], north, south, west, east]:
            pl.semaphore_signal(barrier, inc=1, device_id=peer, device_id_type=MESH)

        @pl.when(is_edge)
        def _():
            for at_row in (3, 7, 11, 15):
                for at_col in range(16):
                    def greet(peer=(at_row, at_col)):
                        pl.semaphore_signal(barrier, inc=1, device_id=peer, device_id_type=MESH)

                    if at_row == 15:
                        pl.when(col != at_col)(greet)
                    else:
                        greet()

    with jax.named_scope("build_left"):
        for copy in local:
            copy.wait()
        tables = tab[...]
        tiled = lax.dot_general(
            tables[32:96], cbuf[...], (((1,), (1,)), ((), ())),
            precision=HIGH, preferred_element_type=F32,
        )
        lanes = lax.broadcasted_iota(jnp.int32, (32, 512), 1)
        subs = lax.broadcasted_iota(jnp.int32, (32, 512), 0)
        diagonal = (lanes >> 5) == (subs & 15)
        left[:, 0:512] = jnp.where(diagonal, tiled[0:32], 0.0).astype(BF16)
        left[:, 512:1024] = jnp.where(diagonal, tiled[32:64], 0.0).astype(BF16)

        dcopy, ycopy = [], {}

        def part_of(i, side, target):
            for part in range(2):
                slot = i * 4 + side * 2 + part
                loads[slot].wait()
                target[i, :, part * 256 : part * 256 + 256] = jnp.dot(
                    left[...], kbuf[slot], preferred_element_type=F32
                )

        def other(i):
            part_of(i, 0, dsend)
            if i == 0:
                pl.semaphore_wait(
                    barrier, 18 + jnp.where(x == 3, 16 - is_edge.astype(jnp.int32), 0)
                )
            copy = pltpu.make_async_remote_copy(
                src_ref=dsend.at[i], dst_ref=drecv.at[i],
                send_sem=dsem.at[0, i], recv_sem=dsem.at[1, i],
                device_id=partner, device_id_type=MESH,
            )
            copy.start()
            dcopy.append(copy)

        def mine(i):
            part_of(i, 1, own)

        def merge(i):
            d = ORDER[i]
            dcopy[i].wait_recv()
            total = own[i] + drecv[i]
            if d == 0:
                own[i] = total
                return
            ysend[d - 1] = total
            ycopy[d] = pltpu.make_async_remote_copy(
                src_ref=ysend.at[d - 1], dst_ref=yrecv.at[d - 1],
                send_sem=ysem.at[0, d - 1], recv_sem=ysem.at[1, d - 1],
                device_id=y_peer[d], device_id_type=MESH,
            )
            ycopy[d].start()

    with jax.named_scope("spectrum"):
        other(0)
        other(1)
        mine(0)
        other(2)
        mine(1)
        merge(0)
        other(3)
        mine(2)
        merge(1)
        mine(3)
        merge(2)

    with jax.named_scope("row_halos"):
        for copy in grids:
            copy.wait()
        fields[(4, *inner)] = mbuf[...].astype(F32)
        ns_copies = []
        for at, (first, last, peer) in enumerate(((8, 264, north), (256, 0, south))):
            copy = pltpu.make_async_remote_copy(
                src_ref=fields.at[:, pl.ds(first, 8), pl.ds(0, 256)],
                dst_ref=fields.at[:, pl.ds(last, 8), pl.ds(0, 256)],
                send_sem=nssem.at[0, at], recv_sem=nssem.at[1, at],
                device_id=peer, device_id_type=MESH,
            )
            copy.start()
            ns_copies.append(copy)
        split = split_rows(tables[0:32])
        wide[...] = jnp.concatenate(
            [*(split[k].astype(F32) for k in (0, 0, 1, 0, 2, 1)), jnp.zeros((64, 128), F32)], axis=0
        ).T.astype(BF16)
        merge(3)

    with jax.named_scope("sum_y"):
        total = own[3]
        for d in (1, 3, 2):
            ycopy[d].wait_recv()
            total = total + yrecv[d - 1]
        split = split_rows(total)
        stack = jnp.concatenate([split[k] for k in (0, 1, 0, 2, 0, 1)], axis=0)
        partial = jnp.dot(wide[:, 0:192], stack, preferred_element_type=F32)
        for at in range(4):
            xsend[at] = partial[at * 32 : at * 32 + 32]
        xcopy = {}
        for d in (2, 1, 3):
            xcopy[d] = pltpu.make_async_remote_copy(
                src_ref=xsend.at[(x + d) % 4], dst_ref=xrecv.at[d - 1],
                send_sem=xsem.at[0, d - 1], recv_sem=xsem.at[1, d - 1],
                device_id=x_peer[d], device_id_type=MESH,
            )
            xcopy[d].start()

    with jax.named_scope("column_halos"):
        for copy in ns_copies:
            copy.wait_recv()

        @pl.when(row == 0)
        def _():
            fields[:, 0:8, 0:256] = jnp.zeros((5, 8, 256), F32)

        @pl.when(is_edge)
        def _():
            fields[:, 264:272, 0:256] = jnp.zeros((5, 8, 256), F32)

        lane = lax.broadcasted_iota(jnp.int32, (272, 128), 1)
        ew_copies = []
        for at, (first, shift, peer) in enumerate(((0, 0, west), (128, 2, east))):
            packed = jnp.zeros((272, 128), F32)
            for j in range(5):
                block = fields[j, :, first : first + 128]
                if 2 * j + shift:
                    block = pltpu.roll(block, 2 * j + shift, 1)
                packed = jnp.where(lane // 2 == j, block, packed)
            packed = jnp.concatenate([packed, jnp.zeros((112, 128), F32)], axis=0)
            ewsend[at] = packed.T[0:16]
            copy = pltpu.make_async_remote_copy(
                src_ref=ewsend.at[at], dst_ref=ewrecv.at[at],
                send_sem=ewsem.at[0, at], recv_sem=ewsem.at[1, at],
                device_id=peer, device_id_type=MESH,
            )
            copy.start()
            ew_copies.append(copy)

    with jax.named_scope("selection"):
        @pl.when(is_edge)
        def _():
            at = lax.broadcasted_iota(jnp.int32, (128, 384), 1)
            column = col * 256 + jnp.where(at >= 320, at - 384, at)
            turned = jnp.concatenate(
                [cellbuf[...].astype(F32), jnp.zeros((96, 128), F32)], axis=0
            ).T.astype(jnp.int32)
            found = jnp.zeros((128, 384), F32)
            for block in range(32):
                found = jnp.where(turned[:, block : block + 1] == column, block + 1.0, found)
            onehot[...] = jnp.where(found > 0.0, 1.0, 0.0).astype(BF16)
            blocks[...] = jnp.broadcast_to(jnp.sum(found, axis=0, keepdims=True), (8, 384))

    with jax.named_scope("sum_x"):
        total = xsend[x]
        for d in (1, 3, 2):
            xcopy[d].wait_recv()
            total = total + xrecv[d - 1]
        zsend[0] = total[:, 0:256]
        zsend[1] = total[:, 256:512]
        for at in range(8):
            gsend[at : at + 1] = total[30 + at // 4 : 31 + at // 4, at % 4 * 128 : at % 4 * 128 + 128]
        here = pl.ds(pl.multiple_of((z * 8 + y * 2 + core) * 8, 8), 8)

        def ghost_copy(index):
            return pltpu.make_async_remote_copy(
                src_ref=gsend, dst_ref=grecv.at[here],
                send_sem=gssem.at[index], recv_sem=grsem,
                device_id=(15, index), device_id_type=MESH,
            )

        @pl.when(x == 3)
        def _():
            for index in range(16):
                pl.when((row != 15) | (col != index))(ghost_copy(index).start)

        zcopy = {}
        for d in (4, 3, 5, 2, 6, 1, 7):
            to = (z + d) % 8
            zcopy[d] = pltpu.make_async_remote_copy(
                src_ref=zsend.at[to // 4, pl.ds(pl.multiple_of((to % 4) * 8, 8), 8)],
                dst_ref=zrecv.at[d - 1],
                send_sem=zsem.at[0, d - 1], recv_sem=zsem.at[1, d - 1],
                device_id=z_peer[d], device_id_type=MESH,
            )
            zcopy[d].start()

    with jax.named_scope("place_halos"):
        for copy in ew_copies:
            copy.wait_recv()
        sides = []
        for at, end in ((0, 15), (1, 0)):
            message = jnp.where(col == end, 0.0, ewrecv[at])
            padded = jnp.concatenate([message, jnp.zeros((112, 384), F32)], axis=0)
            sides.append(padded.T[0:272])
        for j in range(5):
            right = pltpu.roll(sides[0], 128 - 2 * j, 1) if j else sides[0]
            wrapped = pltpu.roll(sides[1], 126 - 2 * j, 1)
            fields[j, :, 256:384] = jnp.where(
                lane < 2, right, jnp.where(lane >= 126, wrapped, 0.0)
            )

    with jax.named_scope("water"):
        def strip(at, carry):
            base = pl.multiple_of(at * 32, 8)
            state = [fields[j, pl.ds(base, 48), :] for j in range(5)]
            values, rest = state[0:3], state[3:5]
            terms = face_terms(*rest)
            for _ in range(2):
                values = advance(*values, *rest, terms)
            for ref, value in zip((surf_o, flow_x_o, flow_y_o), values):
                ref[pl.ds(base, 32), :] = value[8:40, 0:256]
            return carry

        lax.fori_loop(0, 8, strip, 0)

    with jax.named_scope("sum_z"):
        total = zsend[z_hi, pl.ds(pl.multiple_of(z_lo * 8, 8), 8)]
        for d in range(1, 8):
            zcopy[d].wait_recv()
            total = total + zrecv[d - 1]
        series_o[...] = total

    with jax.named_scope("ghost"):
        @pl.when(is_edge)
        def _():
            grecv[here] = gsend[...]
            pltpu.make_async_copy(
                grecv.at[pl.ds(0, 504)], grecv.at[pl.ds(0, 504)], grsem
            ).wait()
            value = grecv[0:64]
            for other_z in range(1, 8):
                value = value + grecv[other_z * 64 : other_z * 64 + 64]
            picked = jnp.dot(
                jnp.concatenate(split_rows(value), axis=0), onehot[...],
                preferred_element_type=F32,
            )
            picked = picked[128:192] + picked[64:128] + picked[0:64]
            at = lax.broadcasted_iota(jnp.int32, (64, 384), 0)
            block = (at >> 4) * 8 + (at & 2) * 2 + ((at >> 3) & 1) * 2 + (at & 1)
            picked = jnp.where((block + 1).astype(F32) == blocks[0:1], picked, 0.0)
            ghost = [
                jnp.sum(jnp.where(((at >> 2) & 1) == step, picked, 0.0), axis=0, keepdims=True)
                for step in range(2)
            ]
            beyond = lax.broadcasted_iota(jnp.int32, (24, 384), 0) == 16
            state = [fields[j, 248:272, :] for j in range(5)]
            rest = [jnp.where(beyond, 1.0, value) for value in state[3:5]]
            values = state[0:3]
            terms = face_terms(*rest)
            for step in range(2):
                values = [
                    jnp.where(beyond, ghost[step], values[0]),
                    jnp.where(beyond, 0.0, values[1]),
                    jnp.where(beyond, 0.0, values[2]),
                ]
                values = advance(*values, *rest, terms)
            for ref, value in zip((surf_o, flow_x_o, flow_y_o), values):
                ref[248:256, :] = value[8:16, 0:256]

    with jax.named_scope("drain"):
        for copy in [*dcopy, *ycopy.values(), *xcopy.values(), *zcopy.values(), *ns_copies, *ew_copies]:
            copy.wait_send()

        @pl.when(x == 3)
        def _():
            for index in range(16):
                pl.when((row != 15) | (col != index))(ghost_copy(index).wait_send)


def write_out(*refs):
    sources, targets, sems = refs[0:4], refs[4:8], refs[8]
    copies = [
        pltpu.make_async_copy(source, target, sems.at[j])
        for j, (source, target) in enumerate(zip(sources, targets))
    ]
    for copy in copies:
        copy.start()
    for copy in copies:
        copy.wait()


def on_device(
    kernel_hat, coefficients, wave_speed_sq, wet_mask, boundary_cell, height, flux_x, flux_y
):
    field = jax.ShapeDtypeStruct((256, 256), F32)
    dma = pltpu.SemaphoreType.DMA
    shapes = (jax.ShapeDtypeStruct((8, 256), F32), field, field, field)
    operands = [
        pltpu.with_memory_space_constraint(value, pltpu.MemorySpace.HBM)
        for value in (
            kernel_hat.reshape(1024, 4096),
            coefficients.T,
            wave_speed_sq,
            wet_mask,
            boundary_cell.reshape(32, 128),
            height,
            flux_x,
            flux_y,
            jnp.asarray(transform_tables()),
        )
    ]
    results = pl.pallas_call(
        kernel,
        out_shape=shapes,
        in_specs=[pl.BlockSpec(memory_space=pltpu.MemorySpace.HBM)] * 9,
        out_specs=[pl.BlockSpec(memory_space=pltpu.VMEM)] * 4,
        scratch_shapes=[
            pltpu.VMEM((16, 1024, 256), BF16),
            pltpu.VMEM((128, 128), F32),
            pltpu.VMEM((512, 128), F32),
            pltpu.VMEM((256, 256), jnp.int32),
            pltpu.VMEM((32, 128), jnp.int32),
            pltpu.VMEM((32, 1024), BF16),
            pltpu.VMEM((4, 32, 512), F32),
            pltpu.VMEM((4, 32, 512), F32),
            pltpu.VMEM((4, 32, 512), F32),
            pltpu.VMEM((3, 32, 512), F32),
            pltpu.VMEM((3, 32, 512), F32),
            pltpu.VMEM((4, 32, 512), F32),
            pltpu.VMEM((3, 32, 512), F32),
            pltpu.VMEM((2, 32, 256), F32),
            pltpu.VMEM((7, 8, 256), F32),
            pltpu.VMEM((8, 128), F32),
            pltpu.VMEM((512, 128), F32),
            pltpu.VMEM((5, 272, 384), F32),
            pltpu.VMEM((2, 16, 384), F32),
            pltpu.VMEM((2, 16, 384), F32),
            pltpu.VMEM((128, 384), BF16),
            pltpu.VMEM((8, 384), F32),
            pltpu.VMEM((128, 256), BF16),
            dma((16,)),
            dma((8,)),
            dma((2, 4)),
            dma((2, 3)),
            dma((2, 3)),
            dma((2, 7)),
            dma((16,)),
            dma(()),
            dma((2, 2)),
            dma((2, 2)),
        ],
        compiler_params=pltpu.CompilerParams(
            collective_id=0, has_side_effects=True, vmem_limit_bytes=48 * 1024 * 1024
        ),
    )(*operands)
    return pl.pallas_call(
        write_out,
        out_shape=shapes,
        in_specs=[pl.BlockSpec(memory_space=pltpu.VMEM)] * 4,
        out_specs=[pl.BlockSpec(memory_space=pltpu.MemorySpace.HBM)] * 4,
        scratch_shapes=[dma((4,))],
        compiler_params=pltpu.CompilerParams(vmem_limit_bytes=16 * 1024 * 1024),
    )(*results)


def solution(mesh):
    return jax.shard_map(
        on_device,
        mesh=mesh,
        in_specs=(
            P(None, "rows", "cols", None),
            P(None, "cols"),
            P("rows", "cols"),
            P("rows", "cols"),
            P(),
            P("rows", "cols"),
            P("rows", "cols"),
            P("rows", "cols"),
        ),
        out_specs=(P("rows", "cols"), P("rows", "cols"), P("rows", "cols"), P("rows", "cols")),
        check_vma=False,
    )
```

```python
import functools

import jax
import jax.numpy as jnp
import numpy as np
from jax import lax
from jax.experimental import pallas as pl
from jax.experimental.pallas import tpu as pltpu
from jax.sharding import PartitionSpec as P

F32 = jnp.float32
BF16 = jnp.bfloat16
HIGH = lax.Precision.HIGHEST
MESH = pl.DeviceIdType.MESH
ORDER = (2, 1, 3, 0)
LOADS = (0, 1, 4, 5, 2, 3, 8, 9, 6, 7, 12, 13, 10, 11, 14, 15)


def transform_tables():
    table = np.zeros((16, 128, 128), np.float32)
    times = np.arange(128)
    inner = times.reshape(4, 4, 8).transpose(1, 0, 2).reshape(-1)
    for row in range(16):
        freqs = row * 16 + np.arange(16)
        angle = 2.0 * np.pi * ((freqs[:, None] * inner[None, :]) % 256) / 256.0
        table[row, 0:16] = np.cos(angle) / 256.0
        table[row, 16:32] = -np.sin(angle) / 256.0
        angle = 2.0 * np.pi * ((freqs[:, None] * times[None, :]) % 256) / 256.0
        table[row, 32:48] = np.cos(angle)
        table[row, 48:64] = -np.sin(angle)
        table[row, 64:80] = np.sin(angle)
        table[row, 80:96] = np.cos(angle)
    return table


def after(values, axis):
    return pltpu.roll(values, values.shape[axis] - 1, axis)


def before(values, axis):
    return pltpu.roll(values, 1, axis)


def split_rows(value):
    high = value.astype(BF16)
    value = value - high.astype(F32)
    middle = value.astype(BF16)
    return [high, middle, (value - middle.astype(F32)).astype(BF16)]


def face_terms(speed, wet, axes=(1, 0)):
    celerity = jnp.sqrt(speed)
    terms = []
    for axis in axes:
        opened = wet * after(wet, axis)
        terms.append((0.5 * opened, opened * (0.25 * (celerity + after(celerity, axis)))))
    return terms


def advance(surface, along_x, along_y, speed, wet, terms, axes=(1, 0)):
    pressure = speed * surface
    changes = []
    for axis, along, across, (half, damp) in zip(
        axes, (along_x, along_y), (along_y, along_x), terms
    ):
        next_along = after(along, axis)
        mass = half * (along + next_along) - damp * (after(surface, axis) - surface)
        push = half * (pressure + after(pressure, axis)) - damp * (next_along - along)
        shear = damp * (across - after(across, axis))
        changes.append(tuple(flux - before(flux, axis) for flux in (mass, push, shear)))
    (mass_x, push_x, shear_x), (mass_y, push_y, shear_y) = changes
    return (
        wet * (surface - 0.25 * (mass_x + mass_y)),
        wet * (along_x - 0.25 * (push_x + shear_y)),
        wet * (along_y - 0.25 * (shear_x + push_y)),
    )


def kernel(
    kern, coef, speed, mask, cells, surf, flow_x, flow_y, table,
    series_o, surf_o, flow_x_o, flow_y_o,
    kbuf, tab, cbuf, mbuf, cellbuf, left, own, dsend, drecv, ysend, yrecv,
    xsend, xrecv, zsend, zrecv, gsend, grecv, fields, ewsend, ewrecv, sides, tail, onehot, blocks, wide,
    ksem, lsem, dsem, ysem, xsem, zsem, gssem, grsem, nssem, ewsem,
):
    row, col = lax.axis_index("rows"), lax.axis_index("cols")
    x, z_lo = row % 4, row // 4
    y, z_hi, core = col // 4, (col // 2) % 2, col % 2
    z = z_hi * 4 + z_lo
    is_edge = row == 15

    def place(at_x, at_y, at_z, at_core):
        return ((at_z % 4) * 4 + at_x, at_y * 4 + (at_z // 4) * 2 + at_core)

    partner = place(x, y, z, 1 - core)
    y_peer = [place(x, (y + d) % 4, z, core) for d in range(4)]
    x_peer = [place((x + d) % 4, y, z, core) for d in range(4)]
    z_peer = [place(x, y, (z + d) % 8, core) for d in range(8)]
    north, south = ((row + 15) % 16, col), ((row + 1) % 16, col)
    west, east = (row, (col + 15) % 16), (row, (col + 1) % 16)

    with jax.named_scope("start_loads"):
        local = [pltpu.make_async_copy(table.at[row], tab, lsem.at[0])]
        local[0].start()
        local.append(pltpu.make_async_copy(coef, cbuf, lsem.at[1]))
        local[1].start()
        loads = []
        for i, d in enumerate(ORDER):
            for side, par in enumerate((1 - core, core)):
                for part in range(2):
                    slot = i * 4 + side * 2 + part
                    start = pl.multiple_of(((((y + d) % 4) * 2 + part) * 2 + par) * 256, 256)
                    loads.append(
                        pltpu.make_async_copy(
                            kern.at[:, pl.ds(start, 256)], kbuf.at[slot], ksem.at[slot]
                        )
                    )
        for slot in LOADS[0:4]:
            loads[slot].start()
        inner = (pl.ds(8, 256), slice(None))
        grids = [
            pltpu.make_async_copy(ref, fields.at[(j, *inner)], lsem.at[2 + j])
            for j, ref in enumerate((surf, flow_x, flow_y, speed))
        ]
        grids += [
            pltpu.make_async_copy(mask, mbuf, lsem.at[6]),
            pltpu.make_async_copy(cells, cellbuf, lsem.at[7]),
        ]
        for copy in grids:
            copy.start()
        for slot in LOADS[4:]:
            loads[slot].start()

    with jax.named_scope("greet_peers"):
        barrier = pltpu.get_barrier_semaphore()
        for peer in [partner, *y_peer[1:], *x_peer[1:], *z_peer[1:], north, south, west, east]:
            pl.semaphore_signal(barrier, inc=1, device_id=peer, device_id_type=MESH)

        @pl.when(is_edge)
        def _():
            for at_row in (3, 7, 11, 15):
                for at_col in range(16):
                    def greet(peer=(at_row, at_col)):
                        pl.semaphore_signal(barrier, inc=1, device_id=peer, device_id_type=MESH)

                    if at_row == 15:
                        pl.when(col != at_col)(greet)
                    else:
                        greet()

    with jax.named_scope("build_left"):
        for copy in local:
            copy.wait()
        tables = tab[...]
        tiled = lax.dot_general(
            tables[32:96], jnp.concatenate([cbuf[...]] * 16, axis=0), (((1,), (1,)), ((), ())),
            precision=HIGH, preferred_element_type=F32,
        )
        lanes = lax.broadcasted_iota(jnp.int32, (32, 512), 1)
        subs = lax.broadcasted_iota(jnp.int32, (32, 512), 0)
        diagonal = (lanes >> 5) == (subs & 15)
        left[:, 0:512] = jnp.where(diagonal, tiled[0:32], 0.0).astype(BF16)
        left[:, 512:1024] = jnp.where(diagonal, tiled[32:64], 0.0).astype(BF16)

        dcopy, ycopy = [], {}

        def part_of(i, side, target):
            for part in range(2):
                slot = i * 4 + side * 2 + part
                loads[slot].wait()
                target[i, :, part * 256 : part * 256 + 256] = jnp.dot(
                    left[...], kbuf[slot], preferred_element_type=F32
                )

        def other(i):
            part_of(i, 0, dsend)
            if i == 0:
                pl.semaphore_wait(
                    barrier, 18 + jnp.where(x == 3, 16 - is_edge.astype(jnp.int32), 0)
                )
            copy = pltpu.make_async_remote_copy(
                src_ref=dsend.at[i], dst_ref=drecv.at[i],
                send_sem=dsem.at[0, i], recv_sem=dsem.at[1, i],
                device_id=partner, device_id_type=MESH,
            )
            copy.start()
            dcopy.append(copy)

        def mine(i):
            part_of(i, 1, own)

        def merge(i):
            d = ORDER[i]
            dcopy[i].wait_recv()
            total = own[i] + drecv[i]
            if d == 0:
                own[i] = total
                return
            ysend[d - 1] = total
            ycopy[d] = pltpu.make_async_remote_copy(
                src_ref=ysend.at[d - 1], dst_ref=yrecv.at[d - 1],
                send_sem=ysem.at[0, d - 1], recv_sem=ysem.at[1, d - 1],
                device_id=y_peer[d], device_id_type=MESH,
            )
            ycopy[d].start()

    with jax.named_scope("spectrum"):
        other(0)
        other(1)

        for copy in grids:
            copy.wait()
        fields[(4, *inner)] = mbuf[...].astype(F32)
        ns_copies = []
        for at, (first, last, peer) in enumerate(((8, 264, north), (256, 0, south))):
            copy = pltpu.make_async_remote_copy(
                src_ref=fields.at[:, pl.ds(first, 8)],
                dst_ref=fields.at[:, pl.ds(last, 8)],
                send_sem=nssem.at[0, at], recv_sem=nssem.at[1, at],
                device_id=peer, device_id_type=MESH,
            )
            copy.start()
            ns_copies.append(copy)
        mine(0)
        other(2)
        mine(1)
        merge(0)
        other(3)
        mine(2)
        merge(1)
        mine(3)
        merge(2)

    with jax.named_scope("widen"):
        split = split_rows(tables[0:32])
        wide[...] = jnp.concatenate(
            [*(split[k].astype(F32) for k in (0, 0, 1, 0, 2, 1)), jnp.zeros((64, 128), F32)], axis=0
        ).T.astype(BF16)
        merge(3)

    with jax.named_scope("column_halos"):
        for copy in ns_copies:
            copy.wait_recv()

        @pl.when(row == 0)
        def _():
            fields[:, 0:8, :] = jnp.zeros((5, 8, 256), F32)

        @pl.when(is_edge)
        def _():
            fields[:, 264:272, :] = jnp.zeros((5, 8, 256), F32)

        lane = lax.broadcasted_iota(jnp.int32, (272, 128), 1)
        ew_copies = []
        for at, (first, shift, peer) in enumerate(((0, 0, west), (128, 4, east))):
            packed = jnp.zeros((272, 128), F32)
            for j in range(5):
                block = fields[j, :, first : first + 128]
                if 4 * j + shift:
                    block = pltpu.roll(block, 4 * j + shift, 1)
                packed = jnp.where((lane >> 2) == j, block, packed)
            packed = jnp.concatenate([packed, jnp.zeros((112, 128), F32)], axis=0)
            ewsend[at] = packed.T[0:24]
            copy = pltpu.make_async_remote_copy(
                src_ref=ewsend.at[at], dst_ref=ewrecv.at[at],
                send_sem=ewsem.at[0, at], recv_sem=ewsem.at[1, at],
                device_id=peer, device_id_type=MESH,
            )
            copy.start()
            ew_copies.append(copy)

    with jax.named_scope("sum_y"):
        total = own[3]
        for d in (1, 3, 2):
            ycopy[d].wait_recv()
            total = total + yrecv[d - 1]
        split = split_rows(total)
        stack = jnp.concatenate([split[k] for k in (0, 1, 0, 2, 0, 1)], axis=0)
        partial = jnp.dot(wide[:, 0:192], stack, preferred_element_type=F32)
        for at in range(4):
            xsend[at] = partial[at * 32 : at * 32 + 32]
        xcopy = {}
        for d in (2, 1, 3):
            xcopy[d] = pltpu.make_async_remote_copy(
                src_ref=xsend.at[(x + d) % 4], dst_ref=xrecv.at[d - 1],
                send_sem=xsem.at[0, d - 1], recv_sem=xsem.at[1, d - 1],
                device_id=x_peer[d], device_id_type=MESH,
            )
            xcopy[d].start()

    with jax.named_scope("selection"):
        @pl.when(is_edge)
        def _():
            at = lax.broadcasted_iota(jnp.int32, (128, 384), 1)
            column = col * 256 + jnp.where(at >= 320, at - 384, at)
            turned = jnp.concatenate(
                [cellbuf[...].astype(F32), jnp.zeros((96, 128), F32)], axis=0
            ).T.astype(jnp.int32)
            found = jnp.zeros((128, 384), F32)
            for block in range(32):
                found = jnp.where(turned[:, block : block + 1] == column, block + 1.0, found)
            onehot[...] = jnp.where(found > 0.0, 1.0, 0.0).astype(BF16)
            blocks[...] = jnp.broadcast_to(jnp.sum(found, axis=0, keepdims=True), (8, 384))

    with jax.named_scope("water"):
        def strip(at, carry):
            base = pl.multiple_of(at * 32, 8)
            state = [fields[j, pl.ds(base, 48), :] for j in range(5)]
            values, rest = state[0:3], state[3:5]
            terms = face_terms(*rest)
            for _ in range(2):
                values = advance(*values, *rest, terms)
            for ref, value in zip((surf_o, flow_x_o, flow_y_o), values):
                ref[pl.ds(base, 32), :] = value[8:40]
            return carry

        lax.fori_loop(0, 8, strip, 0)

    with jax.named_scope("sum_x"):
        total = xsend[x]
        for d in (1, 3, 2):
            xcopy[d].wait_recv()
            total = total + xrecv[d - 1]
        zsend[0] = total[:, 0:256]
        zsend[1] = total[:, 256:512]
        for at in range(8):
            gsend[at : at + 1] = total[30 + at // 4 : 31 + at // 4, at % 4 * 128 : at % 4 * 128 + 128]
        here = pl.ds(pl.multiple_of((z * 8 + y * 2 + core) * 8, 8), 8)

        def ghost_copy(index):
            return pltpu.make_async_remote_copy(
                src_ref=gsend, dst_ref=grecv.at[here],
                send_sem=gssem.at[index], recv_sem=grsem,
                device_id=(15, index), device_id_type=MESH,
            )

        @pl.when(x == 3)
        def _():
            for index in range(16):
                pl.when((row != 15) | (col != index))(ghost_copy(index).start)

        zcopy = {}
        for d in (4, 3, 5, 2, 6, 1, 7):
            to = (z + d) % 8
            zcopy[d] = pltpu.make_async_remote_copy(
                src_ref=zsend.at[to // 4, pl.ds(pl.multiple_of((to % 4) * 8, 8), 8)],
                dst_ref=zrecv.at[d - 1],
                send_sem=zsem.at[0, d - 1], recv_sem=zsem.at[1, d - 1],
                device_id=z_peer[d], device_id_type=MESH,
            )
            zcopy[d].start()

    with jax.named_scope("side_water"):
        for copy in ew_copies:
            copy.wait_recv()
        from_east = jnp.where(col == 15, 0.0, ewrecv[0])
        from_west = jnp.where(col == 0, 0.0, ewrecv[1])
        for j in range(5):
            for at, piece in enumerate((from_west, ewsend[0], ewsend[1], from_east)):
                sides[j, at * 4 : at * 4 + 4] = piece[j * 4 : j * 4 + 4]
        state = [sides[j] for j in range(5)]
        values, rest = state[0:3], state[3:5]
        terms = face_terms(*rest, (0, 1))
        for _ in range(2):
            values = advance(*values, *rest, terms, (0, 1))
        turned = jnp.concatenate([*values, jnp.zeros((80, 384), F32)], axis=0).T[8:264]
        lane = lax.broadcasted_iota(jnp.int32, (256, 128), 1)
        for j, ref in enumerate((surf_o, flow_x_o, flow_y_o)):
            ref[:, 0:128] = jnp.where(
                lane < 2, pltpu.roll(turned, 124 - 16 * j, 1), ref[:, 0:128]
            )
            ref[:, 128:256] = jnp.where(
                lane >= 126, pltpu.roll(turned, 116 - 16 * j, 1), ref[:, 128:256]
            )

        @pl.when(is_edge)
        def _():
            blank = jnp.zeros((104, 256), F32)
            right, left_side = (
                jnp.concatenate([piece[:, 128:384], blank], axis=0).T[120:144]
                for piece in (from_east, from_west)
            )
            lane = lax.broadcasted_iota(jnp.int32, (24, 128), 1)
            for j in range(5):
                first = pltpu.roll(right, 128 - 4 * j, 1) if j else right
                wrapped = pltpu.roll(left_side, 124 - 4 * j, 1)
                tail[j] = jnp.where(lane < 2, first, jnp.where(lane >= 126, wrapped, 0.0))

    with jax.named_scope("sum_z"):
        total = zsend[z_hi, pl.ds(pl.multiple_of(z_lo * 8, 8), 8)]
        for d in range(1, 8):
            zcopy[d].wait_recv()
            total = total + zrecv[d - 1]
        series_o[...] = total

    with jax.named_scope("ghost"):
        @pl.when(is_edge)
        def _():
            grecv[here] = gsend[...]
            pltpu.make_async_copy(
                grecv.at[pl.ds(0, 504)], grecv.at[pl.ds(0, 504)], grsem
            ).wait()
            value = grecv[0:64]
            for other_z in range(1, 8):
                value = value + grecv[other_z * 64 : other_z * 64 + 64]
            picked = jnp.dot(
                jnp.concatenate(split_rows(value), axis=0), onehot[...],
                preferred_element_type=F32,
            )
            picked = picked[128:192] + picked[64:128] + picked[0:64]
            at = lax.broadcasted_iota(jnp.int32, (64, 384), 0)
            block = (at >> 4) * 8 + (at & 2) * 2 + ((at >> 3) & 1) * 2 + (at & 1)
            picked = jnp.where((block + 1).astype(F32) == blocks[0:1], picked, 0.0)
            ghost = [
                jnp.sum(jnp.where(((at >> 2) & 1) == step, picked, 0.0), axis=0, keepdims=True)
                for step in range(2)
            ]
            beyond = lax.broadcasted_iota(jnp.int32, (24, 384), 0) == 16
            state = [
                jnp.concatenate([fields[j, 248:272, :], tail[j]], axis=1) for j in range(5)
            ]
            rest = [jnp.where(beyond, 1.0, value) for value in state[3:5]]
            values = state[0:3]
            terms = face_terms(*rest)
            for step in range(2):
                values = [
                    jnp.where(beyond, ghost[step], values[0]),
                    jnp.where(beyond, 0.0, values[1]),
                    jnp.where(beyond, 0.0, values[2]),
                ]
                values = advance(*values, *rest, terms)
            for ref, value in zip((surf_o, flow_x_o, flow_y_o), values):
                ref[248:256, :] = value[8:16, 0:256]

    with jax.named_scope("drain"):
        for copy in [*dcopy, *ycopy.values(), *xcopy.values(), *zcopy.values(), *ns_copies, *ew_copies]:
            copy.wait_send()

        @pl.when(x == 3)
        def _():
            for index in range(16):
                pl.when((row != 15) | (col != index))(ghost_copy(index).wait_send)


def write_out(*refs):
    sources, targets, sems = refs[0:4], refs[4:8], refs[8]
    copies = [
        pltpu.make_async_copy(source, target, sems.at[j])
        for j, (source, target) in enumerate(zip(sources, targets))
    ]
    for copy in copies:
        copy.start()
    for copy in copies:
        copy.wait()


def on_device(
    kernel_hat, coefficients, wave_speed_sq, wet_mask, boundary_cell, height, flux_x, flux_y
):
    field = jax.ShapeDtypeStruct((256, 256), F32)
    dma = pltpu.SemaphoreType.DMA
    shapes = (jax.ShapeDtypeStruct((8, 256), F32), field, field, field)
    operands = [
        pltpu.with_memory_space_constraint(value, pltpu.MemorySpace.HBM)
        for value in (
            kernel_hat.reshape(1024, 4096),
            coefficients.T,
            wave_speed_sq,
            wet_mask,
            boundary_cell.reshape(32, 128),
            height,
            flux_x,
            flux_y,
            jnp.asarray(transform_tables()),
        )
    ]
    results = pl.pallas_call(
        kernel,
        out_shape=shapes,
        in_specs=[pl.BlockSpec(memory_space=pltpu.MemorySpace.HBM)] * 9,
        out_specs=[pl.BlockSpec(memory_space=pltpu.VMEM)] * 4,
        scratch_shapes=[
            pltpu.VMEM((16, 1024, 256), BF16),
            pltpu.VMEM((128, 128), F32),
            pltpu.VMEM((32, 128), F32),
            pltpu.VMEM((256, 256), jnp.int32),
            pltpu.VMEM((32, 128), jnp.int32),
            pltpu.VMEM((32, 1024), BF16),
            pltpu.VMEM((4, 32, 512), F32),
            pltpu.VMEM((4, 32, 512), F32),
            pltpu.VMEM((4, 32, 512), F32),
            pltpu.VMEM((3, 32, 512), F32),
            pltpu.VMEM((3, 32, 512), F32),
            pltpu.VMEM((4, 32, 512), F32),
            pltpu.VMEM((3, 32, 512), F32),
            pltpu.VMEM((2, 32, 256), F32),
            pltpu.VMEM((7, 8, 256), F32),
            pltpu.VMEM((8, 128), F32),
            pltpu.VMEM((512, 128), F32),
            pltpu.VMEM((5, 272, 256), F32),
            pltpu.VMEM((2, 24, 384), F32),
            pltpu.VMEM((2, 24, 384), F32),
            pltpu.VMEM((5, 16, 384), F32),
            pltpu.VMEM((5, 24, 128), F32),
            pltpu.VMEM((128, 384), BF16),
            pltpu.VMEM((8, 384), F32),
            pltpu.VMEM((128, 256), BF16),
            dma((16,)),
            dma((8,)),
            dma((2, 4)),
            dma((2, 3)),
            dma((2, 3)),
            dma((2, 7)),
            dma((16,)),
            dma(()),
            dma((2, 2)),
            dma((2, 2)),
        ],
        compiler_params=pltpu.CompilerParams(
            collective_id=0, has_side_effects=True, vmem_limit_bytes=48 * 1024 * 1024
        ),
    )(*operands)
    return pl.pallas_call(
        write_out,
        out_shape=shapes,
        in_specs=[pl.BlockSpec(memory_space=pltpu.VMEM)] * 4,
        out_specs=[pl.BlockSpec(memory_space=pltpu.MemorySpace.HBM)] * 4,
        scratch_shapes=[dma((4,))],
        compiler_params=pltpu.CompilerParams(vmem_limit_bytes=16 * 1024 * 1024),
    )(*results)


def solution(mesh):
    return jax.shard_map(
        on_device,
        mesh=mesh,
        in_specs=(
            P(None, "rows", "cols", None),
            P(None, "cols"),
            P("rows", "cols"),
            P("rows", "cols"),
            P(),
            P("rows", "cols"),
            P("rows", "cols"),
            P("rows", "cols"),
        ),
        out_specs=(P("rows", "cols"), P("rows", "cols"), P("rows", "cols"), P("rows", "cols")),
        check_vma=False,
    )
```

```python
import functools

import jax
import jax.numpy as jnp
import numpy as np
from jax import lax
from jax.experimental import pallas as pl
from jax.experimental.pallas import tpu as pltpu
from jax.sharding import PartitionSpec as P

F32 = jnp.float32
BF16 = jnp.bfloat16
HIGH = lax.Precision.HIGHEST
MESH = pl.DeviceIdType.MESH
ORDER = (2, 1, 3, 0)
LOADS = (0, 4, 8, 12, 1, 5, 9, 13, 2, 6, 10, 14, 3, 7, 11, 15)


def transform_tables():
    table = np.zeros((16, 128, 128), np.float32)
    times = np.arange(128)
    inner = times.reshape(4, 4, 8).transpose(1, 0, 2).reshape(-1)
    for row in range(16):
        freqs = row * 16 + np.arange(16)
        angle = 2.0 * np.pi * ((freqs[:, None] * inner[None, :]) % 256) / 256.0
        table[row, 0:16] = np.cos(angle) / 256.0
        table[row, 16:32] = -np.sin(angle) / 256.0
        angle = 2.0 * np.pi * ((freqs[:, None] * times[None, :]) % 256) / 256.0
        table[row, 32:48] = np.cos(angle)
        table[row, 48:64] = -np.sin(angle)
        table[row, 64:80] = np.sin(angle)
        table[row, 80:96] = np.cos(angle)
    return table


def after(values, axis):
    return pltpu.roll(values, values.shape[axis] - 1, axis)


def before(values, axis):
    return pltpu.roll(values, 1, axis)


def split_rows(value):
    high = value.astype(BF16)
    value = value - high.astype(F32)
    middle = value.astype(BF16)
    return [high, middle, (value - middle.astype(F32)).astype(BF16)]


def face_terms(speed, wet, axes=(1, 0)):
    celerity = jnp.sqrt(speed)
    terms = []
    for axis in axes:
        opened = wet * after(wet, axis)
        terms.append((0.5 * opened, opened * (0.25 * (celerity + after(celerity, axis)))))
    return terms


def advance(surface, along_x, along_y, speed, wet, terms, axes=(1, 0)):
    pressure = speed * surface
    changes = []
    for axis, along, across, (half, damp) in zip(
        axes, (along_x, along_y), (along_y, along_x), terms
    ):
        next_along = after(along, axis)
        mass = half * (along + next_along) - damp * (after(surface, axis) - surface)
        push = half * (pressure + after(pressure, axis)) - damp * (next_along - along)
        shear = damp * (across - after(across, axis))
        changes.append(tuple(flux - before(flux, axis) for flux in (mass, push, shear)))
    (mass_x, push_x, shear_x), (mass_y, push_y, shear_y) = changes
    return (
        wet * (surface - 0.25 * (mass_x + mass_y)),
        wet * (along_x - 0.25 * (push_x + shear_y)),
        wet * (along_y - 0.25 * (shear_x + push_y)),
    )


def kernel(
    kern, coef, speed, mask, cells, surf, flow_x, flow_y, table,
    series_o, surf_o, flow_x_o, flow_y_o,
    kbuf, tab, cbuf, mbuf, cellbuf, left, own, dsend, drecv, ysend, yrecv,
    xsend, xrecv, zsend, zrecv, gsend, grecv, fields, ewsend, ewrecv, sides, tail, onehot, blocks, wide,
    ksem, lsem, dsem, ysem, xsem, zsem, gssem, grsem, nssem, ewsem,
):
    row, col = lax.axis_index("rows"), lax.axis_index("cols")
    x, z_lo = row % 4, row // 4
    y, z_hi, core = col // 4, (col // 2) % 2, col % 2
    z = z_hi * 4 + z_lo
    is_edge = row == 15

    def place(at_x, at_y, at_z, at_core):
        return ((at_z % 4) * 4 + at_x, at_y * 4 + (at_z // 4) * 2 + at_core)

    partner = place(x, y, z, 1 - core)
    y_peer = [place(x, (y + d) % 4, z, core) for d in range(4)]
    x_peer = [place((x + d) % 4, y, z, core) for d in range(4)]
    z_peer = [place(x, y, (z + d) % 8, core) for d in range(8)]
    north, south = ((row + 15) % 16, col), ((row + 1) % 16, col)
    west, east = (row, (col + 15) % 16), (row, (col + 1) % 16)

    with jax.named_scope("start_loads"):
        local = [
            pltpu.make_async_copy(coef, cbuf, lsem.at[1]),
            pltpu.make_async_copy(table.at[row], tab, lsem.at[0]),
        ]
        for copy in local:
            copy.start()
        inner = (pl.ds(8, 256), slice(None))
        grids = [
            pltpu.make_async_copy(ref, fields.at[(j, *inner)], lsem.at[2 + j])
            for j, ref in enumerate((surf, flow_x, flow_y, speed))
        ]
        grids += [
            pltpu.make_async_copy(mask, mbuf, lsem.at[6]),
            pltpu.make_async_copy(cells, cellbuf, lsem.at[7]),
        ]
        for copy in grids:
            copy.start()
        loads = []
        for i, d in enumerate(ORDER):
            for side, par in enumerate((1 - core, core)):
                for part in range(2):
                    slot = i * 4 + side * 2 + part
                    start = pl.multiple_of(((((y + d) % 4) * 2 + part) * 2 + par) * 256, 256)
                    loads.append(
                        pltpu.make_async_copy(
                            kern.at[:, pl.ds(start, 256)], kbuf.at[slot], ksem.at[slot]
                        )
                    )
        for slot in LOADS[0:4]:
            loads[slot].start()

    with jax.named_scope("greet_peers"):
        barrier = pltpu.get_barrier_semaphore()
        for peer in [partner, *y_peer[1:], *x_peer[1:], *z_peer[1:]]:
            pl.semaphore_signal(barrier, inc=1, device_id=peer, device_id_type=MESH)
        around = ((north, row > 0), (south, row < 15), (west, col > 0), (east, col < 15))
        greetings = 14 + jnp.where(x == 3, 16 - is_edge.astype(jnp.int32), 0)
        for peer, inside in around:
            greetings = greetings + inside.astype(jnp.int32)

            @pl.when(inside)
            def _():
                pl.semaphore_signal(barrier, inc=1, device_id=peer, device_id_type=MESH)

        @pl.when(is_edge)
        def _():
            for at_row in (3, 7, 11, 15):
                for at_col in range(16):
                    def greet(peer=(at_row, at_col)):
                        pl.semaphore_signal(barrier, inc=1, device_id=peer, device_id_type=MESH)

                    if at_row == 15:
                        pl.when(col != at_col)(greet)
                    else:
                        greet()

    with jax.named_scope("more_loads"):
        for slot in LOADS[4:]:
            loads[slot].start()

    with jax.named_scope("wait_coef"):
        local[0].wait()
    with jax.named_scope("wait_table"):
        local[1].wait()

    with jax.named_scope("build_left"):
        tables = tab[...]
        tiled = lax.dot_general(
            tables[32:96], jnp.concatenate([cbuf[...]] * 16, axis=0), (((1,), (1,)), ((), ())),
            precision=HIGH, preferred_element_type=F32,
        )
        lanes = lax.broadcasted_iota(jnp.int32, (32, 512), 1)
        subs = lax.broadcasted_iota(jnp.int32, (32, 512), 0)
        diagonal = (lanes >> 5) == (subs & 15)
        left[:, 0:512] = jnp.where(diagonal, tiled[0:32], 0.0).astype(BF16)
        left[:, 512:1024] = jnp.where(diagonal, tiled[32:64], 0.0).astype(BF16)

        dcopy, ycopy, xcopy = {}, {}, {}

        def products(part, side, target):
            for i in range(4):
                loads[i * 4 + side * 2 + part].wait()
            for i in range(4):
                target[part, i] = jnp.dot(
                    left[...], kbuf[i * 4 + side * 2 + part], preferred_element_type=F32
                )

        def to_partner(part):
            dcopy[part] = pltpu.make_async_remote_copy(
                src_ref=dsend.at[part], dst_ref=drecv.at[part],
                send_sem=dsem.at[0, part], recv_sem=dsem.at[1, part],
                device_id=partner, device_id_type=MESH,
            )
            dcopy[part].start()

        def merge(part):
            dcopy[part].wait_recv()
            for i, d in enumerate(ORDER):
                total = own[part, i] + drecv[part, i]
                if d == 0:
                    own[part, i] = total
                    continue
                ysend[part, d - 1] = total
                ycopy[part, d] = pltpu.make_async_remote_copy(
                    src_ref=ysend.at[part, d - 1], dst_ref=yrecv.at[part, d - 1],
                    send_sem=ysem.at[0, part, d - 1], recv_sem=ysem.at[1, part, d - 1],
                    device_id=y_peer[d], device_id_type=MESH,
                )
                ycopy[part, d].start()

        def sum_y(part):
            total = own[part, 3]
            for d in (1, 3, 2):
                ycopy[part, d].wait_recv()
                total = total + yrecv[part, d - 1]
            split = split_rows(total)
            stack = jnp.concatenate([split[k] for k in (0, 1, 0, 2, 0, 1)], axis=0)
            partial = jnp.dot(wide[:, 0:192], stack, preferred_element_type=F32)
            for at in range(4):
                xsend[part, at] = partial[at * 32 : at * 32 + 32]
            for d in (2, 1, 3):
                xcopy[part, d] = pltpu.make_async_remote_copy(
                    src_ref=xsend.at[part, (x + d) % 4], dst_ref=xrecv.at[part, d - 1],
                    send_sem=xsem.at[0, part, d - 1], recv_sem=xsem.at[1, part, d - 1],
                    device_id=x_peer[d], device_id_type=MESH,
                )
                xcopy[part, d].start()

        def z_copy(part, k):
            lo = (z_lo + k) % 4
            d = (part * 4 + lo + 8 - z) % 8
            at = (d + 7) % 8
            return d, pltpu.make_async_remote_copy(
                src_ref=zsend.at[part, pl.ds(pl.multiple_of(lo * 8, 8), 8)],
                dst_ref=zrecv.at[at],
                send_sem=zsem.at[0, at], recv_sem=zsem.at[1, at],
                device_id=place(x, y, part * 4 + lo, core), device_id_type=MESH,
            )

        def sum_x(part):
            total = xsend[part, x]
            for d in (1, 3, 2):
                xcopy[part, d].wait_recv()
                total = total + xrecv[part, d - 1]
            zsend[part] = total
            for step in range(2):
                for half in range(2):
                    at = step * 4 + part * 2 + half
                    gsend[at : at + 1] = total[30 + step : 31 + step, half * 128 : half * 128 + 128]
            for k in (2, 1, 3, 0):
                d, copy = z_copy(part, k)
                if k == 0:
                    pl.when(d != 0)(copy.start)
                else:
                    copy.start()

        def strip(at, carry):
            base = pl.multiple_of(at * 32, 8)
            state = [fields[j, pl.ds(base, 48), :] for j in range(5)]
            values, rest = state[0:3], state[3:5]
            terms = face_terms(*rest)
            for _ in range(2):
                values = advance(*values, *rest, terms)
            for ref, value in zip((surf_o, flow_x_o, flow_y_o), values):
                ref[pl.ds(base, 32), :] = value[8:40]
            return carry

    with jax.named_scope("spectrum"):
        products(0, 0, dsend)
    with jax.named_scope("barrier"):
        pl.semaphore_wait(barrier, greetings)
    with jax.named_scope("spectrum_1"):
        to_partner(0)
        products(1, 0, dsend)
        to_partner(1)
    with jax.named_scope("row_halos"):
        for copy in grids:
            copy.wait()
        fields[(4, *inner)] = mbuf[...].astype(F32)
        ns_copies = []
        for at, (first, last, peer, inside) in enumerate(
            ((8, 264, north, row > 0), (256, 0, south, row < 15))
        ):
            copy = pltpu.make_async_remote_copy(
                src_ref=fields.at[:, pl.ds(first, 8)],
                dst_ref=fields.at[:, pl.ds(last, 8)],
                send_sem=nssem.at[0, at], recv_sem=nssem.at[1, at],
                device_id=peer, device_id_type=MESH,
            )
            pl.when(inside)(copy.start)
            ns_copies.append((copy, inside))
    with jax.named_scope("spectrum_2"):
        products(0, 1, own)
    with jax.named_scope("merge_0"):
        merge(0)
    with jax.named_scope("spectrum_3"):
        products(1, 1, own)
    with jax.named_scope("merge_1"):
        merge(1)

    with jax.named_scope("widen"):
        split = split_rows(tables[0:32])
        wide[...] = jnp.concatenate(
            [*(split[k].astype(F32) for k in (0, 0, 1, 0, 2, 1)), jnp.zeros((64, 128), F32)], axis=0
        ).T.astype(BF16)
    with jax.named_scope("water"):
        lax.fori_loop(1, 5, strip, 0)
    with jax.named_scope("sum_y_0"):
        sum_y(0)
    with jax.named_scope("sum_y_1"):
        sum_y(1)

    with jax.named_scope("column_halos"):
        pl.when(row < 15)(ns_copies[0][0].wait_recv)
        pl.when(row > 0)(ns_copies[1][0].wait_recv)

        @pl.when(row == 0)
        def _():
            fields[:, 0:8, :] = jnp.zeros((5, 8, 256), F32)

        @pl.when(is_edge)
        def _():
            fields[:, 264:272, :] = jnp.zeros((5, 8, 256), F32)

        lane = lax.broadcasted_iota(jnp.int32, (272, 128), 1)
        ew_copies = []
        for at, (first, shift, peer, inside) in enumerate(
            ((0, 0, west, col > 0), (128, 4, east, col < 15))
        ):
            packed = jnp.zeros((272, 128), F32)
            for j in range(5):
                block = fields[j, :, first : first + 128]
                if 4 * j + shift:
                    block = pltpu.roll(block, 4 * j + shift, 1)
                packed = jnp.where((lane >> 2) == j, block, packed)
            packed = jnp.concatenate([packed, jnp.zeros((112, 128), F32)], axis=0)
            ewsend[at] = packed.T[0:24]
            copy = pltpu.make_async_remote_copy(
                src_ref=ewsend.at[at], dst_ref=ewrecv.at[at],
                send_sem=ewsem.at[0, at], recv_sem=ewsem.at[1, at],
                device_id=peer, device_id_type=MESH,
            )
            pl.when(inside)(copy.start)
            ew_copies.append((copy, inside))

    with jax.named_scope("water_1"):
        lax.fori_loop(5, 7, strip, 0)
    with jax.named_scope("sum_x_0"):
        sum_x(0)
    with jax.named_scope("sum_x_1"):
        sum_x(1)

    with jax.named_scope("ghost_send"):
        here = pl.ds(pl.multiple_of((z * 8 + y * 2 + core) * 8, 8), 8)

        def ghost_copy(index):
            return pltpu.make_async_remote_copy(
                src_ref=gsend, dst_ref=grecv.at[here],
                send_sem=gssem.at[index], recv_sem=grsem,
                device_id=(15, index), device_id_type=MESH,
            )

        @pl.when(x == 3)
        def _():
            for index in range(16):
                pl.when((row != 15) | (col != index))(ghost_copy(index).start)

    with jax.named_scope("more_water"):
        lax.fori_loop(0, 2, lambda at, carry: strip(at * 7, carry), 0)

    with jax.named_scope("selection"):
        @pl.when(is_edge)
        def _():
            at = lax.broadcasted_iota(jnp.int32, (128, 384), 1)
            column = col * 256 + jnp.where(at >= 320, at - 384, at)
            turned = jnp.concatenate(
                [cellbuf[...].astype(F32), jnp.zeros((96, 128), F32)], axis=0
            ).T.astype(jnp.int32)
            found = jnp.zeros((128, 384), F32)
            for block in range(32):
                found = jnp.where(turned[:, block : block + 1] == column, block + 1.0, found)
            onehot[...] = jnp.where(found > 0.0, 1.0, 0.0).astype(BF16)
            blocks[...] = jnp.broadcast_to(jnp.sum(found, axis=0, keepdims=True), (8, 384))

    with jax.named_scope("side_water"):
        for at, ((copy, _), inside) in enumerate(zip(ew_copies, (col < 15, col > 0))):
            pl.when(inside)(copy.wait_recv)

            @pl.when(~inside)
            def _():
                ewrecv[at] = jnp.zeros((24, 384), F32)

        from_east, from_west = ewrecv[0], ewrecv[1]
        for j in range(5):
            for at, piece in enumerate((from_west, ewsend[0], ewsend[1], from_east)):
                sides[j, at * 4 : at * 4 + 4] = piece[j * 4 : j * 4 + 4]
        state = [sides[j] for j in range(5)]
        values, rest = state[0:3], state[3:5]
        terms = face_terms(*rest, (0, 1))
        for _ in range(2):
            values = advance(*values, *rest, terms, (0, 1))
        turned = jnp.concatenate([*values, jnp.zeros((80, 384), F32)], axis=0).T[8:264]
        lane = lax.broadcasted_iota(jnp.int32, (256, 128), 1)
        for j, ref in enumerate((surf_o, flow_x_o, flow_y_o)):
            ref[:, 0:128] = jnp.where(
                lane < 2, pltpu.roll(turned, 124 - 16 * j, 1), ref[:, 0:128]
            )
            ref[:, 128:256] = jnp.where(
                lane >= 126, pltpu.roll(turned, 116 - 16 * j, 1), ref[:, 128:256]
            )

        @pl.when(is_edge)
        def _():
            blank = jnp.zeros((104, 256), F32)
            right, left_side = (
                jnp.concatenate([piece[:, 128:384], blank], axis=0).T[120:144]
                for piece in (from_east, from_west)
            )
            lane = lax.broadcasted_iota(jnp.int32, (24, 128), 1)
            for j in range(5):
                first = pltpu.roll(right, 128 - 4 * j, 1) if j else right
                wrapped = pltpu.roll(left_side, 124 - 4 * j, 1)
                tail[j] = jnp.where(lane < 2, first, jnp.where(lane >= 126, wrapped, 0.0))

    with jax.named_scope("sum_z"):
        total = zsend[z_hi, pl.ds(pl.multiple_of(z_lo * 8, 8), 8)]
        for d in range(1, 8):
            pltpu.make_async_copy(zrecv.at[d - 1], zrecv.at[d - 1], zsem.at[1, d - 1]).wait()
            total = total + zrecv[d - 1]
        series_o[...] = total

    with jax.named_scope("ghost"):
        @pl.when(is_edge)
        def _():
            grecv[here] = gsend[...]
            pltpu.make_async_copy(
                grecv.at[pl.ds(0, 504)], grecv.at[pl.ds(0, 504)], grsem
            ).wait()
            value = grecv[0:64]
            for other_z in range(1, 8):
                value = value + grecv[other_z * 64 : other_z * 64 + 64]
            picked = jnp.dot(
                jnp.concatenate(split_rows(value), axis=0), onehot[...],
                preferred_element_type=F32,
            )
            picked = picked[128:192] + picked[64:128] + picked[0:64]
            at = lax.broadcasted_iota(jnp.int32, (64, 384), 0)
            block = (at >> 4) * 8 + (at & 2) * 2 + ((at >> 3) & 1) * 2 + (at & 1)
            picked = jnp.where((block + 1).astype(F32) == blocks[0:1], picked, 0.0)
            ghost = [
                jnp.sum(jnp.where(((at >> 2) & 1) == step, picked, 0.0), axis=0, keepdims=True)
                for step in range(2)
            ]
            beyond = lax.broadcasted_iota(jnp.int32, (24, 384), 0) == 16
            state = [
                jnp.concatenate([fields[j, 248:272, :], tail[j]], axis=1) for j in range(5)
            ]
            rest = [jnp.where(beyond, 1.0, value) for value in state[3:5]]
            values = state[0:3]
            terms = face_terms(*rest)
            for step in range(2):
                values = [
                    jnp.where(beyond, ghost[step], values[0]),
                    jnp.where(beyond, 0.0, values[1]),
                    jnp.where(beyond, 0.0, values[2]),
                ]
                values = advance(*values, *rest, terms)
            for ref, value in zip((surf_o, flow_x_o, flow_y_o), values):
                ref[248:256, :] = value[8:16, 0:256]

    with jax.named_scope("drain"):
        for copy in [*dcopy.values(), *ycopy.values(), *xcopy.values()]:
            copy.wait_send()
        for copy, inside in [*ns_copies, *ew_copies]:
            pl.when(inside)(copy.wait_send)
        for part in range(2):
            for k in range(4):
                d, copy = z_copy(part, k)
                pl.when(d != 0)(copy.wait_send)

        @pl.when(x == 3)
        def _():
            for index in range(16):
                pl.when((row != 15) | (col != index))(ghost_copy(index).wait_send)


def write_out(*refs):
    sources, targets, sems = refs[0:4], refs[4:8], refs[8]
    copies = [
        pltpu.make_async_copy(source, target, sems.at[j])
        for j, (source, target) in enumerate(zip(sources, targets))
    ]
    for copy in copies:
        copy.start()
    for copy in copies:
        copy.wait()


def on_device(
    kernel_hat, coefficients, wave_speed_sq, wet_mask, boundary_cell, height, flux_x, flux_y
):
    field = jax.ShapeDtypeStruct((256, 256), F32)
    dma = pltpu.SemaphoreType.DMA
    shapes = (jax.ShapeDtypeStruct((8, 256), F32), field, field, field)
    operands = [
        pltpu.with_memory_space_constraint(value, pltpu.MemorySpace.HBM)
        for value in (
            kernel_hat.reshape(1024, 4096),
            coefficients.T,
            wave_speed_sq,
            wet_mask,
            boundary_cell.reshape(32, 128),
            height,
            flux_x,
            flux_y,
            jnp.asarray(transform_tables()),
        )
    ]
    results = pl.pallas_call(
        kernel,
        out_shape=shapes,
        in_specs=[pl.BlockSpec(memory_space=pltpu.MemorySpace.HBM)] * 9,
        out_specs=[pl.BlockSpec(memory_space=pltpu.VMEM)] * 4,
        scratch_shapes=[
            pltpu.VMEM((16, 1024, 256), BF16),
            pltpu.VMEM((128, 128), F32),
            pltpu.VMEM((32, 128), F32),
            pltpu.VMEM((256, 256), jnp.int32),
            pltpu.VMEM((32, 128), jnp.int32),
            pltpu.VMEM((32, 1024), BF16),
            pltpu.VMEM((2, 4, 32, 256), F32),
            pltpu.VMEM((2, 4, 32, 256), F32),
            pltpu.VMEM((2, 4, 32, 256), F32),
            pltpu.VMEM((2, 3, 32, 256), F32),
            pltpu.VMEM((2, 3, 32, 256), F32),
            pltpu.VMEM((2, 4, 32, 256), F32),
            pltpu.VMEM((2, 3, 32, 256), F32),
            pltpu.VMEM((2, 32, 256), F32),
            pltpu.VMEM((7, 8, 256), F32),
            pltpu.VMEM((8, 128), F32),
            pltpu.VMEM((512, 128), F32),
            pltpu.VMEM((5, 272, 256), F32),
            pltpu.VMEM((2, 24, 384), F32),
            pltpu.VMEM((2, 24, 384), F32),
            pltpu.VMEM((5, 16, 384), F32),
            pltpu.VMEM((5, 24, 128), F32),
            pltpu.VMEM((128, 384), BF16),
            pltpu.VMEM((8, 384), F32),
            pltpu.VMEM((128, 256), BF16),
            dma((16,)),
            dma((8,)),
            dma((2, 2)),
            dma((2, 2, 3)),
            dma((2, 2, 3)),
            dma((2, 8)),
            dma((16,)),
            dma(()),
            dma((2, 2)),
            dma((2, 2)),
        ],
        compiler_params=pltpu.CompilerParams(
            collective_id=0, has_side_effects=True, vmem_limit_bytes=48 * 1024 * 1024
        ),
    )(*operands)
    return pl.pallas_call(
        write_out,
        out_shape=shapes,
        in_specs=[pl.BlockSpec(memory_space=pltpu.VMEM)] * 4,
        out_specs=[pl.BlockSpec(memory_space=pltpu.MemorySpace.HBM)] * 4,
        scratch_shapes=[dma((4,))],
        compiler_params=pltpu.CompilerParams(vmem_limit_bytes=16 * 1024 * 1024),
    )(*results)


def solution(mesh):
    return jax.shard_map(
        on_device,
        mesh=mesh,
        in_specs=(
            P(None, "rows", "cols", None),
            P(None, "cols"),
            P("rows", "cols"),
            P("rows", "cols"),
            P(),
            P("rows", "cols"),
            P("rows", "cols"),
            P("rows", "cols"),
        ),
        out_specs=(P("rows", "cols"), P("rows", "cols"), P("rows", "cols"), P("rows", "cols")),
        check_vma=False,
    )
```

```python
import functools

import jax
import jax.numpy as jnp
import numpy as np
from jax import lax
from jax.experimental import pallas as pl
from jax.experimental.pallas import tpu as pltpu
from jax.sharding import PartitionSpec as P

F32 = jnp.float32
BF16 = jnp.bfloat16
HIGH = lax.Precision.HIGHEST
MESH = pl.DeviceIdType.MESH
ORDER = (2, 1, 3, 0)
LOADS = (0, 4, 8, 12, 1, 5, 9, 13, 2, 6, 10, 14, 3, 7, 11, 15)


def transform_tables():
    table = np.zeros((16, 128, 128), np.float32)
    times = np.arange(128)
    inner = times.reshape(4, 4, 8).transpose(1, 0, 2).reshape(-1)
    for row in range(16):
        freqs = row * 16 + np.arange(16)
        angle = 2.0 * np.pi * ((freqs[:, None] * inner[None, :]) % 256) / 256.0
        table[row, 0:16] = np.cos(angle) / 256.0
        table[row, 16:32] = -np.sin(angle) / 256.0
        angle = 2.0 * np.pi * ((freqs[:, None] * times[None, :]) % 256) / 256.0
        table[row, 32:48] = np.cos(angle)
        table[row, 48:64] = -np.sin(angle)
        table[row, 64:80] = np.sin(angle)
        table[row, 80:96] = np.cos(angle)
    return table


def after(values, axis):
    return pltpu.roll(values, values.shape[axis] - 1, axis)


def before(values, axis):
    return pltpu.roll(values, 1, axis)


def split_rows(value):
    high = value.astype(BF16)
    value = value - high.astype(F32)
    middle = value.astype(BF16)
    return [high, middle, (value - middle.astype(F32)).astype(BF16)]


def face_terms(speed, wet, axes=(1, 0)):
    celerity = jnp.sqrt(speed)
    terms = []
    for axis in axes:
        opened = wet * after(wet, axis)
        terms.append((0.5 * opened, opened * (0.25 * (celerity + after(celerity, axis)))))
    return terms


def advance(surface, along_x, along_y, speed, wet, terms, axes=(1, 0)):
    pressure = speed * surface
    changes = []
    for axis, along, across, (half, damp) in zip(
        axes, (along_x, along_y), (along_y, along_x), terms
    ):
        next_along = after(along, axis)
        mass = half * (along + next_along) - damp * (after(surface, axis) - surface)
        push = half * (pressure + after(pressure, axis)) - damp * (next_along - along)
        shear = damp * (across - after(across, axis))
        changes.append(tuple(flux - before(flux, axis) for flux in (mass, push, shear)))
    (mass_x, push_x, shear_x), (mass_y, push_y, shear_y) = changes
    return (
        wet * (surface - 0.25 * (mass_x + mass_y)),
        wet * (along_x - 0.25 * (push_x + shear_y)),
        wet * (along_y - 0.25 * (shear_x + push_y)),
    )


def kernel(
    kern, coef, speed, mask, cells, surf, flow_x, flow_y, table,
    series_o, surf_o, flow_x_o, flow_y_o,
    kbuf, tab, cbuf, mbuf, cellbuf, left, own, dsend, drecv, ysend, yrecv,
    xsend, xrecv, zsend, zrecv, gsend, gearly, gtotal, gpair, grecv, fields, ewsend, ewrecv, sides, tail, onehot, blocks, wide,
    ksem, lsem, dsem, ysem, xsem, zsem, gxsem, gpsem, gssem, grsem, nssem, ewsem, known,
):
    row, col = lax.axis_index("rows"), lax.axis_index("cols")
    x, z_lo = row % 4, row // 4
    y, z_hi, core = col // 4, (col // 2) % 2, col % 2
    z = z_hi * 4 + z_lo
    is_edge = row == 15

    def place(at_x, at_y, at_z, at_core):
        return ((at_z % 4) * 4 + at_x, at_y * 4 + (at_z // 4) * 2 + at_core)

    partner = place(x, y, z, 1 - core)
    y_peer = [place(x, (y + d) % 4, z, core) for d in range(4)]
    x_peer = [place((x + d) % 4, y, z, core) for d in range(4)]
    z_peer = [place(x, y, (z + d) % 8, core) for d in range(8)]
    north, south = ((row + 15) % 16, col), ((row + 1) % 16, col)
    west, east = (row, (col + 15) % 16), (row, (col + 1) % 16)

    with jax.named_scope("start_loads"):
        local = [
            pltpu.make_async_copy(coef, cbuf, lsem.at[1]),
            pltpu.make_async_copy(table.at[row], tab, lsem.at[0]),
        ]
        for copy in local:
            copy.start()
        loads = []
        for i, d in enumerate(ORDER):
            for side, par in enumerate((1 - core, core)):
                for part in range(2):
                    slot = i * 4 + side * 2 + part
                    start = pl.multiple_of(((((y + d) % 4) * 2 + part) * 2 + par) * 256, 256)
                    loads.append(
                        pltpu.make_async_copy(
                            kern.at[:, pl.ds(start, 256)], kbuf.at[slot], ksem.at[slot]
                        )
                    )
        for slot in LOADS[0:4]:
            loads[slot].start()

    with jax.named_scope("greet_peers"):
        barrier = pltpu.get_barrier_semaphore()
        near = [partner, *y_peer[1:], *x_peer[1:], *(z_peer[d] for d in (1, 2, 6, 7))]
        for peer in near:
            pl.semaphore_signal(barrier, inc=1, device_id=peer, device_id_type=MESH)
        greetings = len(near)
        for peer, inside in ((north, row > 0), (south, row < 15)):
            greetings = greetings + inside.astype(jnp.int32)

            @pl.when(inside)
            def _():
                pl.semaphore_signal(barrier, inc=1, device_id=peer, device_id_type=MESH)

    with jax.named_scope("more_loads"):
        for slot in LOADS[4:8]:
            loads[slot].start()
        inner = (pl.ds(8, 256), slice(None))
        grids = [
            pltpu.make_async_copy(ref, fields.at[(j, *inner)], lsem.at[2 + j])
            for j, ref in enumerate((surf, flow_x, flow_y, speed))
        ]
        grids += [
            pltpu.make_async_copy(mask, mbuf, lsem.at[6]),
            pltpu.make_async_copy(cells, cellbuf, lsem.at[7]),
        ]
        for copy in grids:
            copy.start()

    with jax.named_scope("wait_coef"):
        local[0].wait()
        for slot in LOADS[8:]:
            loads[slot].start()
    with jax.named_scope("wait_table"):
        local[1].wait()

    with jax.named_scope("build_left"):
        tables = tab[...]
        tiled = lax.dot_general(
            tables[32:96], jnp.concatenate([cbuf[...]] * 16, axis=0), (((1,), (1,)), ((), ())),
            precision=HIGH, preferred_element_type=F32,
        )
        lanes = lax.broadcasted_iota(jnp.int32, (32, 512), 1)
        subs = lax.broadcasted_iota(jnp.int32, (32, 512), 0)
        diagonal = (lanes >> 5) == (subs & 15)
        left[:, 0:512] = jnp.where(diagonal, tiled[0:32], 0.0).astype(BF16)
        left[:, 512:1024] = jnp.where(diagonal, tiled[32:64], 0.0).astype(BF16)

        dcopy, ycopy, xcopy = {}, {}, {}

        def products(part, side, target):
            for i in range(4):
                loads[i * 4 + side * 2 + part].wait()
            for i in range(4):
                target[part, i] = jnp.dot(
                    left[...], kbuf[i * 4 + side * 2 + part], preferred_element_type=F32
                )

        def to_partner(part):
            dcopy[part] = pltpu.make_async_remote_copy(
                src_ref=dsend.at[part], dst_ref=drecv.at[part],
                send_sem=dsem.at[0, part], recv_sem=dsem.at[1, part],
                device_id=partner, device_id_type=MESH,
            )
            dcopy[part].start()

        def merge(part):
            dcopy[part].wait_recv()
            for i, d in enumerate(ORDER):
                total = own[part, i] + drecv[part, i]
                if d == 0:
                    own[part, i] = total
                    continue
                ysend[part, d - 1] = total
                ycopy[part, d] = pltpu.make_async_remote_copy(
                    src_ref=ysend.at[part, d - 1], dst_ref=yrecv.at[part, d - 1],
                    send_sem=ysem.at[0, part, d - 1], recv_sem=ysem.at[1, part, d - 1],
                    device_id=y_peer[d], device_id_type=MESH,
                )
                ycopy[part, d].start()

        def early_ghost(d):
            return pltpu.make_async_remote_copy(
                src_ref=gsend, dst_ref=gearly.at[d],
                send_sem=gxsem.at[0], recv_sem=gxsem.at[1 + d],
                device_id=place(3, y, z, core), device_id_type=MESH,
            )

        def ahead(part, partial):
            for step in range(2):
                for half in range(2):
                    at = step * 4 + part * 2 + half
                    line = 126 + step
                    gsend[at : at + 1] = partial[line : line + 1, half * 128 : half * 128 + 128]
            if part == 1:
                pl.when(x < 3)(early_ghost(x).start)

        def sum_y(part):
            total = own[part, 3]
            for d in (1, 3, 2):
                ycopy[part, d].wait_recv()
                total = total + yrecv[part, d - 1]
            split = split_rows(total)
            stack = jnp.concatenate([split[k] for k in (0, 1, 0, 2, 0, 1)], axis=0)
            partial = jnp.dot(wide[:, 0:192], stack, preferred_element_type=F32)
            for at in range(4):
                xsend[part, at] = partial[at * 32 : at * 32 + 32]
            ahead(part, partial)
            for d in (2, 1, 3):
                xcopy[part, d] = pltpu.make_async_remote_copy(
                    src_ref=xsend.at[part, (x + d) % 4], dst_ref=xrecv.at[part, d - 1],
                    send_sem=xsem.at[0, part, d - 1], recv_sem=xsem.at[1, part, d - 1],
                    device_id=x_peer[d], device_id_type=MESH,
                )
                xcopy[part, d].start()

        def z_copy(part, k):
            lo = (z_lo + k) % 4
            d = (part * 4 + lo + 8 - z) % 8
            at = (d + 7) % 8
            return d, pltpu.make_async_remote_copy(
                src_ref=zsend.at[part, pl.ds(pl.multiple_of(lo * 8, 8), 8)],
                dst_ref=zrecv.at[at],
                send_sem=zsem.at[0, at], recv_sem=zsem.at[1, at],
                device_id=place(x, y, part * 4 + lo, core), device_id_type=MESH,
            )

        def sum_x(part):
            total = xsend[part, x]
            for d in (1, 3, 2):
                xcopy[part, d].wait_recv()
                total = total + xrecv[part, d - 1]
            zsend[part] = total
            for k in (2, 1, 3, 0):
                d, copy = z_copy(part, k)
                if k == 0:
                    pl.when(d != 0)(copy.start)
                else:
                    copy.start()

        def strip(at, carry):
            base = pl.multiple_of(at * 32, 8)
            state = [fields[j, pl.ds(base, 48), :] for j in range(5)]
            values, rest = state[0:3], state[3:5]
            terms = face_terms(*rest)
            for _ in range(2):
                values = advance(*values, *rest, terms)
            for ref, value in zip((surf_o, flow_x_o, flow_y_o), values):
                ref[pl.ds(base, 32), :] = value[8:40]
            return carry

    with jax.named_scope("spectrum"):
        products(0, 0, dsend)
    with jax.named_scope("barrier"):
        pl.semaphore_wait(barrier, greetings)
    with jax.named_scope("spectrum_1"):
        to_partner(0)
        products(1, 0, dsend)
        to_partner(1)
    with jax.named_scope("row_halos"):
        for copy in grids:
            copy.wait()
        fields[(4, *inner)] = mbuf[...].astype(F32)
        ns_copies = []
        for at, (first, last, peer, inside) in enumerate(
            ((8, 264, north, row > 0), (256, 0, south, row < 15))
        ):
            copy = pltpu.make_async_remote_copy(
                src_ref=fields.at[:, pl.ds(first, 8)],
                dst_ref=fields.at[:, pl.ds(last, 8)],
                send_sem=nssem.at[0, at], recv_sem=nssem.at[1, at],
                device_id=peer, device_id_type=MESH,
            )
            pl.when(inside)(copy.start)
            ns_copies.append((copy, inside))
    with jax.named_scope("spectrum_2"):
        products(0, 1, own)
    with jax.named_scope("merge_0"):
        merge(0)
    with jax.named_scope("spectrum_3"):
        products(1, 1, own)
    with jax.named_scope("merge_1"):
        merge(1)

    with jax.named_scope("widen"):
        split = split_rows(tables[0:32])
        wide[...] = jnp.concatenate(
            [*(split[k].astype(F32) for k in (0, 0, 1, 0, 2, 1)), jnp.zeros((64, 128), F32)], axis=0
        ).T.astype(BF16)
    with jax.named_scope("water"):
        lax.fori_loop(1, 3, strip, 0)
    with jax.named_scope("sum_y_0"):
        sum_y(0)
        for at, d in enumerate((2, 6)):
            pl.semaphore_signal(known.at[at], inc=1, device_id=z_peer[d], device_id_type=MESH)
    with jax.named_scope("sum_y_1"):
        sum_y(1)

    with jax.named_scope("column_halos"):
        pl.when(row < 15)(ns_copies[0][0].wait_recv)
        pl.when(row > 0)(ns_copies[1][0].wait_recv)

        @pl.when(row == 0)
        def _():
            fields[:, 0:8, :] = jnp.zeros((5, 8, 256), F32)

        @pl.when(is_edge)
        def _():
            fields[:, 264:272, :] = jnp.zeros((5, 8, 256), F32)

        lane = lax.broadcasted_iota(jnp.int32, (272, 128), 1)
        ew_copies = []
        for at, (first, shift, peer, inside) in enumerate(
            ((0, 0, west, col > 0), (128, 4, east, col < 15))
        ):
            packed = jnp.zeros((272, 128), F32)
            for j in range(5):
                block = fields[j, :, first : first + 128]
                if 4 * j + shift:
                    block = pltpu.roll(block, 4 * j + shift, 1)
                packed = jnp.where((lane >> 2) == j, block, packed)
            packed = jnp.concatenate([packed, jnp.zeros((112, 128), F32)], axis=0)
            ewsend[at] = packed.T[0:24]
            copy = pltpu.make_async_remote_copy(
                src_ref=ewsend.at[at], dst_ref=ewrecv.at[at],
                send_sem=ewsem.at[0, at], recv_sem=ewsem.at[1, at],
                device_id=peer, device_id_type=MESH,
            )
            ew_copies.append((copy, inside))

    with jax.named_scope("far"):
        for at in range(2):
            pl.semaphore_wait(known.at[at], 1)
        for copy, inside in ew_copies:
            pl.when(inside)(copy.start)

    with jax.named_scope("water_1"):
        lax.fori_loop(3, 6, strip, 0)
    with jax.named_scope("sum_x_0"):
        sum_x(0)
    with jax.named_scope("ghost_send"):
        here = pl.ds(pl.multiple_of((z * 4 + y) * 8, 8), 8)

        def ghost_copy(index):
            return pltpu.make_async_remote_copy(
                src_ref=gtotal, dst_ref=grecv.at[here],
                send_sem=gssem.at[index], recv_sem=grsem,
                device_id=(15, index * 2 + core), device_id_type=MESH,
            )

        @pl.when(x == 3)
        def _():
            total = gsend[...]
            for d in range(3):
                early_ghost(d).wait_recv()
                total = total + gearly[d]
            gtotal[...] = total
            for index in range(8):
                pl.when((row != 15) | (col != index * 2 + core))(ghost_copy(index).start)

    with jax.named_scope("sum_x_1"):
        sum_x(1)

    with jax.named_scope("more_water"):
        lax.fori_loop(6, 9, lambda at, carry: strip(at % 8, carry), 0)

    with jax.named_scope("selection"):
        @pl.when(is_edge)
        def _():
            at = lax.broadcasted_iota(jnp.int32, (128, 384), 1)
            column = col * 256 + jnp.where(at >= 320, at - 384, at)
            turned = jnp.concatenate(
                [cellbuf[...].astype(F32), jnp.zeros((96, 128), F32)], axis=0
            ).T.astype(jnp.int32)
            found = jnp.zeros((128, 384), F32)
            for block in range(32):
                found = jnp.where(turned[:, block : block + 1] == column, block + 1.0, found)
            onehot[...] = jnp.where(found > 0.0, 1.0, 0.0).astype(BF16)
            blocks[...] = jnp.broadcast_to(jnp.sum(found, axis=0, keepdims=True), (8, 384))

    with jax.named_scope("side_water"):
        for at, ((copy, _), inside) in enumerate(zip(ew_copies, (col < 15, col > 0))):
            pl.when(inside)(copy.wait_recv)

            @pl.when(~inside)
            def _():
                ewrecv[at] = jnp.zeros((24, 384), F32)

        from_east, from_west = ewrecv[0], ewrecv[1]
        for j in range(5):
            for at, piece in enumerate((from_west, ewsend[0], ewsend[1], from_east)):
                sides[j, at * 4 : at * 4 + 4] = piece[j * 4 : j * 4 + 4]
        state = [sides[j] for j in range(5)]
        values, rest = state[0:3], state[3:5]
        terms = face_terms(*rest, (0, 1))
        for _ in range(2):
            values = advance(*values, *rest, terms, (0, 1))
        turned = jnp.concatenate([*values, jnp.zeros((80, 384), F32)], axis=0).T[8:264]
        lane = lax.broadcasted_iota(jnp.int32, (256, 128), 1)
        for j, ref in enumerate((surf_o, flow_x_o, flow_y_o)):
            ref[:, 0:128] = jnp.where(
                lane < 2, pltpu.roll(turned, 124 - 16 * j, 1), ref[:, 0:128]
            )
            ref[:, 128:256] = jnp.where(
                lane >= 126, pltpu.roll(turned, 116 - 16 * j, 1), ref[:, 128:256]
            )

        @pl.when(is_edge)
        def _():
            blank = jnp.zeros((104, 256), F32)
            right, left_side = (
                jnp.concatenate([piece[:, 128:384], blank], axis=0).T[120:144]
                for piece in (from_east, from_west)
            )
            lane = lax.broadcasted_iota(jnp.int32, (24, 128), 1)
            for j in range(5):
                first = pltpu.roll(right, 128 - 4 * j, 1) if j else right
                wrapped = pltpu.roll(left_side, 124 - 4 * j, 1)
                tail[j] = jnp.where(lane < 2, first, jnp.where(lane >= 126, wrapped, 0.0))

    with jax.named_scope("sum_z"):
        total = zsend[z_hi, pl.ds(pl.multiple_of(z_lo * 8, 8), 8)]
        for d in range(1, 8):
            pltpu.make_async_copy(zrecv.at[d - 1], zrecv.at[d - 1], zsem.at[1, d - 1]).wait()
            total = total + zrecv[d - 1]
        series_o[...] = total

    with jax.named_scope("ghost"):
        @pl.when(is_edge)
        def _():
            grecv[here] = gtotal[...]
            pltpu.make_async_copy(
                grecv.at[pl.ds(0, 248)], grecv.at[pl.ds(0, 248)], grsem
            ).wait()
            value = grecv[0:32]
            for other_z in range(1, 8):
                value = value + grecv[other_z * 32 : other_z * 32 + 32]
            gpair[core] = value
            share = pltpu.make_async_remote_copy(
                src_ref=gpair.at[core], dst_ref=gpair.at[core],
                send_sem=gpsem.at[0], recv_sem=gpsem.at[1],
                device_id=partner, device_id_type=MESH,
            )
            share.start()
            share.wait_send()
            share.wait_recv()
            value = jnp.concatenate([gpair[0], gpair[1]], axis=0)
            picked = jnp.dot(
                jnp.concatenate(split_rows(value), axis=0), onehot[...],
                preferred_element_type=F32,
            )
            picked = picked[128:192] + picked[64:128] + picked[0:64]
            at = lax.broadcasted_iota(jnp.int32, (64, 384), 0)
            block = ((at >> 3) & 3) * 8 + (at & 2) * 2 + (at >> 5) * 2 + (at & 1)
            picked = jnp.where((block + 1).astype(F32) == blocks[0:1], picked, 0.0)
            ghost = [
                jnp.sum(jnp.where(((at >> 2) & 1) == step, picked, 0.0), axis=0, keepdims=True)
                for step in range(2)
            ]
            beyond = lax.broadcasted_iota(jnp.int32, (24, 384), 0) == 16
            state = [
                jnp.concatenate([fields[j, 248:272, :], tail[j]], axis=1) for j in range(5)
            ]
            rest = [jnp.where(beyond, 1.0, value) for value in state[3:5]]
            values = state[0:3]
            terms = face_terms(*rest)
            for step in range(2):
                values = [
                    jnp.where(beyond, ghost[step], values[0]),
                    jnp.where(beyond, 0.0, values[1]),
                    jnp.where(beyond, 0.0, values[2]),
                ]
                values = advance(*values, *rest, terms)
            for ref, value in zip((surf_o, flow_x_o, flow_y_o), values):
                ref[248:256, :] = value[8:16, 0:256]

    with jax.named_scope("drain"):
        for copy in [*dcopy.values(), *ycopy.values(), *xcopy.values()]:
            copy.wait_send()
        for copy, inside in [*ns_copies, *ew_copies]:
            pl.when(inside)(copy.wait_send)
        for part in range(2):
            for k in range(4):
                d, copy = z_copy(part, k)
                pl.when(d != 0)(copy.wait_send)
        pl.when(x < 3)(early_ghost(x).wait_send)

        @pl.when(x == 3)
        def _():
            for index in range(8):
                pl.when((row != 15) | (col != index * 2 + core))(ghost_copy(index).wait_send)


def write_out(*refs):
    sources, targets, sems = refs[0:4], refs[4:8], refs[8]
    copies = [
        pltpu.make_async_copy(source, target, sems.at[j])
        for j, (source, target) in enumerate(zip(sources, targets))
    ]
    for copy in copies:
        copy.start()
    for copy in copies:
        copy.wait()


def on_device(
    kernel_hat, coefficients, wave_speed_sq, wet_mask, boundary_cell, height, flux_x, flux_y
):
    field = jax.ShapeDtypeStruct((256, 256), F32)
    dma = pltpu.SemaphoreType.DMA
    shapes = (jax.ShapeDtypeStruct((8, 256), F32), field, field, field)
    operands = [
        pltpu.with_memory_space_constraint(value, pltpu.MemorySpace.HBM)
        for value in (
            kernel_hat.reshape(1024, 4096),
            coefficients.T,
            wave_speed_sq,
            wet_mask,
            boundary_cell.reshape(32, 128),
            height,
            flux_x,
            flux_y,
            jnp.asarray(transform_tables()),
        )
    ]
    results = pl.pallas_call(
        kernel,
        out_shape=shapes,
        in_specs=[pl.BlockSpec(memory_space=pltpu.MemorySpace.HBM)] * 9,
        out_specs=[pl.BlockSpec(memory_space=pltpu.VMEM)] * 4,
        scratch_shapes=[
            pltpu.VMEM((16, 1024, 256), BF16),
            pltpu.VMEM((128, 128), F32),
            pltpu.VMEM((32, 128), F32),
            pltpu.VMEM((256, 256), jnp.int32),
            pltpu.VMEM((32, 128), jnp.int32),
            pltpu.VMEM((32, 1024), BF16),
            pltpu.VMEM((2, 4, 32, 256), F32),
            pltpu.VMEM((2, 4, 32, 256), F32),
            pltpu.VMEM((2, 4, 32, 256), F32),
            pltpu.VMEM((2, 3, 32, 256), F32),
            pltpu.VMEM((2, 3, 32, 256), F32),
            pltpu.VMEM((2, 4, 32, 256), F32),
            pltpu.VMEM((2, 3, 32, 256), F32),
            pltpu.VMEM((2, 32, 256), F32),
            pltpu.VMEM((7, 8, 256), F32),
            pltpu.VMEM((8, 128), F32),
            pltpu.VMEM((3, 8, 128), F32),
            pltpu.VMEM((8, 128), F32),
            pltpu.VMEM((2, 32, 128), F32),
            pltpu.VMEM((256, 128), F32),
            pltpu.VMEM((5, 272, 256), F32),
            pltpu.VMEM((2, 24, 384), F32),
            pltpu.VMEM((2, 24, 384), F32),
            pltpu.VMEM((5, 16, 384), F32),
            pltpu.VMEM((5, 24, 128), F32),
            pltpu.VMEM((128, 384), BF16),
            pltpu.VMEM((8, 384), F32),
            pltpu.VMEM((128, 256), BF16),
            dma((16,)),
            dma((8,)),
            dma((2, 2)),
            dma((2, 2, 3)),
            dma((2, 2, 3)),
            dma((2, 8)),
            dma((4,)),
            dma((2,)),
            dma((8,)),
            dma(()),
            dma((2, 2)),
            dma((2, 2)),
            pltpu.SemaphoreType.REGULAR((2,)),
        ],
        compiler_params=pltpu.CompilerParams(
            collective_id=0, has_side_effects=True, vmem_limit_bytes=48 * 1024 * 1024
        ),
    )(*operands)
    return pl.pallas_call(
        write_out,
        out_shape=shapes,
        in_specs=[pl.BlockSpec(memory_space=pltpu.VMEM)] * 4,
        out_specs=[pl.BlockSpec(memory_space=pltpu.MemorySpace.HBM)] * 4,
        scratch_shapes=[dma((4,))],
        compiler_params=pltpu.CompilerParams(vmem_limit_bytes=16 * 1024 * 1024),
    )(*results)


def solution(mesh):
    return jax.shard_map(
        on_device,
        mesh=mesh,
        in_specs=(
            P(None, "rows", "cols", None),
            P(None, "cols"),
            P("rows", "cols"),
            P("rows", "cols"),
            P(),
            P("rows", "cols"),
            P("rows", "cols"),
            P("rows", "cols"),
        ),
        out_specs=(P("rows", "cols"), P("rows", "cols"), P("rows", "cols"), P("rows", "cols")),
        check_vma=False,
    )
```

```python
import functools

import jax
import jax.numpy as jnp
import numpy as np
from jax import lax
from jax.experimental import pallas as pl
from jax.experimental.pallas import tpu as pltpu
from jax.sharding import PartitionSpec as P

F32 = jnp.float32
BF16 = jnp.bfloat16
HIGH = lax.Precision.HIGHEST
MESH = pl.DeviceIdType.MESH
ORDER = (2, 1, 3, 0)
LOADS = (0, 4, 8, 12, 1, 5, 9, 13, 2, 6, 10, 14, 3, 7, 11, 15)


def transform_tables():
    table = np.zeros((16, 128, 128), np.float32)
    times = np.arange(128)
    inner = times.reshape(4, 4, 8).transpose(1, 0, 2).reshape(-1)
    for row in range(16):
        freqs = row * 16 + np.arange(16)
        angle = 2.0 * np.pi * ((freqs[:, None] * inner[None, :]) % 256) / 256.0
        table[row, 0:16] = np.cos(angle) / 256.0
        table[row, 16:32] = -np.sin(angle) / 256.0
        angle = 2.0 * np.pi * ((freqs[:, None] * times[None, :]) % 256) / 256.0
        table[row, 32:48] = np.cos(angle)
        table[row, 48:64] = -np.sin(angle)
        table[row, 64:80] = np.sin(angle)
        table[row, 80:96] = np.cos(angle)
    return table


def after(values, axis):
    return pltpu.roll(values, values.shape[axis] - 1, axis)


def before(values, axis):
    return pltpu.roll(values, 1, axis)


def split_rows(value):
    high = value.astype(BF16)
    value = value - high.astype(F32)
    middle = value.astype(BF16)
    return [high, middle, (value - middle.astype(F32)).astype(BF16)]


def face_terms(speed, wet, axes=(1, 0)):
    celerity = jnp.sqrt(speed)
    terms = []
    for axis in axes:
        opened = wet * after(wet, axis)
        terms.append((0.5 * opened, opened * (0.25 * (celerity + after(celerity, axis)))))
    return terms


def advance(surface, along_x, along_y, speed, wet, terms, axes=(1, 0)):
    pressure = speed * surface
    changes = []
    for axis, along, across, (half, damp) in zip(
        axes, (along_x, along_y), (along_y, along_x), terms
    ):
        next_along = after(along, axis)
        mass = half * (along + next_along) - damp * (after(surface, axis) - surface)
        push = half * (pressure + after(pressure, axis)) - damp * (next_along - along)
        shear = damp * (across - after(across, axis))
        changes.append(tuple(flux - before(flux, axis) for flux in (mass, push, shear)))
    (mass_x, push_x, shear_x), (mass_y, push_y, shear_y) = changes
    return (
        wet * (surface - 0.25 * (mass_x + mass_y)),
        wet * (along_x - 0.25 * (push_x + shear_y)),
        wet * (along_y - 0.25 * (shear_x + push_y)),
    )


def kernel(
    kern, coef, speed, mask, cells, surf, flow_x, flow_y, table,
    series_o, surf_o, flow_x_o, flow_y_o,
    kbuf, tab, cbuf, mbuf, cellbuf, left, own, dsend, drecv, ysend, yrecv,
    xsend, xrecv, zsend, zrecv, gsend, gearly, gtotal, gpair, grecv, fields, ewsend, ewrecv, sides, tail, onehot, blocks, wide,
    ksem, lsem, bsem, dsem, ysem, xsem, zsem, gxsem, gpsem, gssem, grsem, nssem, ewsem, known,
):
    row, col = lax.axis_index("rows"), lax.axis_index("cols")
    x, z_lo = row % 4, row // 4
    y, z_hi, core = col // 4, (col // 2) % 2, col % 2
    z = z_hi * 4 + z_lo
    is_edge = row == 15

    def place(at_x, at_y, at_z, at_core):
        return ((at_z % 4) * 4 + at_x, at_y * 4 + (at_z // 4) * 2 + at_core)

    partner = place(x, y, z, 1 - core)
    y_peer = [place(x, (y + d) % 4, z, core) for d in range(4)]
    x_peer = [place((x + d) % 4, y, z, core) for d in range(4)]
    z_peer = [place(x, y, (z + d) % 8, core) for d in range(8)]
    north, south = ((row + 15) % 16, col), ((row + 1) % 16, col)
    west, east = (row, (col + 15) % 16), (row, (col + 1) % 16)

    with jax.named_scope("start_loads"):
        local = [
            pltpu.make_async_copy(
                table.at[row, pl.ds(32, 64)], tab.at[pl.ds(32, 64)], lsem.at[0]
            ),
            pltpu.make_async_copy(coef, cbuf, lsem.at[1]),
            pltpu.make_async_copy(table.at[row, pl.ds(0, 32)], tab.at[pl.ds(0, 32)], lsem.at[8]),
        ]
        for copy in local[0:2]:
            copy.start()
        loads = []
        for i, d in enumerate(ORDER):
            for side, par in enumerate((1 - core, core)):
                for part in range(2):
                    slot = i * 4 + side * 2 + part
                    start = pl.multiple_of(((((y + d) % 4) * 2 + part) * 2 + par) * 256, 256)
                    loads.append(
                        pltpu.make_async_copy(
                            kern.at[:, pl.ds(start, 256)], kbuf.at[slot], ksem.at[slot]
                        )
                    )
        for slot in LOADS[0:4]:
            loads[slot].start()

    with jax.named_scope("greet_peers"):
        barrier = pltpu.get_barrier_semaphore()
        near = [partner, *y_peer[1:], *x_peer[1:], *(z_peer[d] for d in (1, 2, 6, 7))]
        for peer in near:
            pl.semaphore_signal(barrier, inc=1, device_id=peer, device_id_type=MESH)
        greetings = len(near)
        for peer, inside in ((north, row > 0), (south, row < 15)):
            greetings = greetings + inside.astype(jnp.int32)

            @pl.when(inside)
            def _():
                pl.semaphore_signal(barrier, inc=1, device_id=peer, device_id_type=MESH)

    with jax.named_scope("more_loads"):
        for slot in LOADS[4:8]:
            loads[slot].start()
        sources = (surf, flow_x, flow_y, speed)
        borders = []
        for side, (source, target) in enumerate(((0, 8), (248, 256))):
            for j in range(5):
                at = bsem.at[side * 5 + j]
                if j < 4:
                    copy = pltpu.make_async_copy(
                        sources[j].at[pl.ds(source, 8)], fields.at[j, pl.ds(target, 8)], at
                    )
                else:
                    copy = pltpu.make_async_copy(
                        mask.at[pl.ds(source, 8)], mbuf.at[pl.ds(source, 8)], at
                    )
                borders.append(copy)
        for copy in borders:
            copy.start()
        middle = pl.ds(8, 240)
        grids = [
            pltpu.make_async_copy(ref.at[middle], fields.at[j, pl.ds(16, 240)], lsem.at[2 + j])
            for j, ref in enumerate(sources)
        ]
        grids += [
            pltpu.make_async_copy(mask.at[middle], mbuf.at[middle], lsem.at[6]),
            pltpu.make_async_copy(cells, cellbuf, lsem.at[7]),
        ]

    with jax.named_scope("wait_coef"):
        for slot in LOADS[8:]:
            loads[slot].start()
        for copy in [*grids, local[2]]:
            copy.start()
        local[0].wait()
    with jax.named_scope("wait_table"):
        local[1].wait()

    with jax.named_scope("build_left"):
        tiled = lax.dot_general(
            tab[32:96], jnp.concatenate([cbuf[...]] * 16, axis=0), (((1,), (1,)), ((), ())),
            precision=HIGH, preferred_element_type=F32,
        )
        lanes = lax.broadcasted_iota(jnp.int32, (32, 512), 1)
        subs = lax.broadcasted_iota(jnp.int32, (32, 512), 0)
        diagonal = (lanes >> 5) == (subs & 15)
        left[:, 0:512] = jnp.where(diagonal, tiled[0:32], 0.0).astype(BF16)
        left[:, 512:1024] = jnp.where(diagonal, tiled[32:64], 0.0).astype(BF16)

        dcopy, ycopy, xcopy = {}, {}, {}

        def products(part, side, target):
            for i in range(4):
                loads[i * 4 + side * 2 + part].wait()
            for i in range(4):
                target[part, i] = jnp.dot(
                    left[...], kbuf[i * 4 + side * 2 + part], preferred_element_type=F32
                )

        def to_partner(part):
            dcopy[part] = pltpu.make_async_remote_copy(
                src_ref=dsend.at[part], dst_ref=drecv.at[part],
                send_sem=dsem.at[0, part], recv_sem=dsem.at[1, part],
                device_id=partner, device_id_type=MESH,
            )
            dcopy[part].start()

        def merge(part):
            dcopy[part].wait_recv()
            for i, d in enumerate(ORDER):
                total = own[part, i] + drecv[part, i]
                if d == 0:
                    own[part, i] = total
                    continue
                ysend[part, d - 1] = total
                ycopy[part, d] = pltpu.make_async_remote_copy(
                    src_ref=ysend.at[part, d - 1], dst_ref=yrecv.at[part, d - 1],
                    send_sem=ysem.at[0, part, d - 1], recv_sem=ysem.at[1, part, d - 1],
                    device_id=y_peer[d], device_id_type=MESH,
                )
                ycopy[part, d].start()

        def early_ghost(d):
            return pltpu.make_async_remote_copy(
                src_ref=gsend, dst_ref=gearly.at[d],
                send_sem=gxsem.at[0], recv_sem=gxsem.at[1 + d],
                device_id=place(3, y, z, core), device_id_type=MESH,
            )

        def ahead(part, partial):
            for step in range(2):
                for half in range(2):
                    at = step * 4 + part * 2 + half
                    line = 126 + step
                    gsend[at : at + 1] = partial[line : line + 1, half * 128 : half * 128 + 128]
            if part == 1:
                pl.when(x < 3)(early_ghost(x).start)

        def sum_y(part):
            total = own[part, 3]
            for d in (1, 3, 2):
                ycopy[part, d].wait_recv()
                total = total + yrecv[part, d - 1]
            split = split_rows(total)
            stack = jnp.concatenate([split[k] for k in (0, 1, 0, 2, 0, 1)], axis=0)
            partial = jnp.dot(wide[:, 0:192], stack, preferred_element_type=F32)
            for at in range(4):
                xsend[part, at] = partial[at * 32 : at * 32 + 32]
            ahead(part, partial)
            for d in (2, 1, 3):
                xcopy[part, d] = pltpu.make_async_remote_copy(
                    src_ref=xsend.at[part, (x + d) % 4], dst_ref=xrecv.at[part, d - 1],
                    send_sem=xsem.at[0, part, d - 1], recv_sem=xsem.at[1, part, d - 1],
                    device_id=x_peer[d], device_id_type=MESH,
                )
                xcopy[part, d].start()

        def z_copy(part, k):
            lo = (z_lo + k) % 4
            d = (part * 4 + lo + 8 - z) % 8
            at = (d + 7) % 8
            return d, pltpu.make_async_remote_copy(
                src_ref=zsend.at[part, pl.ds(pl.multiple_of(lo * 8, 8), 8)],
                dst_ref=zrecv.at[at],
                send_sem=zsem.at[0, at], recv_sem=zsem.at[1, at],
                device_id=place(x, y, part * 4 + lo, core), device_id_type=MESH,
            )

        def sum_x(part):
            total = xsend[part, x]
            for d in (1, 3, 2):
                xcopy[part, d].wait_recv()
                total = total + xrecv[part, d - 1]
            zsend[part] = total
            for k in (2, 1, 3, 0):
                d, copy = z_copy(part, k)
                if k == 0:
                    pl.when(d != 0)(copy.start)
                else:
                    copy.start()

        def strip(at, carry):
            base = pl.multiple_of(at * 32, 8)
            state = [fields[j, pl.ds(base, 48), :] for j in range(5)]
            values, rest = state[0:3], state[3:5]
            terms = face_terms(*rest)
            for _ in range(2):
                values = advance(*values, *rest, terms)
            for ref, value in zip((surf_o, flow_x_o, flow_y_o), values):
                ref[pl.ds(base, 32), :] = value[8:40]
            return carry

    with jax.named_scope("spectrum"):
        products(0, 0, dsend)
    with jax.named_scope("barrier"):
        pl.semaphore_wait(barrier, greetings)
    with jax.named_scope("spectrum_1"):
        to_partner(0)
        products(1, 0, dsend)
        to_partner(1)
    with jax.named_scope("row_halos"):
        for copy in borders:
            copy.wait()
        for source in (0, 248):
            fields[4, source + 8 : source + 16, :] = mbuf[source : source + 8].astype(F32)
        ns_copies = []
        for at, (first, last, peer, inside) in enumerate(
            ((8, 264, north, row > 0), (256, 0, south, row < 15))
        ):
            copy = pltpu.make_async_remote_copy(
                src_ref=fields.at[:, pl.ds(first, 8)],
                dst_ref=fields.at[:, pl.ds(last, 8)],
                send_sem=nssem.at[0, at], recv_sem=nssem.at[1, at],
                device_id=peer, device_id_type=MESH,
            )
            pl.when(inside)(copy.start)
            ns_copies.append((copy, inside))
    with jax.named_scope("spectrum_2"):
        products(0, 1, own)
    with jax.named_scope("merge_0"):
        merge(0)
        for d in range(1, 4):
            pl.semaphore_signal(known.at[d + 1], inc=1, device_id=y_peer[d], device_id_type=MESH)
    with jax.named_scope("spectrum_3"):
        products(1, 1, own)
    with jax.named_scope("merge_1"):
        merge(1)

    with jax.named_scope("widen"):
        local[2].wait()
        split = split_rows(tab[0:32])
        wide[...] = jnp.concatenate(
            [*(split[k].astype(F32) for k in (0, 0, 1, 0, 2, 1)), jnp.zeros((64, 128), F32)], axis=0
        ).T.astype(BF16)
        for copy in grids:
            copy.wait()
        fields[4, 16:256, :] = mbuf[8:248].astype(F32)

    with jax.named_scope("water"):
        lax.fori_loop(1, 3, strip, 0)
    with jax.named_scope("relay"):
        for d in range(1, 4):
            pl.semaphore_wait(known.at[d + 1], 1)
        for at, d in enumerate((2, 6)):
            pl.semaphore_signal(known.at[at], inc=1, device_id=z_peer[d], device_id_type=MESH)

    with jax.named_scope("sum_y_0"):
        sum_y(0)

    with jax.named_scope("sum_y_1"):
        sum_y(1)

    with jax.named_scope("column_halos"):
        pl.when(row < 15)(ns_copies[0][0].wait_recv)
        pl.when(row > 0)(ns_copies[1][0].wait_recv)

        @pl.when(row == 0)
        def _():
            fields[:, 0:8, :] = jnp.zeros((5, 8, 256), F32)

        @pl.when(is_edge)
        def _():
            fields[:, 264:272, :] = jnp.zeros((5, 8, 256), F32)

        lane = lax.broadcasted_iota(jnp.int32, (272, 128), 1)
        ew_copies = []
        for at, (first, shift, peer, inside) in enumerate(
            ((0, 0, west, col > 0), (128, 4, east, col < 15))
        ):
            packed = jnp.zeros((272, 128), F32)
            for j in range(5):
                block = fields[j, :, first : first + 128]
                if 4 * j + shift:
                    block = pltpu.roll(block, 4 * j + shift, 1)
                packed = jnp.where((lane >> 2) == j, block, packed)
            packed = jnp.concatenate([packed, jnp.zeros((112, 128), F32)], axis=0)
            ewsend[at] = packed.T[0:24]
            copy = pltpu.make_async_remote_copy(
                src_ref=ewsend.at[at], dst_ref=ewrecv.at[at],
                send_sem=ewsem.at[0, at], recv_sem=ewsem.at[1, at],
                device_id=peer, device_id_type=MESH,
            )
            ew_copies.append((copy, inside))

    with jax.named_scope("far"):
        for at in range(2):
            pl.semaphore_wait(known.at[at], 1)
        for copy, inside in ew_copies:
            pl.when(inside)(copy.start)

    with jax.named_scope("water_1"):
        lax.fori_loop(3, 6, strip, 0)
    with jax.named_scope("sum_x_0"):
        sum_x(0)
    with jax.named_scope("ghost_send"):
        here = pl.ds(pl.multiple_of((z * 4 + y) * 8, 8), 8)

        def ghost_copy(index):
            return pltpu.make_async_remote_copy(
                src_ref=gtotal, dst_ref=grecv.at[here],
                send_sem=gssem.at[index], recv_sem=grsem,
                device_id=(15, index * 2 + core), device_id_type=MESH,
            )

        @pl.when(x == 3)
        def _():
            total = gsend[...]
            for d in range(3):
                early_ghost(d).wait_recv()
                total = total + gearly[d]
            gtotal[...] = total
            for index in range(8):
                pl.when((row != 15) | (col != index * 2 + core))(ghost_copy(index).start)

    with jax.named_scope("sum_x_1"):
        sum_x(1)

    with jax.named_scope("more_water"):
        lax.fori_loop(6, 9, lambda at, carry: strip(at % 8, carry), 0)

    with jax.named_scope("selection"):
        @pl.when(is_edge)
        def _():
            at = lax.broadcasted_iota(jnp.int32, (128, 384), 1)
            column = col * 256 + jnp.where(at >= 320, at - 384, at)
            turned = jnp.concatenate(
                [cellbuf[...].astype(F32), jnp.zeros((96, 128), F32)], axis=0
            ).T.astype(jnp.int32)
            found = jnp.zeros((128, 384), F32)
            for block in range(32):
                found = jnp.where(turned[:, block : block + 1] == column, block + 1.0, found)
            onehot[...] = jnp.where(found > 0.0, 1.0, 0.0).astype(BF16)
            blocks[...] = jnp.broadcast_to(jnp.sum(found, axis=0, keepdims=True), (8, 384))

    with jax.named_scope("side_water"):
        for at, ((copy, _), inside) in enumerate(zip(ew_copies, (col < 15, col > 0))):
            pl.when(inside)(copy.wait_recv)

            @pl.when(~inside)
            def _():
                ewrecv[at] = jnp.zeros((24, 384), F32)

        from_east, from_west = ewrecv[0], ewrecv[1]
        for j in range(5):
            for at, piece in enumerate((from_west, ewsend[0], ewsend[1], from_east)):
                sides[j, at * 4 : at * 4 + 4] = piece[j * 4 : j * 4 + 4]
        state = [sides[j] for j in range(5)]
        values, rest = state[0:3], state[3:5]
        terms = face_terms(*rest, (0, 1))
        for _ in range(2):
            values = advance(*values, *rest, terms, (0, 1))
        turned = jnp.concatenate([*values, jnp.zeros((80, 384), F32)], axis=0).T[8:264]
        lane = lax.broadcasted_iota(jnp.int32, (256, 128), 1)
        for j, ref in enumerate((surf_o, flow_x_o, flow_y_o)):
            ref[:, 0:128] = jnp.where(
                lane < 2, pltpu.roll(turned, 124 - 16 * j, 1), ref[:, 0:128]
            )
            ref[:, 128:256] = jnp.where(
                lane >= 126, pltpu.roll(turned, 116 - 16 * j, 1), ref[:, 128:256]
            )

        @pl.when(is_edge)
        def _():
            blank = jnp.zeros((104, 256), F32)
            right, left_side = (
                jnp.concatenate([piece[:, 128:384], blank], axis=0).T[120:144]
                for piece in (from_east, from_west)
            )
            lane = lax.broadcasted_iota(jnp.int32, (24, 128), 1)
            for j in range(5):
                first = pltpu.roll(right, 128 - 4 * j, 1) if j else right
                wrapped = pltpu.roll(left_side, 124 - 4 * j, 1)
                tail[j] = jnp.where(lane < 2, first, jnp.where(lane >= 126, wrapped, 0.0))

    with jax.named_scope("sum_z"):
        total = zsend[z_hi, pl.ds(pl.multiple_of(z_lo * 8, 8), 8)]
        for d in range(1, 8):
            pltpu.make_async_copy(zrecv.at[d - 1], zrecv.at[d - 1], zsem.at[1, d - 1]).wait()
            total = total + zrecv[d - 1]
        series_o[...] = total

    with jax.named_scope("ghost"):
        @pl.when(is_edge)
        def _():
            grecv[here] = gtotal[...]
            pltpu.make_async_copy(
                grecv.at[pl.ds(0, 248)], grecv.at[pl.ds(0, 248)], grsem
            ).wait()
            value = grecv[0:32]
            for other_z in range(1, 8):
                value = value + grecv[other_z * 32 : other_z * 32 + 32]
            gpair[core] = value
            share = pltpu.make_async_remote_copy(
                src_ref=gpair.at[core], dst_ref=gpair.at[core],
                send_sem=gpsem.at[0], recv_sem=gpsem.at[1],
                device_id=partner, device_id_type=MESH,
            )
            share.start()
            share.wait_send()
            share.wait_recv()
            value = jnp.concatenate([gpair[0], gpair[1]], axis=0)
            picked = jnp.dot(
                jnp.concatenate(split_rows(value), axis=0), onehot[...],
                preferred_element_type=F32,
            )
            picked = picked[128:192] + picked[64:128] + picked[0:64]
            at = lax.broadcasted_iota(jnp.int32, (64, 384), 0)
            block = ((at >> 3) & 3) * 8 + (at & 2) * 2 + (at >> 5) * 2 + (at & 1)
            picked = jnp.where((block + 1).astype(F32) == blocks[0:1], picked, 0.0)
            ghost = [
                jnp.sum(jnp.where(((at >> 2) & 1) == step, picked, 0.0), axis=0, keepdims=True)
                for step in range(2)
            ]
            beyond = lax.broadcasted_iota(jnp.int32, (24, 384), 0) == 16
            state = [
                jnp.concatenate([fields[j, 248:272, :], tail[j]], axis=1) for j in range(5)
            ]
            rest = [jnp.where(beyond, 1.0, value) for value in state[3:5]]
            values = state[0:3]
            terms = face_terms(*rest)
            for step in range(2):
                values = [
                    jnp.where(beyond, ghost[step], values[0]),
                    jnp.where(beyond, 0.0, values[1]),
                    jnp.where(beyond, 0.0, values[2]),
                ]
                values = advance(*values, *rest, terms)
            for ref, value in zip((surf_o, flow_x_o, flow_y_o), values):
                ref[248:256, :] = value[8:16, 0:256]

    with jax.named_scope("drain"):
        for copy in [*dcopy.values(), *ycopy.values(), *xcopy.values()]:
            copy.wait_send()
        for copy, inside in [*ns_copies, *ew_copies]:
            pl.when(inside)(copy.wait_send)
        for part in range(2):
            for k in range(4):
                d, copy = z_copy(part, k)
                pl.when(d != 0)(copy.wait_send)
        pl.when(x < 3)(early_ghost(x).wait_send)

        @pl.when(x == 3)
        def _():
            for index in range(8):
                pl.when((row != 15) | (col != index * 2 + core))(ghost_copy(index).wait_send)


def write_out(*refs):
    sources, targets, sems = refs[0:4], refs[4:8], refs[8]
    copies = [
        pltpu.make_async_copy(source, target, sems.at[j])
        for j, (source, target) in enumerate(zip(sources, targets))
    ]
    for copy in copies:
        copy.start()
    for copy in copies:
        copy.wait()


def on_device(
    kernel_hat, coefficients, wave_speed_sq, wet_mask, boundary_cell, height, flux_x, flux_y
):
    field = jax.ShapeDtypeStruct((256, 256), F32)
    dma = pltpu.SemaphoreType.DMA
    shapes = (jax.ShapeDtypeStruct((8, 256), F32), field, field, field)
    operands = [
        pltpu.with_memory_space_constraint(value, pltpu.MemorySpace.HBM)
        for value in (
            kernel_hat.reshape(1024, 4096),
            coefficients.T,
            wave_speed_sq,
            wet_mask,
            boundary_cell.reshape(32, 128),
            height,
            flux_x,
            flux_y,
            jnp.asarray(transform_tables()),
        )
    ]
    results = pl.pallas_call(
        kernel,
        out_shape=shapes,
        in_specs=[pl.BlockSpec(memory_space=pltpu.MemorySpace.HBM)] * 9,
        out_specs=[pl.BlockSpec(memory_space=pltpu.VMEM)] * 4,
        scratch_shapes=[
            pltpu.VMEM((16, 1024, 256), BF16),
            pltpu.VMEM((128, 128), F32),
            pltpu.VMEM((32, 128), F32),
            pltpu.VMEM((256, 256), jnp.int32),
            pltpu.VMEM((32, 128), jnp.int32),
            pltpu.VMEM((32, 1024), BF16),
            pltpu.VMEM((2, 4, 32, 256), F32),
            pltpu.VMEM((2, 4, 32, 256), F32),
            pltpu.VMEM((2, 4, 32, 256), F32),
            pltpu.VMEM((2, 3, 32, 256), F32),
            pltpu.VMEM((2, 3, 32, 256), F32),
            pltpu.VMEM((2, 4, 32, 256), F32),
            pltpu.VMEM((2, 3, 32, 256), F32),
            pltpu.VMEM((2, 32, 256), F32),
            pltpu.VMEM((7, 8, 256), F32),
            pltpu.VMEM((8, 128), F32),
            pltpu.VMEM((3, 8, 128), F32),
            pltpu.VMEM((8, 128), F32),
            pltpu.VMEM((2, 32, 128), F32),
            pltpu.VMEM((256, 128), F32),
            pltpu.VMEM((5, 272, 256), F32),
            pltpu.VMEM((2, 24, 384), F32),
            pltpu.VMEM((2, 24, 384), F32),
            pltpu.VMEM((5, 16, 384), F32),
            pltpu.VMEM((5, 24, 128), F32),
            pltpu.VMEM((128, 384), BF16),
            pltpu.VMEM((8, 384), F32),
            pltpu.VMEM((128, 256), BF16),
            dma((16,)),
            dma((9,)),
            dma((10,)),
            dma((2, 2)),
            dma((2, 2, 3)),
            dma((2, 2, 3)),
            dma((2, 8)),
            dma((4,)),
            dma((2,)),
            dma((8,)),
            dma(()),
            dma((2, 2)),
            dma((2, 2)),
            pltpu.SemaphoreType.REGULAR((5,)),
        ],
        compiler_params=pltpu.CompilerParams(
            collective_id=0, has_side_effects=True, vmem_limit_bytes=48 * 1024 * 1024
        ),
    )(*operands)
    return pl.pallas_call(
        write_out,
        out_shape=shapes,
        in_specs=[pl.BlockSpec(memory_space=pltpu.VMEM)] * 4,
        out_specs=[pl.BlockSpec(memory_space=pltpu.MemorySpace.HBM)] * 4,
        scratch_shapes=[dma((4,))],
        compiler_params=pltpu.CompilerParams(vmem_limit_bytes=16 * 1024 * 1024),
    )(*results)


def solution(mesh):
    return jax.shard_map(
        on_device,
        mesh=mesh,
        in_specs=(
            P(None, "rows", "cols", None),
            P(None, "cols"),
            P("rows", "cols"),
            P("rows", "cols"),
            P(),
            P("rows", "cols"),
            P("rows", "cols"),
            P("rows", "cols"),
        ),
        out_specs=(P("rows", "cols"), P("rows", "cols"), P("rows", "cols"), P("rows", "cols")),
        check_vma=False,
    )
```

```python
import functools

import jax
import jax.numpy as jnp
import numpy as np
from jax import lax
from jax.experimental import pallas as pl
from jax.experimental.pallas import tpu as pltpu
from jax.sharding import PartitionSpec as P

F32 = jnp.float32
BF16 = jnp.bfloat16
HIGH = lax.Precision.HIGHEST
MESH = pl.DeviceIdType.MESH
ORDER = (2, 1, 3, 0)
LOADS = (0, 4, 8, 12, 2, 6, 10, 14, 1, 5, 9, 13, 3, 7, 11, 15)


def transform_tables():
    table = np.zeros((16, 128, 128), np.float32)
    times = np.arange(128)
    inner = times.reshape(4, 4, 8).transpose(1, 0, 2).reshape(-1)
    for row in range(16):
        freqs = row * 16 + np.arange(16)
        angle = 2.0 * np.pi * ((freqs[:, None] * inner[None, :]) % 256) / 256.0
        table[row, 0:16] = np.cos(angle) / 256.0
        table[row, 16:32] = -np.sin(angle) / 256.0
        angle = 2.0 * np.pi * ((freqs[:, None] * times[None, :]) % 256) / 256.0
        table[row, 32:48] = np.cos(angle)
        table[row, 48:64] = -np.sin(angle)
        table[row, 64:80] = np.sin(angle)
        table[row, 80:96] = np.cos(angle)
    return table


def after(values, axis):
    return pltpu.roll(values, values.shape[axis] - 1, axis)


def before(values, axis):
    return pltpu.roll(values, 1, axis)


def split_rows(value):
    high = value.astype(BF16)
    value = value - high.astype(F32)
    middle = value.astype(BF16)
    return [high, middle, (value - middle.astype(F32)).astype(BF16)]


def face_terms(speed, wet, axes=(1, 0)):
    celerity = jnp.sqrt(speed)
    terms = []
    for axis in axes:
        opened = wet * after(wet, axis)
        terms.append((0.5 * opened, opened * (0.25 * (celerity + after(celerity, axis)))))
    return terms


def advance(surface, along_x, along_y, speed, wet, terms, axes=(1, 0)):
    pressure = speed * surface
    changes = []
    for axis, along, across, (half, damp) in zip(
        axes, (along_x, along_y), (along_y, along_x), terms
    ):
        next_along = after(along, axis)
        mass = half * (along + next_along) - damp * (after(surface, axis) - surface)
        push = half * (pressure + after(pressure, axis)) - damp * (next_along - along)
        shear = damp * (across - after(across, axis))
        changes.append(tuple(flux - before(flux, axis) for flux in (mass, push, shear)))
    (mass_x, push_x, shear_x), (mass_y, push_y, shear_y) = changes
    return (
        wet * (surface - 0.25 * (mass_x + mass_y)),
        wet * (along_x - 0.25 * (push_x + shear_y)),
        wet * (along_y - 0.25 * (shear_x + push_y)),
    )


def kernel(
    kern, coef, speed, mask, cells, surf, flow_x, flow_y, table,
    series_o, surf_o, flow_x_o, flow_y_o,
    kbuf, tab, cbuf, mbuf, cellbuf, left, own, dsend, drecv, ysend, yrecv,
    xsend, xrecv, zsend, zrecv, gsend, gearly, gtotal, gpair, grecv, fields, ewsend, ewrecv, sides, tail, onehot, blocks, wide,
    ksem, lsem, bsem, dsem, ysem, xsem, zsem, gxsem, gpsem, gssem, grsem, nssem, ewsem, known,
):
    row, col = lax.axis_index("rows"), lax.axis_index("cols")
    x, z_lo = row % 4, row // 4
    y, z_hi, core = col // 4, (col // 2) % 2, col % 2
    z = z_hi * 4 + z_lo
    is_edge = row == 15

    def place(at_x, at_y, at_z, at_core):
        return ((at_z % 4) * 4 + at_x, at_y * 4 + (at_z // 4) * 2 + at_core)

    partner = place(x, y, z, 1 - core)
    y_peer = [place(x, (y + d) % 4, z, core) for d in range(4)]
    x_peer = [place((x + d) % 4, y, z, core) for d in range(4)]
    z_peer = [place(x, y, (z + d) % 8, core) for d in range(8)]
    north, south = ((row + 15) % 16, col), ((row + 1) % 16, col)
    west, east = (row, (col + 15) % 16), (row, (col + 1) % 16)

    with jax.named_scope("start_loads"):
        local = [
            pltpu.make_async_copy(
                table.at[row, pl.ds(32, 64)], tab.at[pl.ds(32, 64)], lsem.at[0]
            ),
            pltpu.make_async_copy(coef, cbuf, lsem.at[1]),
            pltpu.make_async_copy(table.at[row, pl.ds(0, 32)], tab.at[pl.ds(0, 32)], lsem.at[8]),
        ]
        for copy in local[0:2]:
            copy.start()
        loads = []
        for i, d in enumerate(ORDER):
            for side, par in enumerate((1 - core, core)):
                for part in range(2):
                    slot = i * 4 + side * 2 + part
                    start = pl.multiple_of(((((y + d) % 4) * 2 + part) * 2 + par) * 256, 256)
                    loads.append(
                        pltpu.make_async_copy(
                            kern.at[:, pl.ds(start, 256)], kbuf.at[slot], ksem.at[slot]
                        )
                    )
        for slot in LOADS[0:4]:
            loads[slot].start()

    with jax.named_scope("greet_peers"):
        barrier = pltpu.get_barrier_semaphore()
        near = [partner, *y_peer[1:], *x_peer[1:], *(z_peer[d] for d in (1, 2, 6, 7))]
        for peer in near:
            pl.semaphore_signal(barrier, inc=1, device_id=peer, device_id_type=MESH)
        greetings = len(near)
        for peer, inside in ((north, row > 0), (south, row < 15)):
            greetings = greetings + inside.astype(jnp.int32)

            @pl.when(inside)
            def _():
                pl.semaphore_signal(barrier, inc=1, device_id=peer, device_id_type=MESH)

    with jax.named_scope("more_loads"):
        for slot in LOADS[4:8]:
            loads[slot].start()
        sources = (surf, flow_x, flow_y, speed)
        borders = []
        for side, (source, target) in enumerate(((0, 8), (248, 256))):
            for j in range(5):
                at = bsem.at[side * 5 + j]
                if j < 4:
                    copy = pltpu.make_async_copy(
                        sources[j].at[pl.ds(source, 8)], fields.at[j, pl.ds(target, 8)], at
                    )
                else:
                    copy = pltpu.make_async_copy(
                        mask.at[pl.ds(source, 8)], mbuf.at[pl.ds(source, 8)], at
                    )
                borders.append(copy)
        for copy in borders:
            copy.start()
        middle = pl.ds(8, 240)
        grids = [
            pltpu.make_async_copy(ref.at[middle], fields.at[j, pl.ds(16, 240)], lsem.at[2 + j])
            for j, ref in enumerate(sources)
        ]
        grids += [
            pltpu.make_async_copy(mask.at[middle], mbuf.at[middle], lsem.at[6]),
            pltpu.make_async_copy(cells, cellbuf, lsem.at[7]),
        ]

    with jax.named_scope("wait_coef"):
        for slot in LOADS[8:]:
            loads[slot].start()
        for copy in [*grids, local[2]]:
            copy.start()
        local[0].wait()
    with jax.named_scope("wait_table"):
        local[1].wait()

    with jax.named_scope("build_left"):
        tiled = lax.dot_general(
            tab[32:96], jnp.concatenate([cbuf[...]] * 16, axis=0), (((1,), (1,)), ((), ())),
            precision=HIGH, preferred_element_type=F32,
        )
        lanes = lax.broadcasted_iota(jnp.int32, (32, 512), 1)
        subs = lax.broadcasted_iota(jnp.int32, (32, 512), 0)
        diagonal = (lanes >> 5) == (subs & 15)
        left[:, 0:512] = jnp.where(diagonal, tiled[0:32], 0.0).astype(BF16)
        left[:, 512:1024] = jnp.where(diagonal, tiled[32:64], 0.0).astype(BF16)

        dcopy, ycopy, xcopy = {}, {}, {}

        def products(part, side, target):
            for i in range(4):
                loads[i * 4 + side * 2 + part].wait()
            for i in range(4):
                target[part, i] = jnp.dot(
                    left[...], kbuf[i * 4 + side * 2 + part], preferred_element_type=F32
                )

        def to_partner(part):
            dcopy[part] = pltpu.make_async_remote_copy(
                src_ref=dsend.at[part], dst_ref=drecv.at[part],
                send_sem=dsem.at[0, part], recv_sem=dsem.at[1, part],
                device_id=partner, device_id_type=MESH,
            )
            dcopy[part].start()

        def merge(part):
            dcopy[part].wait_recv()
            for i, d in enumerate(ORDER):
                total = own[part, i] + drecv[part, i]
                if d == 0:
                    own[part, i] = total
                    continue
                ysend[part, d - 1] = total
                ycopy[part, d] = pltpu.make_async_remote_copy(
                    src_ref=ysend.at[part, d - 1], dst_ref=yrecv.at[part, d - 1],
                    send_sem=ysem.at[0, part, d - 1], recv_sem=ysem.at[1, part, d - 1],
                    device_id=y_peer[d], device_id_type=MESH,
                )
                ycopy[part, d].start()

        def early_ghost(d):
            return pltpu.make_async_remote_copy(
                src_ref=gsend, dst_ref=gearly.at[d],
                send_sem=gxsem.at[0], recv_sem=gxsem.at[1 + d],
                device_id=place(3, y, z, core), device_id_type=MESH,
            )

        def ahead(part, partial):
            for step in range(2):
                for half in range(2):
                    at = step * 4 + part * 2 + half
                    line = 126 + step
                    gsend[at : at + 1] = partial[line : line + 1, half * 128 : half * 128 + 128]
            if part == 1:
                pl.when(x < 3)(early_ghost(x).start)

        def sum_y(part):
            total = own[part, 3]
            for d in (1, 3, 2):
                ycopy[part, d].wait_recv()
                total = total + yrecv[part, d - 1]
            split = split_rows(total)
            stack = jnp.concatenate([split[k] for k in (0, 1, 0, 2, 0, 1)], axis=0)
            partial = jnp.dot(wide[:, 0:192], stack, preferred_element_type=F32)
            for at in range(4):
                xsend[part, at] = partial[at * 32 : at * 32 + 32]
            ahead(part, partial)
            for d in (2, 1, 3):
                xcopy[part, d] = pltpu.make_async_remote_copy(
                    src_ref=xsend.at[part, (x + d) % 4], dst_ref=xrecv.at[part, d - 1],
                    send_sem=xsem.at[0, part, d - 1], recv_sem=xsem.at[1, part, d - 1],
                    device_id=x_peer[d], device_id_type=MESH,
                )
                xcopy[part, d].start()

        def z_copy(part, k):
            lo = (z_lo + k) % 4
            d = (part * 4 + lo + 8 - z) % 8
            at = (d + 7) % 8
            return d, pltpu.make_async_remote_copy(
                src_ref=zsend.at[part, pl.ds(pl.multiple_of(lo * 8, 8), 8)],
                dst_ref=zrecv.at[at],
                send_sem=zsem.at[0, at], recv_sem=zsem.at[1, at],
                device_id=place(x, y, part * 4 + lo, core), device_id_type=MESH,
            )

        def sum_x(part):
            total = xsend[part, x]
            for d in (1, 3, 2):
                xcopy[part, d].wait_recv()
                total = total + xrecv[part, d - 1]
            zsend[part] = total
            for k in (2, 1, 3, 0):
                d, copy = z_copy(part, k)
                if k == 0:
                    pl.when(d != 0)(copy.start)
                else:
                    copy.start()

        def strip(at, carry):
            base = pl.multiple_of(at * 32, 8)
            state = [fields[j, pl.ds(base, 48), :] for j in range(5)]
            values, rest = state[0:3], state[3:5]
            terms = face_terms(*rest)
            for _ in range(2):
                values = advance(*values, *rest, terms)
            for ref, value in zip((surf_o, flow_x_o, flow_y_o), values):
                ref[pl.ds(base, 32), :] = value[8:40]
            return carry

    with jax.named_scope("spectrum"):
        products(0, 0, dsend)
    with jax.named_scope("barrier"):
        pl.semaphore_wait(barrier, greetings)
    with jax.named_scope("spectrum_1"):
        to_partner(0)
        products(0, 1, own)
    with jax.named_scope("row_halos"):
        for copy in borders:
            copy.wait()
        for source in (0, 248):
            fields[4, source + 8 : source + 16, :] = mbuf[source : source + 8].astype(F32)
        ns_copies = []
        for at, (first, last, peer, inside) in enumerate(
            ((8, 264, north, row > 0), (256, 0, south, row < 15))
        ):
            copy = pltpu.make_async_remote_copy(
                src_ref=fields.at[:, pl.ds(first, 8)],
                dst_ref=fields.at[:, pl.ds(last, 8)],
                send_sem=nssem.at[0, at], recv_sem=nssem.at[1, at],
                device_id=peer, device_id_type=MESH,
            )
            pl.when(inside)(copy.start)
            ns_copies.append((copy, inside))
    with jax.named_scope("spectrum_2"):
        products(1, 0, dsend)
        to_partner(1)
    with jax.named_scope("merge_0"):
        merge(0)
        for d in range(1, 4):
            pl.semaphore_signal(known.at[d + 1], inc=1, device_id=y_peer[d], device_id_type=MESH)
    with jax.named_scope("spectrum_3"):
        products(1, 1, own)
    with jax.named_scope("merge_1"):
        merge(1)

    with jax.named_scope("widen"):
        local[2].wait()
        split = split_rows(tab[0:32])
        wide[...] = jnp.concatenate(
            [*(split[k].astype(F32) for k in (0, 0, 1, 0, 2, 1)), jnp.zeros((64, 128), F32)], axis=0
        ).T.astype(BF16)
        for copy in grids:
            copy.wait()
        fields[4, 16:256, :] = mbuf[8:248].astype(F32)

    with jax.named_scope("water"):
        lax.fori_loop(1, 3, strip, 0)
    with jax.named_scope("relay"):
        for d in range(1, 4):
            pl.semaphore_wait(known.at[d + 1], 1)
        for at, d in enumerate((2, 6)):
            pl.semaphore_signal(known.at[at], inc=1, device_id=z_peer[d], device_id_type=MESH)

    with jax.named_scope("sum_y_0"):
        sum_y(0)

    with jax.named_scope("column_halos"):
        pl.when(row < 15)(ns_copies[0][0].wait_recv)
        pl.when(row > 0)(ns_copies[1][0].wait_recv)

        @pl.when(row == 0)
        def _():
            fields[:, 0:8, :] = jnp.zeros((5, 8, 256), F32)

        @pl.when(is_edge)
        def _():
            fields[:, 264:272, :] = jnp.zeros((5, 8, 256), F32)

        lane = lax.broadcasted_iota(jnp.int32, (272, 128), 1)
        ew_copies = []
        for at, (first, shift, peer, inside) in enumerate(
            ((0, 0, west, col > 0), (128, 4, east, col < 15))
        ):
            packed = jnp.zeros((272, 128), F32)
            for j in range(5):
                block = fields[j, :, first : first + 128]
                if 4 * j + shift:
                    block = pltpu.roll(block, 4 * j + shift, 1)
                packed = jnp.where((lane >> 2) == j, block, packed)
            packed = jnp.concatenate([packed, jnp.zeros((112, 128), F32)], axis=0)
            ewsend[at] = packed.T[0:24]
            copy = pltpu.make_async_remote_copy(
                src_ref=ewsend.at[at], dst_ref=ewrecv.at[at],
                send_sem=ewsem.at[0, at], recv_sem=ewsem.at[1, at],
                device_id=peer, device_id_type=MESH,
            )
            ew_copies.append((copy, inside))

    with jax.named_scope("sum_y_1"):
        sum_y(1)

    with jax.named_scope("far"):
        for at in range(2):
            pl.semaphore_wait(known.at[at], 1)
        for copy, inside in ew_copies:
            pl.when(inside)(copy.start)

    with jax.named_scope("water_1"):
        lax.fori_loop(3, 6, strip, 0)
    with jax.named_scope("sum_x_0"):
        sum_x(0)
    with jax.named_scope("ghost_send"):
        here = pl.ds(pl.multiple_of((z * 4 + y) * 8, 8), 8)

        def ghost_copy(index):
            return pltpu.make_async_remote_copy(
                src_ref=gtotal, dst_ref=grecv.at[here],
                send_sem=gssem.at[index], recv_sem=grsem,
                device_id=(15, index * 2 + core), device_id_type=MESH,
            )

        @pl.when(x == 3)
        def _():
            total = gsend[...]
            for d in range(3):
                early_ghost(d).wait_recv()
                total = total + gearly[d]
            gtotal[...] = total
            for index in range(8):
                pl.when((row != 15) | (col != index * 2 + core))(ghost_copy(index).start)

    with jax.named_scope("sum_x_1"):
        sum_x(1)

    with jax.named_scope("more_water"):
        lax.fori_loop(6, 9, lambda at, carry: strip(at % 8, carry), 0)

    with jax.named_scope("selection"):
        @pl.when(is_edge)
        def _():
            at = lax.broadcasted_iota(jnp.int32, (128, 384), 1)
            column = col * 256 + jnp.where(at >= 320, at - 384, at)
            turned = jnp.concatenate(
                [cellbuf[...].astype(F32), jnp.zeros((96, 128), F32)], axis=0
            ).T.astype(jnp.int32)
            found = jnp.zeros((128, 384), F32)
            for block in range(32):
                found = jnp.where(turned[:, block : block + 1] == column, block + 1.0, found)
            onehot[...] = jnp.where(found > 0.0, 1.0, 0.0).astype(BF16)
            blocks[...] = jnp.broadcast_to(jnp.sum(found, axis=0, keepdims=True), (8, 384))

    with jax.named_scope("side_water"):
        for at, ((copy, _), inside) in enumerate(zip(ew_copies, (col < 15, col > 0))):
            pl.when(inside)(copy.wait_recv)

            @pl.when(~inside)
            def _():
                ewrecv[at] = jnp.zeros((24, 384), F32)

        from_east, from_west = ewrecv[0], ewrecv[1]
        for j in range(5):
            for at, piece in enumerate((from_west, ewsend[0], ewsend[1], from_east)):
                sides[j, at * 4 : at * 4 + 4] = piece[j * 4 : j * 4 + 4]
        state = [sides[j] for j in range(5)]
        values, rest = state[0:3], state[3:5]
        terms = face_terms(*rest, (0, 1))
        for _ in range(2):
            values = advance(*values, *rest, terms, (0, 1))
        turned = jnp.concatenate([*values, jnp.zeros((80, 384), F32)], axis=0).T[8:264]
        lane = lax.broadcasted_iota(jnp.int32, (256, 128), 1)
        for j, ref in enumerate((surf_o, flow_x_o, flow_y_o)):
            ref[:, 0:128] = jnp.where(
                lane < 2, pltpu.roll(turned, 124 - 16 * j, 1), ref[:, 0:128]
            )
            ref[:, 128:256] = jnp.where(
                lane >= 126, pltpu.roll(turned, 116 - 16 * j, 1), ref[:, 128:256]
            )

        @pl.when(is_edge)
        def _():
            blank = jnp.zeros((104, 256), F32)
            right, left_side = (
                jnp.concatenate([piece[:, 128:384], blank], axis=0).T[120:144]
                for piece in (from_east, from_west)
            )
            lane = lax.broadcasted_iota(jnp.int32, (24, 128), 1)
            for j in range(5):
                first = pltpu.roll(right, 128 - 4 * j, 1) if j else right
                wrapped = pltpu.roll(left_side, 124 - 4 * j, 1)
                tail[j] = jnp.where(lane < 2, first, jnp.where(lane >= 126, wrapped, 0.0))

    with jax.named_scope("sum_z"):
        total = zsend[z_hi, pl.ds(pl.multiple_of(z_lo * 8, 8), 8)]
        for d in range(1, 8):
            pltpu.make_async_copy(zrecv.at[d - 1], zrecv.at[d - 1], zsem.at[1, d - 1]).wait()
            total = total + zrecv[d - 1]
        series_o[...] = total

    with jax.named_scope("ghost"):
        @pl.when(is_edge)
        def _():
            grecv[here] = gtotal[...]
            pltpu.make_async_copy(
                grecv.at[pl.ds(0, 248)], grecv.at[pl.ds(0, 248)], grsem
            ).wait()
            value = grecv[0:32]
            for other_z in range(1, 8):
                value = value + grecv[other_z * 32 : other_z * 32 + 32]
            gpair[core] = value
            share = pltpu.make_async_remote_copy(
                src_ref=gpair.at[core], dst_ref=gpair.at[core],
                send_sem=gpsem.at[0], recv_sem=gpsem.at[1],
                device_id=partner, device_id_type=MESH,
            )
            share.start()
            share.wait_send()
            share.wait_recv()
            value = jnp.concatenate([gpair[0], gpair[1]], axis=0)
            picked = jnp.dot(
                jnp.concatenate(split_rows(value), axis=0), onehot[...],
                preferred_element_type=F32,
            )
            picked = picked[128:192] + picked[64:128] + picked[0:64]
            at = lax.broadcasted_iota(jnp.int32, (64, 384), 0)
            block = ((at >> 3) & 3) * 8 + (at & 2) * 2 + (at >> 5) * 2 + (at & 1)
            picked = jnp.where((block + 1).astype(F32) == blocks[0:1], picked, 0.0)
            ghost = [
                jnp.sum(jnp.where(((at >> 2) & 1) == step, picked, 0.0), axis=0, keepdims=True)
                for step in range(2)
            ]
            beyond = lax.broadcasted_iota(jnp.int32, (24, 384), 0) == 16
            state = [
                jnp.concatenate([fields[j, 248:272, :], tail[j]], axis=1) for j in range(5)
            ]
            rest = [jnp.where(beyond, 1.0, value) for value in state[3:5]]
            values = state[0:3]
            terms = face_terms(*rest)
            for step in range(2):
                values = [
                    jnp.where(beyond, ghost[step], values[0]),
                    jnp.where(beyond, 0.0, values[1]),
                    jnp.where(beyond, 0.0, values[2]),
                ]
                values = advance(*values, *rest, terms)
            for ref, value in zip((surf_o, flow_x_o, flow_y_o), values):
                ref[248:256, :] = value[8:16, 0:256]

    with jax.named_scope("drain"):
        for copy in [*dcopy.values(), *ycopy.values(), *xcopy.values()]:
            copy.wait_send()
        for copy, inside in [*ns_copies, *ew_copies]:
            pl.when(inside)(copy.wait_send)
        for part in range(2):
            for k in range(4):
                d, copy = z_copy(part, k)
                pl.when(d != 0)(copy.wait_send)
        pl.when(x < 3)(early_ghost(x).wait_send)

        @pl.when(x == 3)
        def _():
            for index in range(8):
                pl.when((row != 15) | (col != index * 2 + core))(ghost_copy(index).wait_send)


def write_out(*refs):
    sources, targets, sems = refs[0:4], refs[4:8], refs[8]
    copies = [
        pltpu.make_async_copy(source, target, sems.at[j])
        for j, (source, target) in enumerate(zip(sources, targets))
    ]
    for copy in copies:
        copy.start()
    for copy in copies:
        copy.wait()


def on_device(
    kernel_hat, coefficients, wave_speed_sq, wet_mask, boundary_cell, height, flux_x, flux_y
):
    field = jax.ShapeDtypeStruct((256, 256), F32)
    dma = pltpu.SemaphoreType.DMA
    shapes = (jax.ShapeDtypeStruct((8, 256), F32), field, field, field)
    operands = [
        pltpu.with_memory_space_constraint(value, pltpu.MemorySpace.HBM)
        for value in (
            kernel_hat.reshape(1024, 4096),
            coefficients.T,
            wave_speed_sq,
            wet_mask,
            boundary_cell.reshape(32, 128),
            height,
            flux_x,
            flux_y,
            jnp.asarray(transform_tables()),
        )
    ]
    results = pl.pallas_call(
        kernel,
        out_shape=shapes,
        in_specs=[pl.BlockSpec(memory_space=pltpu.MemorySpace.HBM)] * 9,
        out_specs=[pl.BlockSpec(memory_space=pltpu.VMEM)] * 4,
        scratch_shapes=[
            pltpu.VMEM((16, 1024, 256), BF16),
            pltpu.VMEM((128, 128), F32),
            pltpu.VMEM((32, 128), F32),
            pltpu.VMEM((256, 256), jnp.int32),
            pltpu.VMEM((32, 128), jnp.int32),
            pltpu.VMEM((32, 1024), BF16),
            pltpu.VMEM((2, 4, 32, 256), F32),
            pltpu.VMEM((2, 4, 32, 256), F32),
            pltpu.VMEM((2, 4, 32, 256), F32),
            pltpu.VMEM((2, 3, 32, 256), F32),
            pltpu.VMEM((2, 3, 32, 256), F32),
            pltpu.VMEM((2, 4, 32, 256), F32),
            pltpu.VMEM((2, 3, 32, 256), F32),
            pltpu.VMEM((2, 32, 256), F32),
            pltpu.VMEM((7, 8, 256), F32),
            pltpu.VMEM((8, 128), F32),
            pltpu.VMEM((3, 8, 128), F32),
            pltpu.VMEM((8, 128), F32),
            pltpu.VMEM((2, 32, 128), F32),
            pltpu.VMEM((256, 128), F32),
            pltpu.VMEM((5, 272, 256), F32),
            pltpu.VMEM((2, 24, 384), F32),
            pltpu.VMEM((2, 24, 384), F32),
            pltpu.VMEM((5, 16, 384), F32),
            pltpu.VMEM((5, 24, 128), F32),
            pltpu.VMEM((128, 384), BF16),
            pltpu.VMEM((8, 384), F32),
            pltpu.VMEM((128, 256), BF16),
            dma((16,)),
            dma((9,)),
            dma((10,)),
            dma((2, 2)),
            dma((2, 2, 3)),
            dma((2, 2, 3)),
            dma((2, 8)),
            dma((4,)),
            dma((2,)),
            dma((8,)),
            dma(()),
            dma((2, 2)),
            dma((2, 2)),
            pltpu.SemaphoreType.REGULAR((5,)),
        ],
        compiler_params=pltpu.CompilerParams(
            collective_id=0, has_side_effects=True, vmem_limit_bytes=48 * 1024 * 1024
        ),
    )(*operands)
    return pl.pallas_call(
        write_out,
        out_shape=shapes,
        in_specs=[pl.BlockSpec(memory_space=pltpu.VMEM)] * 4,
        out_specs=[pl.BlockSpec(memory_space=pltpu.MemorySpace.HBM)] * 4,
        scratch_shapes=[dma((4,))],
        compiler_params=pltpu.CompilerParams(vmem_limit_bytes=16 * 1024 * 1024),
    )(*results)


def solution(mesh):
    return jax.shard_map(
        on_device,
        mesh=mesh,
        in_specs=(
            P(None, "rows", "cols", None),
            P(None, "cols"),
            P("rows", "cols"),
            P("rows", "cols"),
            P(),
            P("rows", "cols"),
            P("rows", "cols"),
            P("rows", "cols"),
        ),
        out_specs=(P("rows", "cols"), P("rows", "cols"), P("rows", "cols"), P("rows", "cols")),
        check_vma=False,
    )
```

```python
import functools

import jax
import jax.numpy as jnp
import numpy as np
from jax import lax
from jax.experimental import pallas as pl
from jax.experimental.pallas import tpu as pltpu
from jax.sharding import PartitionSpec as P

F32 = jnp.float32
BF16 = jnp.bfloat16
HIGH = lax.Precision.HIGHEST
MESH = pl.DeviceIdType.MESH
ORDER = (2, 1, 3, 0)
LOADS = (0, 4, 8, 12, 2, 6, 10, 14, 1, 5, 9, 13, 3, 7, 11, 15)


def transform_tables():
    table = np.zeros((16, 128, 128), np.float32)
    times = np.arange(128)
    inner = times.reshape(4, 4, 8).transpose(1, 0, 2).reshape(-1)
    for row in range(16):
        freqs = row * 16 + np.arange(16)
        angle = 2.0 * np.pi * ((freqs[:, None] * inner[None, :]) % 256) / 256.0
        table[row, 0:16] = np.cos(angle) / 256.0
        table[row, 16:32] = -np.sin(angle) / 256.0
        angle = 2.0 * np.pi * ((freqs[:, None] * times[None, :]) % 256) / 256.0
        table[row, 32:48] = np.cos(angle)
        table[row, 48:64] = -np.sin(angle)
        table[row, 64:80] = np.sin(angle)
        table[row, 80:96] = np.cos(angle)
    return table


def after(values, axis):
    return pltpu.roll(values, values.shape[axis] - 1, axis)


def before(values, axis):
    return pltpu.roll(values, 1, axis)


def split_rows(value):
    high = value.astype(BF16)
    value = value - high.astype(F32)
    middle = value.astype(BF16)
    return [high, middle, (value - middle.astype(F32)).astype(BF16)]


def face_terms(speed, wet, axes=(1, 0)):
    celerity = jnp.sqrt(speed)
    terms = []
    for axis in axes:
        opened = wet * after(wet, axis)
        terms.append((0.5 * opened, opened * (0.25 * (celerity + after(celerity, axis)))))
    return terms


def advance(surface, along_x, along_y, speed, wet, terms, axes=(1, 0)):
    pressure = speed * surface
    changes = []
    for axis, along, across, (half, damp) in zip(
        axes, (along_x, along_y), (along_y, along_x), terms
    ):
        next_along = after(along, axis)
        mass = half * (along + next_along) - damp * (after(surface, axis) - surface)
        push = half * (pressure + after(pressure, axis)) - damp * (next_along - along)
        shear = damp * (across - after(across, axis))
        changes.append(tuple(flux - before(flux, axis) for flux in (mass, push, shear)))
    (mass_x, push_x, shear_x), (mass_y, push_y, shear_y) = changes
    return (
        wet * (surface - 0.25 * (mass_x + mass_y)),
        wet * (along_x - 0.25 * (push_x + shear_y)),
        wet * (along_y - 0.25 * (shear_x + push_y)),
    )


def kernel(
    kern, coef, speed, mask, cells, surf, flow_x, flow_y, table,
    series_o, surf_o, flow_x_o, flow_y_o,
    kbuf, tab, cbuf, mbuf, cellbuf, left, own, dsend, drecv, ysend, yrecv,
    xsend, xrecv, zsend, zrecv, gsend, gearly, gtotal, gpair, grecv, fields, ewsend, ewrecv, sides, tail, onehot, blocks, wide,
    ksem, lsem, bsem, dsem, ysem, xsem, zsem, gxsem, gpsem, gssem, grsem, nssem, ewsem, known,
):
    row, col = lax.axis_index("rows"), lax.axis_index("cols")
    x, z_lo = row % 4, row // 4
    y, z_hi, core = col // 4, (col // 2) % 2, col % 2
    z = z_hi * 4 + z_lo
    is_edge = row == 15

    def place(at_x, at_y, at_z, at_core):
        return ((at_z % 4) * 4 + at_x, at_y * 4 + (at_z // 4) * 2 + at_core)

    partner = place(x, y, z, 1 - core)
    y_peer = [place(x, (y + d) % 4, z, core) for d in range(4)]
    x_peer = [place((x + d) % 4, y, z, core) for d in range(4)]
    z_peer = [place(x, y, (z + d) % 8, core) for d in range(8)]
    north, south = ((row + 15) % 16, col), ((row + 1) % 16, col)
    west, east = (row, (col + 15) % 16), (row, (col + 1) % 16)

    with jax.named_scope("start_loads"):
        local = [
            pltpu.make_async_copy(
                table.at[row, pl.ds(32, 64)], tab.at[pl.ds(32, 64)], lsem.at[0]
            ),
            pltpu.make_async_copy(coef, cbuf, lsem.at[1]),
            pltpu.make_async_copy(table.at[row, pl.ds(0, 32)], tab.at[pl.ds(0, 32)], lsem.at[8]),
        ]
        for copy in local[0:2]:
            copy.start()
        loads = []
        for i, d in enumerate(ORDER):
            for side, par in enumerate((1 - core, core)):
                for part in range(2):
                    slot = i * 4 + side * 2 + part
                    start = pl.multiple_of(((((y + d) % 4) * 2 + part) * 2 + par) * 256, 256)
                    loads.append(
                        pltpu.make_async_copy(
                            kern.at[:, pl.ds(start, 256)], kbuf.at[slot], ksem.at[slot]
                        )
                    )
        for slot in LOADS[0:4]:
            loads[slot].start()

    with jax.named_scope("greet_peers"):
        barrier = pltpu.get_barrier_semaphore()
        near = [partner, *y_peer[1:], *x_peer[1:], *(z_peer[d] for d in (1, 2, 6, 7))]
        for peer in near:
            pl.semaphore_signal(barrier, inc=1, device_id=peer, device_id_type=MESH)
        greetings = len(near)
        for peer, inside in ((north, row > 0), (south, row < 15)):
            greetings = greetings + inside.astype(jnp.int32)

            @pl.when(inside)
            def _():
                pl.semaphore_signal(barrier, inc=1, device_id=peer, device_id_type=MESH)

    with jax.named_scope("more_loads"):
        for slot in LOADS[4:8]:
            loads[slot].start()
        sources = (surf, flow_x, flow_y, speed)
        borders = []
        for side, (source, target) in enumerate(((0, 8), (248, 256))):
            for j in range(5):
                at = bsem.at[side * 5 + j]
                if j < 4:
                    copy = pltpu.make_async_copy(
                        sources[j].at[pl.ds(source, 8)], fields.at[j, pl.ds(target, 8)], at
                    )
                else:
                    copy = pltpu.make_async_copy(
                        mask.at[pl.ds(source, 8)], mbuf.at[pl.ds(source, 8)], at
                    )
                borders.append(copy)
        for copy in borders:
            copy.start()
        middle = pl.ds(8, 240)
        grids = [
            pltpu.make_async_copy(ref.at[middle], fields.at[j, pl.ds(16, 240)], lsem.at[2 + j])
            for j, ref in enumerate(sources)
        ]
        grids += [
            pltpu.make_async_copy(mask.at[middle], mbuf.at[middle], lsem.at[6]),
            pltpu.make_async_copy(cells, cellbuf, lsem.at[7]),
        ]

    with jax.named_scope("wait_coef"):
        for slot in LOADS[8:]:
            loads[slot].start()
        for copy in [*grids, local[2]]:
            copy.start()
        local[0].wait()
    with jax.named_scope("wait_table"):
        local[1].wait()

    with jax.named_scope("build_left"):
        tiled = lax.dot_general(
            tab[32:96], jnp.concatenate([cbuf[...]] * 16, axis=0), (((1,), (1,)), ((), ())),
            precision=HIGH, preferred_element_type=F32,
        )
        lanes = lax.broadcasted_iota(jnp.int32, (32, 512), 1)
        subs = lax.broadcasted_iota(jnp.int32, (32, 512), 0)
        diagonal = (lanes >> 5) == (subs & 15)
        left[:, 0:512] = jnp.where(diagonal, tiled[0:32], 0.0).astype(BF16)
        left[:, 512:1024] = jnp.where(diagonal, tiled[32:64], 0.0).astype(BF16)

        dcopy, ycopy, xcopy = {}, {}, {}

        def products(part, side, target):
            for i in range(4):
                loads[i * 4 + side * 2 + part].wait()
            for i in range(4):
                target[part, i] = jnp.dot(
                    left[...], kbuf[i * 4 + side * 2 + part], preferred_element_type=F32
                )

        def to_partner(part):
            dcopy[part] = pltpu.make_async_remote_copy(
                src_ref=dsend.at[part], dst_ref=drecv.at[part],
                send_sem=dsem.at[0, part], recv_sem=dsem.at[1, part],
                device_id=partner, device_id_type=MESH,
            )
            dcopy[part].start()

        def merge(part):
            dcopy[part].wait_recv()
            for i, d in enumerate(ORDER):
                total = own[part, i] + drecv[part, i]
                if d == 0:
                    own[part, i] = total
                    continue
                ysend[part, d - 1] = total
                ycopy[part, d] = pltpu.make_async_remote_copy(
                    src_ref=ysend.at[part, d - 1], dst_ref=yrecv.at[part, d - 1],
                    send_sem=ysem.at[0, part, d - 1], recv_sem=ysem.at[1, part, d - 1],
                    device_id=y_peer[d], device_id_type=MESH,
                )
                ycopy[part, d].start()

        def early_ghost(d):
            return pltpu.make_async_remote_copy(
                src_ref=gsend, dst_ref=gearly.at[d],
                send_sem=gxsem.at[0], recv_sem=gxsem.at[1 + d],
                device_id=place(3, y, z, core), device_id_type=MESH,
            )

        def ahead(part, partial):
            for step in range(2):
                for half in range(2):
                    at = step * 4 + part * 2 + half
                    line = 126 + step
                    gsend[at : at + 1] = partial[line : line + 1, half * 128 : half * 128 + 128]
            if part == 1:
                pl.when(x < 3)(early_ghost(x).start)

        def sum_y(part):
            total = own[part, 3]
            for d in (1, 3, 2):
                ycopy[part, d].wait_recv()
                total = total + yrecv[part, d - 1]
            split = split_rows(total)
            stack = jnp.concatenate([split[k] for k in (0, 1, 0, 2, 0, 1)], axis=0)
            partial = jnp.dot(wide[:, 0:192], stack, preferred_element_type=F32)
            for at in range(4):
                xsend[part, at] = partial[at * 32 : at * 32 + 32]
            ahead(part, partial)
            for d in (2, 1, 3):
                xcopy[part, d] = pltpu.make_async_remote_copy(
                    src_ref=xsend.at[part, (x + d) % 4], dst_ref=xrecv.at[part, d - 1],
                    send_sem=xsem.at[0, part, d - 1], recv_sem=xsem.at[1, part, d - 1],
                    device_id=x_peer[d], device_id_type=MESH,
                )
                xcopy[part, d].start()

        def z_copy(part, k):
            lo = (z_lo + k) % 4
            d = (part * 4 + lo + 8 - z) % 8
            at = (d + 7) % 8
            return d, pltpu.make_async_remote_copy(
                src_ref=zsend.at[part, pl.ds(pl.multiple_of(lo * 8, 8), 8)],
                dst_ref=zrecv.at[at],
                send_sem=zsem.at[0, at], recv_sem=zsem.at[1, at],
                device_id=place(x, y, part * 4 + lo, core), device_id_type=MESH,
            )

        def sum_x(part):
            total = xsend[part, x]
            for d in (1, 3, 2):
                xcopy[part, d].wait_recv()
                total = total + xrecv[part, d - 1]
            zsend[part] = total
            for k in (2, 1, 3, 0):
                d, copy = z_copy(part, k)
                if k == 0:
                    pl.when(d != 0)(copy.start)
                else:
                    copy.start()

        def strip(at, carry):
            base = pl.multiple_of(at * 32, 8)
            state = [fields[j, pl.ds(base, 48), :] for j in range(5)]
            values, rest = state[0:3], state[3:5]
            terms = face_terms(*rest)
            for _ in range(2):
                values = advance(*values, *rest, terms)
            for ref, value in zip((surf_o, flow_x_o, flow_y_o), values):
                ref[pl.ds(base, 32), :] = value[8:40]
            return carry

    with jax.named_scope("spectrum"):
        products(0, 0, dsend)
    with jax.named_scope("barrier"):
        pl.semaphore_wait(barrier, greetings)
    with jax.named_scope("spectrum_1"):
        to_partner(0)
        products(0, 1, own)
    with jax.named_scope("row_halos"):
        for copy in borders:
            copy.wait()
        for source in (0, 248):
            fields[4, source + 8 : source + 16, :] = mbuf[source : source + 8].astype(F32)
        ns_copies = []
        for at, (first, last, peer, inside) in enumerate(
            ((8, 264, north, row > 0), (256, 0, south, row < 15))
        ):
            copy = pltpu.make_async_remote_copy(
                src_ref=fields.at[:, pl.ds(first, 8)],
                dst_ref=fields.at[:, pl.ds(last, 8)],
                send_sem=nssem.at[0, at], recv_sem=nssem.at[1, at],
                device_id=peer, device_id_type=MESH,
            )
            pl.when(inside)(copy.start)
            ns_copies.append((copy, inside))
    with jax.named_scope("spectrum_2"):
        products(1, 0, dsend)
        to_partner(1)
    with jax.named_scope("merge_0"):
        merge(0)
        for d in range(1, 4):
            pl.semaphore_signal(known.at[d + 1], inc=1, device_id=y_peer[d], device_id_type=MESH)
    with jax.named_scope("spectrum_3"):
        products(1, 1, own)
    with jax.named_scope("merge_1"):
        merge(1)

    with jax.named_scope("widen"):
        local[2].wait()
        split = split_rows(tab[0:32])
        wide[...] = jnp.concatenate(
            [*(split[k].astype(F32) for k in (0, 0, 1, 0, 2, 1)), jnp.zeros((64, 128), F32)], axis=0
        ).T.astype(BF16)
        for copy in grids:
            copy.wait()
        fields[4, 16:256, :] = mbuf[8:248].astype(F32)

    with jax.named_scope("water"):
        lax.fori_loop(1, 3, strip, 0)
    with jax.named_scope("relay"):
        for d in range(1, 4):
            pl.semaphore_wait(known.at[d + 1], 1)
        for at, d in enumerate((2, 6)):
            pl.semaphore_signal(known.at[at], inc=1, device_id=z_peer[d], device_id_type=MESH)

    with jax.named_scope("sum_y_0"):
        sum_y(0)

    with jax.named_scope("column_halos"):
        pl.when(row < 15)(ns_copies[0][0].wait_recv)
        pl.when(row > 0)(ns_copies[1][0].wait_recv)

        @pl.when(row == 0)
        def _():
            fields[:, 0:8, :] = jnp.zeros((5, 8, 256), F32)

        @pl.when(is_edge)
        def _():
            fields[:, 264:272, :] = jnp.zeros((5, 8, 256), F32)

        lane = lax.broadcasted_iota(jnp.int32, (272, 128), 1)
        ew_copies = []
        for at, (first, shift, peer, inside) in enumerate(
            ((0, 0, west, col > 0), (128, 4, east, col < 15))
        ):
            packed = jnp.zeros((272, 128), F32)
            for j in range(5):
                block = fields[j, :, first : first + 128]
                if 4 * j + shift:
                    block = pltpu.roll(block, 4 * j + shift, 1)
                packed = jnp.where((lane >> 2) == j, block, packed)
            packed = jnp.concatenate([packed, jnp.zeros((112, 128), F32)], axis=0)
            ewsend[at] = packed.T[0:24]
            copy = pltpu.make_async_remote_copy(
                src_ref=ewsend.at[at], dst_ref=ewrecv.at[at],
                send_sem=ewsem.at[0, at], recv_sem=ewsem.at[1, at],
                device_id=peer, device_id_type=MESH,
            )
            ew_copies.append((copy, inside))

    with jax.named_scope("sum_y_1"):
        sum_y(1)

    with jax.named_scope("far"):
        for at in range(2):
            pl.semaphore_wait(known.at[at], 1)
        for copy, inside in ew_copies:
            pl.when(inside)(copy.start)

    with jax.named_scope("water_1"):
        lax.fori_loop(3, 7, strip, 0)
    with jax.named_scope("sum_x_0"):
        sum_x(0)
    with jax.named_scope("ghost_send"):
        here = pl.ds(pl.multiple_of((z * 4 + y) * 8, 8), 8)

        def ghost_copy(index):
            return pltpu.make_async_remote_copy(
                src_ref=gtotal, dst_ref=grecv.at[here],
                send_sem=gssem.at[index], recv_sem=grsem,
                device_id=(15, index * 2 + core), device_id_type=MESH,
            )

        @pl.when(x == 3)
        def _():
            total = gsend[...]
            for d in range(3):
                early_ghost(d).wait_recv()
                total = total + gearly[d]
            gtotal[...] = total
            for index in range(8):
                pl.when((row != 15) | (col != index * 2 + core))(ghost_copy(index).start)

    with jax.named_scope("sum_x_1"):
        sum_x(1)

    with jax.named_scope("more_water"):
        lax.fori_loop(7, 9, lambda at, carry: strip(at % 8, carry), 0)

    with jax.named_scope("selection"):
        @pl.when(is_edge)
        def _():
            at = lax.broadcasted_iota(jnp.int32, (128, 384), 1)
            column = col * 256 + jnp.where(at >= 320, at - 384, at)
            turned = jnp.concatenate(
                [cellbuf[...].astype(F32), jnp.zeros((96, 128), F32)], axis=0
            ).T.astype(jnp.int32)
            found = jnp.zeros((128, 384), F32)
            for block in range(32):
                found = jnp.where(turned[:, block : block + 1] == column, block + 1.0, found)
            onehot[...] = jnp.where(found > 0.0, 1.0, 0.0).astype(BF16)
            blocks[...] = jnp.broadcast_to(jnp.sum(found, axis=0, keepdims=True), (8, 384))

    with jax.named_scope("side_water"):
        for at, ((copy, _), inside) in enumerate(zip(ew_copies, (col < 15, col > 0))):
            pl.when(inside)(copy.wait_recv)

            @pl.when(~inside)
            def _():
                ewrecv[at] = jnp.zeros((24, 384), F32)

        from_east, from_west = ewrecv[0], ewrecv[1]
        for j in range(5):
            for at, piece in enumerate((from_west, ewsend[0], ewsend[1], from_east)):
                sides[j, at * 4 : at * 4 + 4] = piece[j * 4 : j * 4 + 4]
        state = [sides[j] for j in range(5)]
        values, rest = state[0:3], state[3:5]
        terms = face_terms(*rest, (0, 1))
        for _ in range(2):
            values = advance(*values, *rest, terms, (0, 1))
        turned = jnp.concatenate([*values, jnp.zeros((80, 384), F32)], axis=0).T[8:264]
        lane = lax.broadcasted_iota(jnp.int32, (256, 128), 1)
        for j, ref in enumerate((surf_o, flow_x_o, flow_y_o)):
            ref[:, 0:128] = jnp.where(
                lane < 2, pltpu.roll(turned, 124 - 16 * j, 1), ref[:, 0:128]
            )
            ref[:, 128:256] = jnp.where(
                lane >= 126, pltpu.roll(turned, 116 - 16 * j, 1), ref[:, 128:256]
            )

        @pl.when(is_edge)
        def _():
            blank = jnp.zeros((104, 256), F32)
            right, left_side = (
                jnp.concatenate([piece[:, 128:384], blank], axis=0).T[120:144]
                for piece in (from_east, from_west)
            )
            lane = lax.broadcasted_iota(jnp.int32, (24, 128), 1)
            for j in range(5):
                first = pltpu.roll(right, 128 - 4 * j, 1) if j else right
                wrapped = pltpu.roll(left_side, 124 - 4 * j, 1)
                tail[j] = jnp.where(lane < 2, first, jnp.where(lane >= 126, wrapped, 0.0))

    with jax.named_scope("sum_z"):
        total = zsend[z_hi, pl.ds(pl.multiple_of(z_lo * 8, 8), 8)]
        for d in range(1, 8):
            pltpu.make_async_copy(zrecv.at[d - 1], zrecv.at[d - 1], zsem.at[1, d - 1]).wait()
            total = total + zrecv[d - 1]
        series_o[...] = total

    with jax.named_scope("ghost"):
        @pl.when(is_edge)
        def _():
            grecv[here] = gtotal[...]
            pltpu.make_async_copy(
                grecv.at[pl.ds(0, 248)], grecv.at[pl.ds(0, 248)], grsem
            ).wait()
            value = grecv[0:32]
            for other_z in range(1, 8):
                value = value + grecv[other_z * 32 : other_z * 32 + 32]
            gpair[core] = value
            share = pltpu.make_async_remote_copy(
                src_ref=gpair.at[core], dst_ref=gpair.at[core],
                send_sem=gpsem.at[0], recv_sem=gpsem.at[1],
                device_id=partner, device_id_type=MESH,
            )
            share.start()
            share.wait_send()
            share.wait_recv()
            value = jnp.concatenate([gpair[0], gpair[1]], axis=0)
            picked = jnp.dot(
                jnp.concatenate(split_rows(value), axis=0), onehot[...],
                preferred_element_type=F32,
            )
            picked = picked[128:192] + picked[64:128] + picked[0:64]
            at = lax.broadcasted_iota(jnp.int32, (64, 384), 0)
            block = ((at >> 3) & 3) * 8 + (at & 2) * 2 + (at >> 5) * 2 + (at & 1)
            picked = jnp.where((block + 1).astype(F32) == blocks[0:1], picked, 0.0)
            ghost = [
                jnp.sum(jnp.where(((at >> 2) & 1) == step, picked, 0.0), axis=0, keepdims=True)
                for step in range(2)
            ]
            beyond = lax.broadcasted_iota(jnp.int32, (24, 384), 0) == 16
            state = [
                jnp.concatenate([fields[j, 248:272, :], tail[j]], axis=1) for j in range(5)
            ]
            rest = [jnp.where(beyond, 1.0, value) for value in state[3:5]]
            values = state[0:3]
            terms = face_terms(*rest)
            for step in range(2):
                values = [
                    jnp.where(beyond, ghost[step], values[0]),
                    jnp.where(beyond, 0.0, values[1]),
                    jnp.where(beyond, 0.0, values[2]),
                ]
                values = advance(*values, *rest, terms)
            for ref, value in zip((surf_o, flow_x_o, flow_y_o), values):
                ref[248:256, :] = value[8:16, 0:256]

    with jax.named_scope("drain"):
        for copy in [*dcopy.values(), *ycopy.values(), *xcopy.values()]:
            copy.wait_send()
        for copy, inside in [*ns_copies, *ew_copies]:
            pl.when(inside)(copy.wait_send)
        for part in range(2):
            for k in range(4):
                d, copy = z_copy(part, k)
                pl.when(d != 0)(copy.wait_send)
        pl.when(x < 3)(early_ghost(x).wait_send)

        @pl.when(x == 3)
        def _():
            for index in range(8):
                pl.when((row != 15) | (col != index * 2 + core))(ghost_copy(index).wait_send)


def write_out(*refs):
    sources, targets, sems = refs[0:4], refs[4:8], refs[8]
    copies = [
        pltpu.make_async_copy(source, target, sems.at[j])
        for j, (source, target) in enumerate(zip(sources, targets))
    ]
    for copy in copies:
        copy.start()
    for copy in copies:
        copy.wait()


def on_device(
    kernel_hat, coefficients, wave_speed_sq, wet_mask, boundary_cell, height, flux_x, flux_y
):
    field = jax.ShapeDtypeStruct((256, 256), F32)
    dma = pltpu.SemaphoreType.DMA
    shapes = (jax.ShapeDtypeStruct((8, 256), F32), field, field, field)
    operands = [
        pltpu.with_memory_space_constraint(value, pltpu.MemorySpace.HBM)
        for value in (
            kernel_hat.reshape(1024, 4096),
            coefficients.T,
            wave_speed_sq,
            wet_mask,
            boundary_cell.reshape(32, 128),
            height,
            flux_x,
            flux_y,
            jnp.asarray(transform_tables()),
        )
    ]
    results = pl.pallas_call(
        kernel,
        out_shape=shapes,
        in_specs=[pl.BlockSpec(memory_space=pltpu.MemorySpace.HBM)] * 9,
        out_specs=[pl.BlockSpec(memory_space=pltpu.VMEM)] * 4,
        scratch_shapes=[
            pltpu.VMEM((16, 1024, 256), BF16),
            pltpu.VMEM((128, 128), F32),
            pltpu.VMEM((32, 128), F32),
            pltpu.VMEM((256, 256), jnp.int32),
            pltpu.VMEM((32, 128), jnp.int32),
            pltpu.VMEM((32, 1024), BF16),
            pltpu.VMEM((2, 4, 32, 256), F32),
            pltpu.VMEM((2, 4, 32, 256), F32),
            pltpu.VMEM((2, 4, 32, 256), F32),
            pltpu.VMEM((2, 3, 32, 256), F32),
            pltpu.VMEM((2, 3, 32, 256), F32),
            pltpu.VMEM((2, 4, 32, 256), F32),
            pltpu.VMEM((2, 3, 32, 256), F32),
            pltpu.VMEM((2, 32, 256), F32),
            pltpu.VMEM((7, 8, 256), F32),
            pltpu.VMEM((8, 128), F32),
            pltpu.VMEM((3, 8, 128), F32),
            pltpu.VMEM((8, 128), F32),
            pltpu.VMEM((2, 32, 128), F32),
            pltpu.VMEM((256, 128), F32),
            pltpu.VMEM((5, 272, 256), F32),
            pltpu.VMEM((2, 24, 384), F32),
            pltpu.VMEM((2, 24, 384), F32),
            pltpu.VMEM((5, 16, 384), F32),
            pltpu.VMEM((5, 24, 128), F32),
            pltpu.VMEM((128, 384), BF16),
            pltpu.VMEM((8, 384), F32),
            pltpu.VMEM((128, 256), BF16),
            dma((16,)),
            dma((9,)),
            dma((10,)),
            dma((2, 2)),
            dma((2, 2, 3)),
            dma((2, 2, 3)),
            dma((2, 8)),
            dma((4,)),
            dma((2,)),
            dma((8,)),
            dma(()),
            dma((2, 2)),
            dma((2, 2)),
            pltpu.SemaphoreType.REGULAR((5,)),
        ],
        compiler_params=pltpu.CompilerParams(
            collective_id=0, has_side_effects=True, vmem_limit_bytes=48 * 1024 * 1024
        ),
    )(*operands)
    return pl.pallas_call(
        write_out,
        out_shape=shapes,
        in_specs=[pl.BlockSpec(memory_space=pltpu.VMEM)] * 4,
        out_specs=[pl.BlockSpec(memory_space=pltpu.MemorySpace.HBM)] * 4,
        scratch_shapes=[dma((4,))],
        compiler_params=pltpu.CompilerParams(vmem_limit_bytes=16 * 1024 * 1024),
    )(*results)


def solution(mesh):
    return jax.shard_map(
        on_device,
        mesh=mesh,
        in_specs=(
            P(None, "rows", "cols", None),
            P(None, "cols"),
            P("rows", "cols"),
            P("rows", "cols"),
            P(),
            P("rows", "cols"),
            P("rows", "cols"),
            P("rows", "cols"),
        ),
        out_specs=(P("rows", "cols"), P("rows", "cols"), P("rows", "cols"), P("rows", "cols")),
        check_vma=False,
    )
```

```python
import functools

import jax
import jax.numpy as jnp
import numpy as np
from jax import lax
from jax.experimental import pallas as pl
from jax.experimental.pallas import tpu as pltpu
from jax.sharding import PartitionSpec as P

F32 = jnp.float32
BF16 = jnp.bfloat16
HIGH = lax.Precision.HIGHEST
MESH = pl.DeviceIdType.MESH
ORDER = (1, 3, 2, 0)
LOADS = (0, 4, 8, 12, 2, 6, 10, 14, 1, 5, 9, 13, 3, 7, 11, 15)


def transform_tables():
    table = np.zeros((16, 128, 128), np.float32)
    times = np.arange(128)
    inner = times.reshape(4, 4, 8).transpose(1, 0, 2).reshape(-1)
    for row in range(16):
        freqs = row * 16 + np.arange(16)
        angle = 2.0 * np.pi * ((freqs[:, None] * inner[None, :]) % 256) / 256.0
        table[row, 0:16] = np.cos(angle) / 256.0
        table[row, 16:32] = -np.sin(angle) / 256.0
        angle = 2.0 * np.pi * ((freqs[:, None] * times[None, :]) % 256) / 256.0
        table[row, 32:48] = np.cos(angle)
        table[row, 48:64] = -np.sin(angle)
        table[row, 64:80] = np.sin(angle)
        table[row, 80:96] = np.cos(angle)
    return table


def after(values, axis):
    return pltpu.roll(values, values.shape[axis] - 1, axis)


def before(values, axis):
    return pltpu.roll(values, 1, axis)


def split_rows(value):
    high = value.astype(BF16)
    value = value - high.astype(F32)
    middle = value.astype(BF16)
    return [high, middle, (value - middle.astype(F32)).astype(BF16)]


def face_terms(speed, wet, axes=(1, 0)):
    celerity = jnp.sqrt(speed)
    terms = []
    for axis in axes:
        opened = wet * after(wet, axis)
        terms.append((0.5 * opened, opened * (0.25 * (celerity + after(celerity, axis)))))
    return terms


def advance(surface, along_x, along_y, speed, wet, terms, axes=(1, 0)):
    pressure = speed * surface
    changes = []
    for axis, along, across, (half, damp) in zip(
        axes, (along_x, along_y), (along_y, along_x), terms
    ):
        next_along = after(along, axis)
        mass = half * (along + next_along) - damp * (after(surface, axis) - surface)
        push = half * (pressure + after(pressure, axis)) - damp * (next_along - along)
        shear = damp * (across - after(across, axis))
        changes.append(tuple(flux - before(flux, axis) for flux in (mass, push, shear)))
    (mass_x, push_x, shear_x), (mass_y, push_y, shear_y) = changes
    return (
        wet * (surface - 0.25 * (mass_x + mass_y)),
        wet * (along_x - 0.25 * (push_x + shear_y)),
        wet * (along_y - 0.25 * (shear_x + push_y)),
    )


def kernel(
    kern, coef, speed, mask, cells, surf, flow_x, flow_y, table,
    series_o, surf_o, flow_x_o, flow_y_o,
    kbuf, tab, cbuf, mbuf, cellbuf, left, own, dsend, drecv, ysend, yrecv,
    xsend, xrecv, zsend, zrecv, gsend, gearly, gtotal, gpair, grecv, fields, ewsend, ewrecv, sides, tail, onehot, blocks, wide,
    ksem, lsem, bsem, dsem, ysem, xsem, zsem, gxsem, gpsem, gssem, grsem, nssem, ewsem, known,
):
    row, col = lax.axis_index("rows"), lax.axis_index("cols")
    x, z_lo = row % 4, row // 4
    y, z_hi, core = col // 4, (col // 2) % 2, col % 2
    z = z_hi * 4 + z_lo
    is_edge = row == 15

    def place(at_x, at_y, at_z, at_core):
        return ((at_z % 4) * 4 + at_x, at_y * 4 + (at_z // 4) * 2 + at_core)

    partner = place(x, y, z, 1 - core)
    y_peer = [place(x, (y + d) % 4, z, core) for d in range(4)]
    x_peer = [place((x + d) % 4, y, z, core) for d in range(4)]
    z_peer = [place(x, y, (z + d) % 8, core) for d in range(8)]
    north, south = ((row + 15) % 16, col), ((row + 1) % 16, col)
    west, east = (row, (col + 15) % 16), (row, (col + 1) % 16)

    with jax.named_scope("start_loads"):
        local = [
            pltpu.make_async_copy(
                table.at[row, pl.ds(32, 64)], tab.at[pl.ds(32, 64)], lsem.at[0]
            ),
            pltpu.make_async_copy(coef, cbuf, lsem.at[1]),
            pltpu.make_async_copy(table.at[row, pl.ds(0, 32)], tab.at[pl.ds(0, 32)], lsem.at[8]),
        ]
        for copy in local[0:2]:
            copy.start()
        loads = []
        for i, d in enumerate(ORDER):
            for side, par in enumerate((1 - core, core)):
                for part in range(2):
                    slot = i * 4 + side * 2 + part
                    start = pl.multiple_of(((((y + d) % 4) * 2 + part) * 2 + par) * 256, 256)
                    loads.append(
                        pltpu.make_async_copy(
                            kern.at[:, pl.ds(start, 256)], kbuf.at[slot], ksem.at[slot]
                        )
                    )
        for slot in LOADS[0:4]:
            loads[slot].start()

    with jax.named_scope("greet_peers"):
        barrier = pltpu.get_barrier_semaphore()
        near = [partner, *y_peer[1:], *x_peer[1:], *(z_peer[d] for d in (1, 2, 6, 7))]
        for peer in near:
            pl.semaphore_signal(barrier, inc=1, device_id=peer, device_id_type=MESH)
        greetings = len(near)
        for peer, inside in ((north, row > 0), (south, row < 15)):
            greetings = greetings + inside.astype(jnp.int32)

            @pl.when(inside)
            def _():
                pl.semaphore_signal(barrier, inc=1, device_id=peer, device_id_type=MESH)

    with jax.named_scope("more_loads"):
        for slot in LOADS[4:8]:
            loads[slot].start()
        sources = (surf, flow_x, flow_y, speed)
        borders = []
        for side, (source, target) in enumerate(((0, 8), (248, 256))):
            for j in range(5):
                at = bsem.at[side * 5 + j]
                if j < 4:
                    copy = pltpu.make_async_copy(
                        sources[j].at[pl.ds(source, 8)], fields.at[j, pl.ds(target, 8)], at
                    )
                else:
                    copy = pltpu.make_async_copy(
                        mask.at[pl.ds(source, 8)], mbuf.at[pl.ds(source, 8)], at
                    )
                borders.append(copy)
        for copy in borders:
            copy.start()
        middle = pl.ds(8, 240)
        grids = [
            pltpu.make_async_copy(ref.at[middle], fields.at[j, pl.ds(16, 240)], lsem.at[2 + j])
            for j, ref in enumerate(sources)
        ]
        grids += [
            pltpu.make_async_copy(mask.at[middle], mbuf.at[middle], lsem.at[6]),
            pltpu.make_async_copy(cells, cellbuf, lsem.at[7]),
        ]

    with jax.named_scope("wait_coef"):
        for slot in LOADS[8:]:
            loads[slot].start()
        for copy in [*grids, local[2]]:
            copy.start()
        local[0].wait()
    with jax.named_scope("wait_table"):
        local[1].wait()

    with jax.named_scope("build_left"):
        tiled = lax.dot_general(
            tab[32:96], jnp.concatenate([cbuf[...]] * 16, axis=0), (((1,), (1,)), ((), ())),
            precision=HIGH, preferred_element_type=F32,
        )
        lanes = lax.broadcasted_iota(jnp.int32, (32, 512), 1)
        subs = lax.broadcasted_iota(jnp.int32, (32, 512), 0)
        diagonal = (lanes >> 5) == (subs & 15)
        left[:, 0:512] = jnp.where(diagonal, tiled[0:32], 0.0).astype(BF16)
        left[:, 512:1024] = jnp.where(diagonal, tiled[32:64], 0.0).astype(BF16)

        dcopy, ycopy, xcopy = {}, {}, {}

        def products(part, side, target):
            for i in range(4):
                loads[i * 4 + side * 2 + part].wait()
            for i in range(4):
                target[part, i] = jnp.dot(
                    left[...], kbuf[i * 4 + side * 2 + part], preferred_element_type=F32
                )

        def to_partner(part):
            dcopy[part] = pltpu.make_async_remote_copy(
                src_ref=dsend.at[part], dst_ref=drecv.at[part],
                send_sem=dsem.at[0, part], recv_sem=dsem.at[1, part],
                device_id=partner, device_id_type=MESH,
            )
            dcopy[part].start()

        def merge(part):
            dcopy[part].wait_recv()
            for i, d in enumerate(ORDER):
                total = own[part, i] + drecv[part, i]
                if d == 0:
                    own[part, i] = total
                    continue
                ysend[part, d - 1] = total
                ycopy[part, d] = pltpu.make_async_remote_copy(
                    src_ref=ysend.at[part, d - 1], dst_ref=yrecv.at[part, d - 1],
                    send_sem=ysem.at[0, part, d - 1], recv_sem=ysem.at[1, part, d - 1],
                    device_id=y_peer[d], device_id_type=MESH,
                )
                ycopy[part, d].start()

        def early_ghost(d):
            return pltpu.make_async_remote_copy(
                src_ref=gsend, dst_ref=gearly.at[d],
                send_sem=gxsem.at[0], recv_sem=gxsem.at[1 + d],
                device_id=place(3, y, z, core), device_id_type=MESH,
            )

        def ahead(part, partial):
            for step in range(2):
                for half in range(2):
                    at = step * 4 + part * 2 + half
                    line = 126 + step
                    gsend[at : at + 1] = partial[line : line + 1, half * 128 : half * 128 + 128]
            if part == 1:
                pl.when(x < 3)(early_ghost(x).start)

        def sum_y(part):
            total = own[part, 3]
            for d in (1, 3, 2):
                ycopy[part, d].wait_recv()
                total = total + yrecv[part, d - 1]
            split = split_rows(total)
            stack = jnp.concatenate([split[k] for k in (0, 1, 0, 2, 0, 1)], axis=0)
            partial = jnp.dot(wide[:, 0:192], stack, preferred_element_type=F32)
            for at in range(4):
                xsend[part, at] = partial[at * 32 : at * 32 + 32]
            ahead(part, partial)
            for d in (1, 3, 2):
                xcopy[part, d] = pltpu.make_async_remote_copy(
                    src_ref=xsend.at[part, (x + d) % 4], dst_ref=xrecv.at[part, d - 1],
                    send_sem=xsem.at[0, part, d - 1], recv_sem=xsem.at[1, part, d - 1],
                    device_id=x_peer[d], device_id_type=MESH,
                )
                xcopy[part, d].start()

        def z_copy(part, k):
            lo = (z_lo + k) % 4
            d = (part * 4 + lo + 8 - z) % 8
            at = (d + 7) % 8
            return d, pltpu.make_async_remote_copy(
                src_ref=zsend.at[part, pl.ds(pl.multiple_of(lo * 8, 8), 8)],
                dst_ref=zrecv.at[at],
                send_sem=zsem.at[0, at], recv_sem=zsem.at[1, at],
                device_id=place(x, y, part * 4 + lo, core), device_id_type=MESH,
            )

        def sum_x(part):
            total = xsend[part, x]
            for d in (1, 3, 2):
                xcopy[part, d].wait_recv()
                total = total + xrecv[part, d - 1]
            zsend[part] = total
            for k in (2, 1, 3, 0):
                d, copy = z_copy(part, k)
                if k == 0:
                    pl.when(d != 0)(copy.start)
                else:
                    copy.start()

        def strip(at, carry):
            base = pl.multiple_of(at * 32, 8)
            state = [fields[j, pl.ds(base, 48), :] for j in range(5)]
            values, rest = state[0:3], state[3:5]
            terms = face_terms(*rest)
            for _ in range(2):
                values = advance(*values, *rest, terms)
            for ref, value in zip((surf_o, flow_x_o, flow_y_o), values):
                ref[pl.ds(base, 32), :] = value[8:40]
            return carry

    with jax.named_scope("spectrum"):
        products(0, 0, dsend)
    with jax.named_scope("barrier"):
        pl.semaphore_wait(barrier, greetings)
    with jax.named_scope("spectrum_1"):
        to_partner(0)
        products(0, 1, own)
    with jax.named_scope("row_halos"):
        for copy in borders:
            copy.wait()
        for source in (0, 248):
            fields[4, source + 8 : source + 16, :] = mbuf[source : source + 8].astype(F32)
        ns_copies = []
        for at, (first, last, peer, inside) in enumerate(
            ((8, 264, north, row > 0), (256, 0, south, row < 15))
        ):
            copy = pltpu.make_async_remote_copy(
                src_ref=fields.at[:, pl.ds(first, 8)],
                dst_ref=fields.at[:, pl.ds(last, 8)],
                send_sem=nssem.at[0, at], recv_sem=nssem.at[1, at],
                device_id=peer, device_id_type=MESH,
            )
            pl.when(inside)(copy.start)
            ns_copies.append((copy, inside))
    with jax.named_scope("spectrum_2"):
        products(1, 0, dsend)
        to_partner(1)
    with jax.named_scope("merge_0"):
        merge(0)
        for d in range(1, 4):
            pl.semaphore_signal(known.at[d + 1], inc=1, device_id=y_peer[d], device_id_type=MESH)
    with jax.named_scope("spectrum_3"):
        products(1, 1, own)
    with jax.named_scope("merge_1"):
        merge(1)

    with jax.named_scope("widen"):
        local[2].wait()
        split = split_rows(tab[0:32])
        wide[...] = jnp.concatenate(
            [*(split[k].astype(F32) for k in (0, 0, 1, 0, 2, 1)), jnp.zeros((64, 128), F32)], axis=0
        ).T.astype(BF16)
        for copy in grids:
            copy.wait()
        fields[4, 16:256, :] = mbuf[8:248].astype(F32)

    with jax.named_scope("water"):
        lax.fori_loop(1, 3, strip, 0)
    with jax.named_scope("relay"):
        for d in range(1, 4):
            pl.semaphore_wait(known.at[d + 1], 1)
        for at, d in enumerate((2, 6)):
            pl.semaphore_signal(known.at[at], inc=1, device_id=z_peer[d], device_id_type=MESH)

    with jax.named_scope("sum_y_0"):
        sum_y(0)

    with jax.named_scope("column_halos"):
        pl.when(row < 15)(ns_copies[0][0].wait_recv)
        pl.when(row > 0)(ns_copies[1][0].wait_recv)

        @pl.when(row == 0)
        def _():
            fields[:, 0:8, :] = jnp.zeros((5, 8, 256), F32)

        @pl.when(is_edge)
        def _():
            fields[:, 264:272, :] = jnp.zeros((5, 8, 256), F32)

        lane = lax.broadcasted_iota(jnp.int32, (272, 128), 1)
        ew_copies = []
        for at, (first, shift, peer, inside) in enumerate(
            ((0, 0, west, col > 0), (128, 4, east, col < 15))
        ):
            packed = jnp.zeros((272, 128), F32)
            for j in range(5):
                block = fields[j, :, first : first + 128]
                if 4 * j + shift:
                    block = pltpu.roll(block, 4 * j + shift, 1)
                packed = jnp.where((lane >> 2) == j, block, packed)
            packed = jnp.concatenate([packed, jnp.zeros((112, 128), F32)], axis=0)
            ewsend[at] = packed.T[0:24]
            copy = pltpu.make_async_remote_copy(
                src_ref=ewsend.at[at], dst_ref=ewrecv.at[at],
                send_sem=ewsem.at[0, at], recv_sem=ewsem.at[1, at],
                device_id=peer, device_id_type=MESH,
            )
            ew_copies.append((copy, inside))

    with jax.named_scope("sum_y_1"):
        sum_y(1)

    with jax.named_scope("far"):
        for at in range(2):
            pl.semaphore_wait(known.at[at], 1)
        for copy, inside in ew_copies:
            pl.when(inside)(copy.start)

    with jax.named_scope("water_1"):
        lax.fori_loop(3, 7, strip, 0)
    with jax.named_scope("sum_x_0"):
        sum_x(0)
    with jax.named_scope("ghost_send"):
        here = pl.ds(pl.multiple_of((z * 4 + y) * 8, 8), 8)

        def ghost_copy(index):
            return pltpu.make_async_remote_copy(
                src_ref=gtotal, dst_ref=grecv.at[here],
                send_sem=gssem.at[index], recv_sem=grsem,
                device_id=(15, index * 2 + core), device_id_type=MESH,
            )

        @pl.when(x == 3)
        def _():
            total = gsend[...]
            for d in range(3):
                early_ghost(d).wait_recv()
                total = total + gearly[d]
            gtotal[...] = total
            for index in range(8):
                pl.when((row != 15) | (col != index * 2 + core))(ghost_copy(index).start)

    with jax.named_scope("sum_x_1"):
        sum_x(1)

    with jax.named_scope("more_water"):
        lax.fori_loop(7, 9, lambda at, carry: strip(at % 8, carry), 0)

    with jax.named_scope("selection"):
        @pl.when(is_edge)
        def _():
            at = lax.broadcasted_iota(jnp.int32, (128, 384), 1)
            column = col * 256 + jnp.where(at >= 320, at - 384, at)
            turned = jnp.concatenate(
                [cellbuf[...].astype(F32), jnp.zeros((96, 128), F32)], axis=0
            ).T.astype(jnp.int32)
            found = jnp.zeros((128, 384), F32)
            for block in range(32):
                found = jnp.where(turned[:, block : block + 1] == column, block + 1.0, found)
            onehot[...] = jnp.where(found > 0.0, 1.0, 0.0).astype(BF16)
            blocks[...] = jnp.broadcast_to(jnp.sum(found, axis=0, keepdims=True), (8, 384))

    with jax.named_scope("side_water"):
        for at, ((copy, _), inside) in enumerate(zip(ew_copies, (col < 15, col > 0))):
            pl.when(inside)(copy.wait_recv)

            @pl.when(~inside)
            def _():
                ewrecv[at] = jnp.zeros((24, 384), F32)

        from_east, from_west = ewrecv[0], ewrecv[1]
        for j in range(5):
            for at, piece in enumerate((from_west, ewsend[0], ewsend[1], from_east)):
                sides[j, at * 4 : at * 4 + 4] = piece[j * 4 : j * 4 + 4]
        state = [sides[j] for j in range(5)]
        values, rest = state[0:3], state[3:5]
        terms = face_terms(*rest, (0, 1))
        for _ in range(2):
            values = advance(*values, *rest, terms, (0, 1))
        turned = jnp.concatenate([*values, jnp.zeros((80, 384), F32)], axis=0).T[8:264]
        lane = lax.broadcasted_iota(jnp.int32, (256, 128), 1)
        for j, ref in enumerate((surf_o, flow_x_o, flow_y_o)):
            ref[:, 0:128] = jnp.where(
                lane < 2, pltpu.roll(turned, 124 - 16 * j, 1), ref[:, 0:128]
            )
            ref[:, 128:256] = jnp.where(
                lane >= 126, pltpu.roll(turned, 116 - 16 * j, 1), ref[:, 128:256]
            )

        @pl.when(is_edge)
        def _():
            blank = jnp.zeros((104, 256), F32)
            right, left_side = (
                jnp.concatenate([piece[:, 128:384], blank], axis=0).T[120:144]
                for piece in (from_east, from_west)
            )
            lane = lax.broadcasted_iota(jnp.int32, (24, 128), 1)
            for j in range(5):
                first = pltpu.roll(right, 128 - 4 * j, 1) if j else right
                wrapped = pltpu.roll(left_side, 124 - 4 * j, 1)
                tail[j] = jnp.where(lane < 2, first, jnp.where(lane >= 126, wrapped, 0.0))

    with jax.named_scope("sum_z"):
        total = zsend[z_hi, pl.ds(pl.multiple_of(z_lo * 8, 8), 8)]
        for d in range(1, 8):
            pltpu.make_async_copy(zrecv.at[d - 1], zrecv.at[d - 1], zsem.at[1, d - 1]).wait()
            total = total + zrecv[d - 1]
        series_o[...] = total

    with jax.named_scope("ghost"):
        @pl.when(is_edge)
        def _():
            grecv[here] = gtotal[...]
            pltpu.make_async_copy(
                grecv.at[pl.ds(0, 248)], grecv.at[pl.ds(0, 248)], grsem
            ).wait()
            value = grecv[0:32]
            for other_z in range(1, 8):
                value = value + grecv[other_z * 32 : other_z * 32 + 32]
            gpair[core] = value
            share = pltpu.make_async_remote_copy(
                src_ref=gpair.at[core], dst_ref=gpair.at[core],
                send_sem=gpsem.at[0], recv_sem=gpsem.at[1],
                device_id=partner, device_id_type=MESH,
            )
            share.start()
            share.wait_send()
            share.wait_recv()
            value = jnp.concatenate([gpair[0], gpair[1]], axis=0)
            picked = jnp.dot(
                jnp.concatenate(split_rows(value), axis=0), onehot[...],
                preferred_element_type=F32,
            )
            picked = picked[128:192] + picked[64:128] + picked[0:64]
            at = lax.broadcasted_iota(jnp.int32, (64, 384), 0)
            block = ((at >> 3) & 3) * 8 + (at & 2) * 2 + (at >> 5) * 2 + (at & 1)
            picked = jnp.where((block + 1).astype(F32) == blocks[0:1], picked, 0.0)
            ghost = [
                jnp.sum(jnp.where(((at >> 2) & 1) == step, picked, 0.0), axis=0, keepdims=True)
                for step in range(2)
            ]
            beyond = lax.broadcasted_iota(jnp.int32, (24, 384), 0) == 16
            state = [
                jnp.concatenate([fields[j, 248:272, :], tail[j]], axis=1) for j in range(5)
            ]
            rest = [jnp.where(beyond, 1.0, value) for value in state[3:5]]
            values = state[0:3]
            terms = face_terms(*rest)
            for step in range(2):
                values = [
                    jnp.where(beyond, ghost[step], values[0]),
                    jnp.where(beyond, 0.0, values[1]),
                    jnp.where(beyond, 0.0, values[2]),
                ]
                values = advance(*values, *rest, terms)
            for ref, value in zip((surf_o, flow_x_o, flow_y_o), values):
                ref[248:256, :] = value[8:16, 0:256]

    with jax.named_scope("drain"):
        for copy in [*dcopy.values(), *ycopy.values(), *xcopy.values()]:
            copy.wait_send()
        for copy, inside in [*ns_copies, *ew_copies]:
            pl.when(inside)(copy.wait_send)
        for part in range(2):
            for k in range(4):
                d, copy = z_copy(part, k)
                pl.when(d != 0)(copy.wait_send)
        pl.when(x < 3)(early_ghost(x).wait_send)

        @pl.when(x == 3)
        def _():
            for index in range(8):
                pl.when((row != 15) | (col != index * 2 + core))(ghost_copy(index).wait_send)


def write_out(*refs):
    sources, targets, sems = refs[0:4], refs[4:8], refs[8]
    copies = [
        pltpu.make_async_copy(source, target, sems.at[j])
        for j, (source, target) in enumerate(zip(sources, targets))
    ]
    for copy in copies:
        copy.start()
    for copy in copies:
        copy.wait()


def on_device(
    kernel_hat, coefficients, wave_speed_sq, wet_mask, boundary_cell, height, flux_x, flux_y
):
    field = jax.ShapeDtypeStruct((256, 256), F32)
    dma = pltpu.SemaphoreType.DMA
    shapes = (jax.ShapeDtypeStruct((8, 256), F32), field, field, field)
    operands = [
        pltpu.with_memory_space_constraint(value, pltpu.MemorySpace.HBM)
        for value in (
            kernel_hat.reshape(1024, 4096),
            coefficients.T,
            wave_speed_sq,
            wet_mask,
            boundary_cell.reshape(32, 128),
            height,
            flux_x,
            flux_y,
            jnp.asarray(transform_tables()),
        )
    ]
    results = pl.pallas_call(
        kernel,
        out_shape=shapes,
        in_specs=[pl.BlockSpec(memory_space=pltpu.MemorySpace.HBM)] * 9,
        out_specs=[pl.BlockSpec(memory_space=pltpu.VMEM)] * 4,
        scratch_shapes=[
            pltpu.VMEM((16, 1024, 256), BF16),
            pltpu.VMEM((128, 128), F32),
            pltpu.VMEM((32, 128), F32),
            pltpu.VMEM((256, 256), jnp.int32),
            pltpu.VMEM((32, 128), jnp.int32),
            pltpu.VMEM((32, 1024), BF16),
            pltpu.VMEM((2, 4, 32, 256), F32),
            pltpu.VMEM((2, 4, 32, 256), F32),
            pltpu.VMEM((2, 4, 32, 256), F32),
            pltpu.VMEM((2, 3, 32, 256), F32),
            pltpu.VMEM((2, 3, 32, 256), F32),
            pltpu.VMEM((2, 4, 32, 256), F32),
            pltpu.VMEM((2, 3, 32, 256), F32),
            pltpu.VMEM((2, 32, 256), F32),
            pltpu.VMEM((7, 8, 256), F32),
            pltpu.VMEM((8, 128), F32),
            pltpu.VMEM((3, 8, 128), F32),
            pltpu.VMEM((8, 128), F32),
            pltpu.VMEM((2, 32, 128), F32),
            pltpu.VMEM((256, 128), F32),
            pltpu.VMEM((5, 272, 256), F32),
            pltpu.VMEM((2, 24, 384), F32),
            pltpu.VMEM((2, 24, 384), F32),
            pltpu.VMEM((5, 16, 384), F32),
            pltpu.VMEM((5, 24, 128), F32),
            pltpu.VMEM((128, 384), BF16),
            pltpu.VMEM((8, 384), F32),
            pltpu.VMEM((128, 256), BF16),
            dma((16,)),
            dma((9,)),
            dma((10,)),
            dma((2, 2)),
            dma((2, 2, 3)),
            dma((2, 2, 3)),
            dma((2, 8)),
            dma((4,)),
            dma((2,)),
            dma((8,)),
            dma(()),
            dma((2, 2)),
            dma((2, 2)),
            pltpu.SemaphoreType.REGULAR((5,)),
        ],
        compiler_params=pltpu.CompilerParams(
            collective_id=0, has_side_effects=True, vmem_limit_bytes=48 * 1024 * 1024
        ),
    )(*operands)
    return pl.pallas_call(
        write_out,
        out_shape=shapes,
        in_specs=[pl.BlockSpec(memory_space=pltpu.VMEM)] * 4,
        out_specs=[pl.BlockSpec(memory_space=pltpu.MemorySpace.HBM)] * 4,
        scratch_shapes=[dma((4,))],
        compiler_params=pltpu.CompilerParams(vmem_limit_bytes=16 * 1024 * 1024),
    )(*results)


def solution(mesh):
    return jax.shard_map(
        on_device,
        mesh=mesh,
        in_specs=(
            P(None, "rows", "cols", None),
            P(None, "cols"),
            P("rows", "cols"),
            P("rows", "cols"),
            P(),
            P("rows", "cols"),
            P("rows", "cols"),
            P("rows", "cols"),
        ),
        out_specs=(P("rows", "cols"), P("rows", "cols"), P("rows", "cols"), P("rows", "cols")),
        check_vma=False,
    )
```
